128 devices in a mesh: dp: 32 (over z, y, core), mp: 4 (over x).
Axes of the slice: x: 4, y: 4, z: 4, core: 2. Of those that a mesh axis runs over, the one named last changes fastest.
Arguments:
- queries: bfloat16 [1024, 64, 128], P('dp', 'mp'), may hold values from -8 to 8
- lookup_sheets: bfloat16 [32768, 16, 8, 128], P('dp', None, 'mp'), may hold values from -6 to 6
- content_sheets: bfloat16 [32768, 16, 8, 128], P('dp', None, 'mp'), may hold values from -12 to 12
- page_table: int32 [1024, 32], replicated, may hold values from 0 to 32767, as said below
- context_len: int32 [1024], replicated, may hold values from 32 to 512, as said below
- out_weight: bfloat16 [8192, 8192], P('mp', 'dp'), may hold values from -0.0625 to 0.0625
Outputs:
- attention: bfloat16 [1024, 64, 128], P('dp', 'mp')
- projected: bfloat16 [1024, 8192], P('mp', 'dp')
The draws below stay inside these ranges and needn't reach their ends.
Inputs may be any that keep to these rules, and one draw needn't show every extreme that they name: `page_table`: every entry names a pool page, 0 to 32767, and every pool page appears exactly once in the whole table. `context_len`: each length lies between 32 and 512; most contexts are short, and some request has exactly 512 tokens.
All inputs are finite; a program needn't handle non-finite values.
Results may differ from the reference program's by a relative error of at most 0.0015.
Values may be sent and summed in bfloat16 or wider, within the bound.
A program may use at most 128 MiB of HBM per device.

```python
import jax
import jax.numpy as jnp
from jax import lax

D = 8192
ASKER_COUNT = 64
LOOKUP_COUNT = 8
SPAN_PER_ASKER = 128
SHEET_CAPACITY = 16
REQ = 1024
SHEET_TOTAL = 32768
MAXPG = 32


def draw_context_len(key, part):
    key_len, key_pos = jax.random.split(jax.random.fold_in(key, 11))
    longest = MAXPG * SHEET_CAPACITY
    lowest = max(longest // 16, 1)
    drawn = jax.random.randint(key_len, (REQ,), 0, longest, dtype=jnp.int32)
    skewed = drawn * drawn // longest * drawn // longest
    lengths = lowest + skewed * (longest - lowest) // longest
    chosen = jax.random.randint(key_pos, (), 0, REQ, dtype=jnp.int32)
    return lengths.at[chosen].set(longest).astype(jnp.int32)


def draw_page_table(key, part):
    shuffled = jax.random.permutation(jax.random.fold_in(key, 23), REQ * MAXPG)
    return shuffled.reshape(REQ, MAXPG).astype(jnp.int32)


def levels(key, dims, cuts, least, top_value):
    def one(axis_at, shards_of):
        steps = jax.random.uniform(jax.random.fold_in(jax.random.fold_in(key, 6), axis_at), (shards_of,), jnp.float32, least / len(cuts), top_value / len(cuts))
        return jnp.repeat(jnp.exp(steps), dims[axis_at] // shards_of).reshape((-1,) + (1,) * (len(dims) - axis_at - 1))

    gain = one(*cuts[0])
    for cut in cuts[1:]:
        gain = gain * one(*cut)
    return gain


def bell_draw(rng, extent, width, reach, pieces=(), kind=jnp.bfloat16):
    loudness = levels(rng, extent, pieces, -0.22, 0.18) if pieces else 1.0
    values = jax.random.normal(rng, extent, jnp.float32) * width * loudness
    return jnp.minimum(jnp.maximum(values, -reach), reach).astype(kind)


def setup_inputs(seed: int = 0) -> dict:
    key_list = jax.random.split(jax.random.key(seed), 7)
    return {
        "queries": bell_draw(key_list[0], (REQ, ASKER_COUNT, SPAN_PER_ASKER), 1.5, 8.0, ((0, 32), (1, 4))),
        "lookup_sheets": bell_draw(key_list[1], (SHEET_TOTAL, SHEET_CAPACITY, LOOKUP_COUNT, SPAN_PER_ASKER), 1.0, 6.0, ((0, 32), (2, 4))),
        "content_sheets": bell_draw(key_list[2], (SHEET_TOTAL, SHEET_CAPACITY, LOOKUP_COUNT, SPAN_PER_ASKER), 2.0, 12.0, ((0, 32), (2, 4))),
        "page_table": draw_page_table(jax.random.fold_in(key_list[6], 71), 0),
        "context_len": draw_context_len(jax.random.fold_in(key_list[6], 71), 0),
        "out_weight": bell_draw(key_list[5], (ASKER_COUNT * SPAN_PER_ASKER, D), (ASKER_COUNT * SPAN_PER_ASKER) ** -0.5, 0.0625, ((0, 4), (1, 32))),
    }


def reference(queries, lookup_sheets, content_sheets, page_table, context_len, out_weight):
    cluster_member = ASKER_COUNT // LOOKUP_COUNT

    def one_request(inputs):
        asker_vector, page_ids, length = inputs
        keys = lookup_sheets[page_ids].astype(jnp.float32)
        values = content_sheets[page_ids].astype(jnp.float32)
        clustered_askers = asker_vector.reshape(LOOKUP_COUNT, cluster_member, SPAN_PER_ASKER).astype(jnp.float32)
        scores = jnp.einsum("kgd,ptkd->kgpt", clustered_askers, keys) * (SPAN_PER_ASKER ** -0.5)
        position = (jnp.arange(MAXPG, dtype=jnp.int32)[:, None] * SHEET_CAPACITY
                    + jnp.arange(SHEET_CAPACITY, dtype=jnp.int32)[None, :])
        is_valid = position < length
        scores = jnp.where(is_valid, scores, -1e30)
        page_peak = jnp.max(scores, axis=-1)
        weights = jnp.where(is_valid, jnp.exp(scores - page_peak[..., None]), 0.0)
        page_mass = jnp.sum(weights, axis=-1)
        rounded = lax.optimization_barrier(weights.astype(jnp.bfloat16)).astype(jnp.float32)
        page_acc = jnp.einsum("kgpt,ptkd->kgpd", rounded, values)
        peak_row = jnp.max(page_peak, axis=-1)
        factor = jnp.exp(page_peak - peak_row[..., None])
        acc_row = jnp.sum(page_acc * factor[..., None], axis=2)
        mass_row = jnp.sum(page_mass * factor, axis=2)
        return (acc_row / mass_row[..., None]).astype(jnp.bfloat16).reshape(ASKER_COUNT, SPAN_PER_ASKER)

    attention = lax.map(one_request, (queries, page_table, context_len))
    flat_rows = attention.reshape(attention.shape[0], ASKER_COUNT * SPAN_PER_ASKER)
    projected = jnp.dot(flat_rows, out_weight, preferred_element_type=jnp.float32).astype(jnp.bfloat16)
    return attention, projected
```

```python
import functools

import jax
import jax.numpy as jnp
from jax import lax
from jax.experimental import pallas as pl
from jax.experimental.pallas import tpu as pltpu
from jax.sharding import Mesh
from jax.sharding import PartitionSpec as P

DP = ("dp_0", "dp_1", "dp_2")
MESH = pl.DeviceIdType.MESH
LOW = -1e30
F32 = jnp.float32
BF16 = jnp.bfloat16
NT = (((1,), (1,)), ((), ()))
VMEM = pl.BlockSpec(memory_space=pltpu.VMEM)
SMEM = pl.BlockSpec(memory_space=pltpu.SMEM)
ANY = pl.BlockSpec(memory_space=pl.ANY)


def wrap(value):
    return lax.rem(value + 8, 4)


def place():
    z, y, c = (lax.axis_index(name) for name in DP)
    return z, y, c, 1 - 2 * c


def plane_id(z, y, c):
    return {"dp_0": z, "dp_1": y, "dp_2": c}


def greet(devices):
    barrier = pltpu.get_barrier_semaphore()
    for device in devices:
        pl.semaphore_signal(barrier, inc=1, device_id=device, device_id_type=MESH)
    pl.semaphore_wait(barrier, len(devices))


def remote(src, dst, send_sem, recv_sem, device):
    return pltpu.make_async_remote_copy(
        src_ref=src,
        dst_ref=dst,
        send_sem=send_sem,
        recv_sem=recv_sem,
        device_id=device,
        device_id_type=MESH,
    )


def plane_gather(own, full, ssem, rsem, dsend, drecv, between=()):
    z, y, c, s = place()
    work = list(between)

    def fill():
        if work:
            work.pop(0)()

    def at(h, a, b):
        return full.at[a, b, c, h] if h == 0 else full.at[b, a, c, h]

    def device(h, a, b):
        return plane_id(a, b, c) if h == 0 else plane_id(b, a, c)

    def mine(h):
        return (z, y) if h == 0 else (y, z)

    sent = []

    def go(h, group, m, src, dst, target):
        copy = remote(src, dst, ssem.at[h, group, m], rsem.at[h, group, m], target)
        copy.start()
        sent.append(copy)

    def come(h, group, m, dst):
        remote(dst, dst, ssem.at[h, group, m], rsem.at[h, group, m], plane_id(z, y, c)).wait_recv()

    def share(h, slot, src, dst):
        copy = remote(src, dst, dsend.at[h, slot], drecv.at[h, slot], plane_id(z, y, 1 - c))
        copy.start()
        sent.append(copy)

    def spread(h, group, slot, src, a, b):
        go(h, group, 0, src, at(h, a, b), device(h, mine(h)[0], wrap(b + s)))
        go(h, group, 1, src, at(h, a, b), device(h, mine(h)[0], wrap(b - s)))

    def first(h):
        a, b = mine(h)
        go(h, 0, 0, own.at[h], at(h, a, b), device(h, wrap(a + s), b))
        go(h, 0, 1, own.at[h], at(h, a, b), device(h, wrap(a - s), b))

    for h in range(2):
        first(h)
    for h in range(2):
        share(h, 0, own.at[h], at(h, *mine(h)))
        spread(h, 1, 0, own.at[h], *mine(h))
    fill()
    for h in range(2):
        a, b = mine(h)
        near = wrap(a - s)
        come(h, 0, 0, at(h, near, b))
        go(h, 0, 2, at(h, near, b), at(h, near, b), device(h, wrap(a + s), b))
        spread(h, 2, 4, at(h, near, b), near, b)
        share(h, 4, at(h, near, b), at(h, near, b))
    for h in range(2):
        a, b = mine(h)
        near = wrap(a + s)
        come(h, 0, 1, at(h, near, b))
        spread(h, 3, 8, at(h, near, b), near, b)
        share(h, 8, at(h, near, b), at(h, near, b))
    fill()
    for h in range(2):
        a, b = mine(h)
        far = wrap(a + 2)
        come(h, 0, 2, at(h, far, b))
        spread(h, 4, 12, at(h, far, b), far, b)
        share(h, 12, at(h, far, b), at(h, far, b))
    fill()
    for group, step in ((1, 0), (2, -1), (3, 1), (4, 2)):
        for h in range(2):
            a, b = mine(h)
            row = wrap(a + step * s)
            near = wrap(b - s)
            come(h, group, 0, at(h, row, near))
            go(h, group, 2, at(h, row, near), at(h, row, near), device(h, a, wrap(b + s)))
            share(h, 4 * (group - 1) + 1, at(h, row, near), at(h, row, near))
            other = wrap(b + s)
            come(h, group, 1, at(h, row, other))
            share(h, 4 * (group - 1) + 2, at(h, row, other), at(h, row, other))
        fill()
    for group, step in ((1, 0), (2, -1), (3, 1), (4, 2)):
        for h in range(2):
            a, b = mine(h)
            row = wrap(a + step * s)
            far = wrap(b + 2)
            come(h, group, 2, at(h, row, far))
            share(h, 4 * (group - 1) + 3, at(h, row, far), at(h, row, far))
    for h in range(2):
        for slot in range(16):
            where = full.at[0, 0, 1 - c, h]
            remote(where, where, dsend.at[h, slot], drecv.at[h, slot], plane_id(z, y, 1 - c)).wait_recv()
    return sent


def gather_sems():
    return [
        pltpu.SemaphoreType.DMA((2, 5, 3)),
        pltpu.SemaphoreType.DMA((2, 5, 3)),
        pltpu.SemaphoreType.DMA((2, 16)),
        pltpu.SemaphoreType.DMA((2, 16)),
    ]


def queries_kernel(pool_bits, page_len, q_ref, table_ref, len_ref, full_ref, list_ref, count_ref,
                   lo_ref, hi_ref, part_ref, ssem, rsem, dsend, drecv):
    z, y, c, s = place()
    me = (z * 4 + y) * 2 + c
    greet([plane_id(wrap(z + 1), y, c), plane_id(wrap(z - 1), y, c), plane_id(z, wrap(y + 1), c),
           plane_id(z, wrap(y - 1), c), plane_id(z, y, 1 - c)])
    full_ref[z, y, c] = q_ref[...]

    def place_pages():
        slots = table_ref.shape[0]
        slot = lax.broadcasted_iota(jnp.int32, (slots, 128), 0)
        lane = lax.broadcasted_iota(jnp.int32, (slots, 128), 1)
        blocks = table_ref.shape[1] // 128
        mine, tokens, page, owner = [], [], [], []
        for t in range(blocks):
            ids = table_ref[:, t * 128:(t + 1) * 128]
            length = jnp.broadcast_to(len_ref[t:t + 1, :], (slots, 128))
            left = jnp.clip(length - slot * page_len, 0, page_len)
            mine.append(jnp.where(((ids >> pool_bits) == me) & (left > 0), 1.0, 0.0))
            tokens.append(left)
            page.append(ids & ((1 << pool_bits) - 1))
            owner.append(lane + t * 128)
        mine, tokens, page, owner = (jnp.concatenate(v, axis=0) for v in (mine, tokens, page, owner))
        rows = slots * blocks
        mine_h = mine.astype(BF16)
        i = lax.broadcasted_iota(jnp.int32, (128, 128), 0)
        j = lax.broadcasted_iota(jnp.int32, (128, 128), 1)
        ahead = jnp.where(i < j, 1.0, 0.0).astype(BF16)
        every = jnp.ones((128, 128), BF16)
        within = jnp.dot(mine_h, ahead, preferred_element_type=F32)
        total = jnp.dot(mine_h, every, preferred_element_type=F32)
        i = lax.broadcasted_iota(jnp.int32, (rows, rows), 0)
        j = lax.broadcasted_iota(jnp.int32, (rows, rows), 1)
        before = jnp.where(j < i, 1.0, 0.0).astype(BF16)
        same = jnp.where((j < i) & (i // slots == j // slots), 1.0, 0.0).astype(BF16)
        offset = jnp.dot(before, total.astype(BF16), preferred_element_type=F32)
        earlier = jnp.dot(same, mine_h, preferred_element_type=F32)
        rank = (within + offset).astype(jnp.int32)
        lo_ref[...] = jnp.where(mine > 0.0, rank & 127, -1)
        hi_ref[...] = jnp.where(mine > 0.0, rank >> 7, -1)
        part_ref[0] = (page & 255).astype(F32)
        part_ref[1] = (owner & 255).astype(F32)
        part_ref[2] = ((page >> 8) + ((owner >> 8) << 2) + ((tokens - 1) << 4)).astype(F32)
        part_ref[3] = jnp.where(earlier > 0.0, 0.0, 1.0)
        return (offset + total)[rows - 1:rows, :]

    def make_list():
        count = place_pages()
        rows = lo_ref.shape[0]
        sub = lax.broadcasted_iota(jnp.int32, (128, 128), 0)
        sub8 = lax.broadcasted_iota(jnp.int32, (8, 128), 0)

        def step(n, total):
            base = pl.multiple_of(n * 8, 8)
            lo8 = lo_ref[pl.ds(base, 8), :]
            hi8 = hi_ref[pl.ds(base, 8), :]
            p8 = [part_ref[k, pl.ds(base, 8), :] for k in range(4)]
            wide, tall = [], []
            for r in range(8):
                wide.append(jnp.where(sub == lo8[r:r + 1, :], 1.0, 0.0).astype(BF16))
                hit = sub8 == hi8[r:r + 1, :]
                tall.append(jnp.concatenate(
                    [jnp.where(hit, p8[k][r:r + 1, :], 0.0) for k in range(4)], axis=0).astype(BF16))
            wide = jnp.concatenate(wide, axis=1)
            tall = jnp.concatenate(tall, axis=1)
            return total + lax.dot_general(wide, tall, NT, preferred_element_type=F32)

        total = lax.fori_loop(0, rows // 8, step, jnp.zeros((128, 32), F32))
        total = jnp.concatenate([total, jnp.zeros((128, 96), F32)], axis=1).T.astype(jnp.int32)
        p0, p1, p2, p3 = (total[8 * k:8 * k + 8, :] for k in range(4))
        page = p0 + ((p2 & 3) << 8)
        owner = p1 + (((p2 >> 2) & 3) << 8)
        tokens = (p2 >> 4) + 1
        place_of = sub8 * 128 + lax.broadcasted_iota(jnp.int32, (8, 128), 1)
        number = jnp.broadcast_to(count, (8, 128)).astype(jnp.int32)
        word = page + (owner << 10) + (tokens << 21) + (p3 << 26)
        list_ref[...] = jnp.where(place_of < number, word, (1024 << 10) + (1 << 21) + (1 << 26))
        count_ref[...] = number

    for copy in plane_gather(q_ref, full_ref, ssem, rsem, dsend, drecv, between=(make_list,)):
        copy.wait_send()


def gather_queries(queries, table, lengths, pool, page_len):
    req = table.shape[1]
    rows = table.shape[0] * req // 128
    mine, heads, dim = queries.shape
    half = mine // 2
    return pl.pallas_call(
        functools.partial(queries_kernel, pool.bit_length() - 1, page_len),
        out_shape=(
            jax.ShapeDtypeStruct((4, 4, 2, 2, half, heads, dim), BF16),
            jax.ShapeDtypeStruct((8, 128), jnp.int32),
            jax.ShapeDtypeStruct((8, 128), jnp.int32),
        ),
        in_specs=[VMEM] * 3,
        out_specs=(VMEM, VMEM, VMEM),
        scratch_shapes=[
            pltpu.VMEM((rows, 128), jnp.int32),
            pltpu.VMEM((rows, 128), jnp.int32),
            pltpu.VMEM((4, rows, 128), F32),
        ] + gather_sems(),
        compiler_params=pltpu.CompilerParams(collective_id=0, has_side_effects=True, vmem_limit_bytes=24 << 20),
        name="gather_queries",
    )(queries.reshape(2, half, heads, dim), table, lengths)


def pages_kernel(scale, list_ref, count_ref, q_ref, k_hbm, v_hbm, acc_ref, k_ref, v_ref, m_ref, l_ref, sems):
    pool = k_ref.shape[0]
    chunks = sems.shape[1]
    size = pool // chunks
    loads = []
    for n in range(chunks):
        rows = pl.ds(n * size, size)
        for w, (src, dst) in enumerate(((k_hbm, k_ref), (v_hbm, v_ref))):
            copy = pltpu.make_async_copy(src.at[rows], dst.at[rows], sems.at[w, n])
            copy.start()
            loads.append(copy)
    lane = lax.broadcasted_iota(jnp.int32, (8, 128), 1)
    blank = jnp.where(lane < 32, LOW, 0.0)

    def clear(d, carry):
        for hh in range(2):
            acc_ref[hh, d, 0:32] = jnp.zeros((32, 8, 128), F32)
            acc_ref[hh, d, 32] = blank
        return carry

    lax.fori_loop(0, acc_ref.shape[1], clear, 0)
    for copy in loads:
        copy.wait()

    i = lax.broadcasted_iota(jnp.int32, (16, 128), 0)
    j = lax.broadcasted_iota(jnp.int32, (16, 128), 1)
    kv_match = (i // 8) == (j % 2)
    token = (j % 32) // 2
    token_of = [jnp.where(kv_match & (j // 32 == n), token, 1 << 20) for n in range(4)]

    def step(n, carry):
        base = n * 16
        entries = []
        for e in range(16):
            word = list_ref[(base + e) >> 7, (base + e) & 127]
            entries.append((word & 1023, (word >> 10) & 2047, (word >> 21) & 31, (word >> 26) & 1))
        results = []
        for g in range(4):
            four = entries[4 * g:4 * g + 4]
            qs = jnp.concatenate([q_ref[jnp.minimum(r, 1023)] for _, r, _, _ in four], axis=0)
            ks = jnp.concatenate([k_ref[p] for p, _, _, _ in four], axis=0)
            vs = jnp.concatenate([v_ref[p] for p, _, _, _ in four], axis=0)
            scores = lax.dot_general(qs, ks, NT, preferred_element_type=F32) * scale
            peaks, masses, weights = [], [], []
            for e, (_, _, tokens, _) in enumerate(four):
                valid = token_of[e] < tokens
                sc = jnp.where(valid, scores[16 * e:16 * e + 16], LOW)
                peak = jnp.max(sc, axis=1, keepdims=True)
                w = jnp.where(valid, jnp.exp(sc - peak), 0.0)
                peaks.append(peak)
                masses.append(jnp.sum(w, axis=1, keepdims=True))
                weights.append(w)
            weights = jnp.concatenate(weights, axis=0).astype(BF16)
            out = jnp.dot(weights, vs, preferred_element_type=F32)
            for e in range(4):
                results.append((peaks[e], masses[e], out[16 * e:16 * e + 16]))
        for (_, r, _, first), (peak, mass, out) in zip(entries, results):
            d = r >> 5
            row = r & 31
            fresh = first == 1
            old_m = jnp.where(fresh, LOW, m_ref[r])
            old_l = jnp.where(fresh, 0.0, l_ref[r])
            peak = jnp.broadcast_to(peak, (16, 128))
            new_m = jnp.maximum(old_m, peak)
            f_old = jnp.exp(old_m - new_m)
            f_new = jnp.exp(peak - new_m)
            new_l = old_l * f_old + mass * f_new
            m_ref[r] = new_m
            l_ref[r] = new_l
            pick = (lane == row) | (lane == row + 32)
            for hh in range(2):
                part = slice(8 * hh, 8 * hh + 8)
                acc_ref[hh, d, row] = acc_ref[hh, d, row] * f_old[part] + out[part] * f_new[part]
                both = jnp.where(lane < 32, new_m[part], new_l[part])
                pltpu.store(acc_ref.at[hh, d, 32], both, mask=pick)
        return carry

    lax.fori_loop(0, (count_ref[0, 0] + 15) // 16, step, 0)


def attend_pages(words, count, all_queries, keys, values):
    req, heads, dim = all_queries.shape
    pool = keys.shape[0]
    return pl.pallas_call(
        functools.partial(pages_kernel, dim ** (-0.5)),
        out_shape=jax.ShapeDtypeStruct((2, req // 32 + 1, 33, 8, 128), F32),
        in_specs=[SMEM, SMEM, VMEM, ANY, ANY],
        out_specs=VMEM,
        scratch_shapes=[
            pltpu.VMEM(keys.shape, BF16),
            pltpu.VMEM(keys.shape, BF16),
            pltpu.VMEM((req + 1, heads, dim), F32),
            pltpu.VMEM((req + 1, heads, dim), F32),
            pltpu.SemaphoreType.DMA((2, 8)),
        ],
        compiler_params=pltpu.CompilerParams(vmem_limit_bytes=62 << 20),
        name="attend_pages",
    )(words, count, all_queries, keys, values)


def merge(dst, other):
    lane = lax.broadcasted_iota(jnp.int32, (8, 128), 1)
    t1, t2 = dst[32], other[32]
    top = jnp.maximum(t1, t2)
    f1 = jnp.exp(t1 - top)
    f2 = jnp.exp(t2 - top)
    mass = t1 * pltpu.roll(f1, 32, 1) + t2 * pltpu.roll(f2, 32, 1)
    for row in range(32):
        dst[row] = dst[row] * f1[:, row:row + 1] + other[row] * f2[:, row:row + 1]
    dst[32] = jnp.where(lane < 32, top, mass)


def finish_kernel(part_hbm, w_ref, att_ref, proj_ref, unit, pair, far1, near1, next1, far2, near2, next2,
                  tmp, own, full, cols, farx, nearx, nextx,
                  lsem, s0, r0, s1, r1, s2, r2, ssem, rsem, dsend, drecv, sx, rx):
    z, y, c, s = place()
    x = lax.axis_index("mp")
    home = plane_id(z, y, c)
    greet([plane_id(wrap(z + 1), y, c), plane_id(wrap(z - 1), y, c), plane_id(z, wrap(y + 1), c),
           plane_id(z, wrap(y - 1), c), plane_id(z, y, 1 - c), {"mp": wrap(x + 1)}, {"mp": wrap(x - 1)}])

    def spot(hh, oa, ob):
        dz = oa + hh * (ob - oa)
        dy = ob + hh * (oa - ob)
        return wrap(z + dz), wrap(y + dy)

    def step_of(n):
        m = n % 3
        return 2 * ((3 - n) // 3) + s * (m * (5 - 3 * m) // 2)

    def load(hh, zt, yt):
        return pltpu.make_async_copy(part_hbm.at[hh, (zt * 4 + yt) * 2 + c], unit.at[hh, zt, yt], lsem.at[hh, zt, yt])

    def swap(hh, zt, yt):
        return remote(part_hbm.at[hh, (zt * 4 + yt) * 2 + 1 - c], pair.at[hh, zt, yt], s0.at[hh, zt, yt],
                      r0.at[hh, zt, yt], plane_id(z, y, 1 - c))

    def hop(hh, sign):
        zt, yt = spot(hh, sign * s, 0)
        return plane_id(zt, yt, c)

    def hop2(hh, sign):
        zt, yt = spot(hh, 0, sign * s)
        return plane_id(zt, yt, c)

    order = (0, 2, 1, 3)

    for oa in order:
        def begin(k, carry, oa=oa):
            hh, ob = k % 2, k // 2
            zt, yt = spot(hh, step_of(oa), step_of(ob))
            load(hh, zt, yt).start()
            swap(hh, zt, yt).start()
            return carry
        lax.fori_loop(0, 8, begin, 0)

    def send1(kind, hh, ob, zt, yt):
        dst = (far1, near1, next1)[kind].at[hh, ob]
        return remote(unit.at[hh, zt, yt], dst, s1.at[kind, hh, ob], r1.at[kind, hh, ob], hop(hh, 1 if kind < 2 else -1))

    def both_cores(hh, zt, yt):
        load(hh, zt, yt).wait()
        swap(hh, zt, yt).wait_recv()
        merge(unit.at[hh, zt, yt], pair.at[hh, zt, yt])

    def far_units(k, carry):
        hh, ob = k % 2, k // 2
        zt, yt = spot(hh, 2, step_of(ob))
        both_cores(hh, zt, yt)
        send1(0, hh, ob, zt, yt).start()
        return carry

    def next_units(k, carry):
        hh, ob = k % 2, k // 2
        zt, yt = spot(hh, -s, step_of(ob))
        both_cores(hh, zt, yt)
        send1(2, hh, ob, zt, yt).start()
        return carry

    def near_units(k, carry):
        hh, ob = k % 2, k // 2
        zt, yt = spot(hh, s, step_of(ob))
        both_cores(hh, zt, yt)
        send1(0, hh, ob, zt, yt).wait_recv()
        merge(unit.at[hh, zt, yt], far1.at[hh, ob])
        send1(1, hh, ob, zt, yt).start()
        return carry

    def own_units(k, carry):
        hh, ob = k % 2, k // 2
        zt, yt = spot(hh, 0, step_of(ob))
        both_cores(hh, zt, yt)
        return carry

    lax.fori_loop(0, 8, far_units, 0)
    lax.fori_loop(0, 8, next_units, 0)
    lax.fori_loop(0, 8, near_units, 0)
    lax.fori_loop(0, 8, own_units, 0)

    def send2(kind, hh, zt, yt):
        dst = (far2, near2, next2)[kind].at[hh]
        return remote(unit.at[hh, zt, yt], dst, s2.at[kind, hh], r2.at[kind, hh], hop2(hh, 1 if kind < 2 else -1))

    def gathered(hh, ob):
        zt, yt = spot(hh, 0, step_of(ob))
        send1(2, hh, ob, zt, yt).wait_recv()
        merge(unit.at[hh, zt, yt], next1.at[hh, ob])
        send1(1, hh, ob, zt, yt).wait_recv()
        merge(unit.at[hh, zt, yt], near1.at[hh, ob])
        return zt, yt

    def far_blocks(hh, carry):
        zt, yt = gathered(hh, 0)
        send2(0, hh, zt, yt).start()
        return carry

    def next_blocks(hh, carry):
        zt, yt = gathered(hh, 2)
        send2(2, hh, zt, yt).start()
        return carry

    def near_blocks(hh, carry):
        zt, yt = gathered(hh, 1)
        send2(0, hh, zt, yt).wait_recv()
        merge(unit.at[hh, zt, yt], far2.at[hh])
        send2(1, hh, zt, yt).start()
        return carry

    def own_blocks(hh, carry):
        zt, yt = gathered(hh, 3)
        send2(2, hh, zt, yt).wait_recv()
        merge(unit.at[hh, zt, yt], next2.at[hh])
        send2(1, hh, zt, yt).wait_recv()
        merge(unit.at[hh, zt, yt], near2.at[hh])
        return carry

    for phase in (far_blocks, next_blocks, near_blocks, own_blocks):
        lax.fori_loop(0, 2, phase, 0)

    masses = [unit[hh, z, y, 32] for hh in range(2)]
    for row in range(32):
        both = [unit[hh, z, y, row] / masses[hh][:, 32 + row:33 + row] for hh in range(2)]
        for hh in range(2):
            tmp[hh, row] = both[hh]
        att_ref[row] = jnp.concatenate(both, axis=0).astype(BF16)
    for hh in range(2):
        for head in range(8):
            own[hh, head] = tmp[hh, :, head, :].astype(BF16)
    for hh in range(2):
        full[z, y, c, hh] = own[hh]

    sent = plane_gather(own, full, ssem, rsem, dsend, drecv)

    def project(step):
        t = wrap(x + step)
        rows = [full[t, :, :, hh, head].reshape(256, 128) for hh in range(2) for head in range(8)]
        cols[t] = jnp.dot(jnp.concatenate(rows, axis=1), w_ref[...], preferred_element_type=F32)
        return t

    def sendx(kind, t):
        return remote(cols.at[t], (farx, nearx, nextx)[kind], sx.at[kind], rx.at[kind],
                      {"mp": wrap(x + (s if kind < 2 else -s))})

    t = project(2)
    sendx(0, t).start()
    t = project(-s)
    sendx(2, t).start()
    t = project(s)
    sendx(0, t).wait_recv()
    cols[t] = cols[t] + farx[...]
    sendx(1, t).start()
    t = project(0)
    sendx(2, t).wait_recv()
    total = cols[t] + nextx[...]
    sendx(1, t).wait_recv()
    proj_ref[...] = (total + nearx[...]).astype(BF16)

    for kind in range(3):
        sendx(kind, t).wait_send()
    for copy in sent:
        copy.wait_send()

    def drain(k, carry):
        hh, ob = k % 2, k // 2
        for oa in range(4):
            zt, yt = spot(hh, step_of(oa), step_of(ob))
            swap(hh, zt, yt).wait_send()
        for kind in range(3):
            send1(kind, hh, ob, z, y).wait_send()
        return carry

    lax.fori_loop(0, 8, drain, 0)

    def drain2(hh, carry):
        for kind in range(3):
            send2(kind, hh, z, y).wait_send()
        return carry

    lax.fori_loop(0, 2, drain2, 0)


def finish(parts, weight, rows):
    unit = (33, 8, 128)
    dma = pltpu.SemaphoreType.DMA
    return pl.pallas_call(
        finish_kernel,
        out_shape=(
            jax.ShapeDtypeStruct((rows, 16, 128), BF16),
            jax.ShapeDtypeStruct((256, weight.shape[1]), BF16),
        ),
        in_specs=[ANY, VMEM],
        out_specs=(VMEM, VMEM),
        scratch_shapes=[
            pltpu.VMEM((2, 4, 4) + unit, F32),
            pltpu.VMEM((2, 4, 4) + unit, F32),
            pltpu.VMEM((2, 4) + unit, F32),
            pltpu.VMEM((2, 4) + unit, F32),
            pltpu.VMEM((2, 4) + unit, F32),
            pltpu.VMEM((2,) + unit, F32),
            pltpu.VMEM((2,) + unit, F32),
            pltpu.VMEM((2,) + unit, F32),
            pltpu.VMEM((2, 32, 8, 128), F32),
            pltpu.VMEM((2, 8, 32, 128), BF16),
            pltpu.VMEM((4, 4, 2, 2, 8, 32, 128), BF16),
            pltpu.VMEM((4, 256, 256), F32),
            pltpu.VMEM((256, 256), F32),
            pltpu.VMEM((256, 256), F32),
            pltpu.VMEM((256, 256), F32),
            dma((2, 4, 4)),
            dma((2, 4, 4)),
            dma((2, 4, 4)),
            dma((3, 2, 4)),
            dma((3, 2, 4)),
            dma((3, 2)),
            dma((3, 2)),
        ] + gather_sems() + [dma((3,)), dma((3,))],
        compiler_params=pltpu.CompilerParams(collective_id=1, has_side_effects=True, vmem_limit_bytes=48 << 20),
        name="finish",
    )(parts, weight)


def body(queries, lookup_sheets, content_sheets, page_table, context_len, out_weight):
    req = page_table.shape[0]
    pool, page_len, kv, dim = lookup_sheets.shape
    rows, heads, _ = queries.shape
    all_queries, words, count = gather_queries(
        queries, page_table.T, context_len.reshape(req // 128, 128), pool, page_len
    )
    parts = attend_pages(
        words,
        count,
        all_queries.reshape(req, heads, dim),
        lookup_sheets.reshape(pool, page_len * kv, dim),
        content_sheets.reshape(pool, page_len * kv, dim),
    )
    return finish(parts, out_weight, rows)


def solution(mesh):
    finer = Mesh(mesh.devices.reshape(4, 4, 2, mesh.shape["mp"]), ("dp_0", "dp_1", "dp_2", "mp"))
    return jax.shard_map(
        body,
        mesh=finer,
        in_specs=(
            P(DP, "mp", None),
            P(DP, None, "mp", None),
            P(DP, None, "mp", None),
            P(),
            P(),
            P("mp", DP),
        ),
        out_specs=(P(DP, "mp", None), P("mp", DP)),
        check_vma=False,
    )
```

```python
import functools

import jax
import jax.numpy as jnp
from jax import lax
from jax.experimental import pallas as pl
from jax.experimental.pallas import tpu as pltpu
from jax.sharding import Mesh
from jax.sharding import PartitionSpec as P

DP = ("dp_0", "dp_1", "dp_2")
MESH = pl.DeviceIdType.MESH
LOW = -1e30
NOTHING = 1040
F32 = jnp.float32
BF16 = jnp.bfloat16
NT = (((1,), (1,)), ((), ()))
VMEM = pl.BlockSpec(memory_space=pltpu.VMEM)
HBM = pl.BlockSpec(memory_space=pltpu.HBM)
SMEM = pl.BlockSpec(memory_space=pltpu.SMEM)


def wrap(value):
    return lax.rem(value + 8, 4)


def place():
    z, y, c = (lax.axis_index(name) for name in DP)
    return z, y, c, 1 - 2 * c


def plane_id(z, y, c):
    return {"dp_0": z, "dp_1": y, "dp_2": c}


def greet(devices):
    barrier = pltpu.get_barrier_semaphore()
    for device in devices:
        pl.semaphore_signal(barrier, inc=1, device_id=device, device_id_type=MESH)
    pl.semaphore_wait(barrier, len(devices))


def remote(src, dst, send_sem, recv_sem, device):
    return pltpu.make_async_remote_copy(
        src_ref=src,
        dst_ref=dst,
        send_sem=send_sem,
        recv_sem=recv_sem,
        device_id=device,
        device_id_type=MESH,
    )


def plane_gather(own, full, ssem, rsem, dsend, drecv, between=()):
    z, y, c, s = place()
    work = list(between)

    def fill():
        if work:
            work.pop(0)()

    def at(h, a, b):
        return full.at[a, b, c, h] if h == 0 else full.at[b, a, c, h]

    def device(h, a, b):
        return plane_id(a, b, c) if h == 0 else plane_id(b, a, c)

    def mine(h):
        return (z, y) if h == 0 else (y, z)

    sent = []

    def go(h, group, m, src, dst, target):
        copy = remote(src, dst, ssem.at[h, group, m], rsem.at[h, group, m], target)
        copy.start()
        sent.append(copy)

    def come(h, group, m, dst):
        remote(dst, dst, ssem.at[h, group, m], rsem.at[h, group, m], plane_id(z, y, c)).wait_recv()

    def share(h, slot, src, dst):
        copy = remote(src, dst, dsend.at[h, slot], drecv.at[h, slot], plane_id(z, y, 1 - c))
        copy.start()
        sent.append(copy)

    def spread(h, group, slot, src, a, b):
        go(h, group, 0, src, at(h, a, b), device(h, mine(h)[0], wrap(b + s)))
        go(h, group, 1, src, at(h, a, b), device(h, mine(h)[0], wrap(b - s)))

    def first(h):
        a, b = mine(h)
        go(h, 0, 0, own.at[h], at(h, a, b), device(h, wrap(a + s), b))
        go(h, 0, 1, own.at[h], at(h, a, b), device(h, wrap(a - s), b))

    for h in range(2):
        first(h)
    for h in range(2):
        share(h, 0, own.at[h], at(h, *mine(h)))
        spread(h, 1, 0, own.at[h], *mine(h))
    fill()
    for h in range(2):
        a, b = mine(h)
        near = wrap(a - s)
        come(h, 0, 0, at(h, near, b))
        go(h, 0, 2, at(h, near, b), at(h, near, b), device(h, wrap(a + s), b))
        spread(h, 2, 4, at(h, near, b), near, b)
        share(h, 4, at(h, near, b), at(h, near, b))
    for h in range(2):
        a, b = mine(h)
        near = wrap(a + s)
        come(h, 0, 1, at(h, near, b))
        spread(h, 3, 8, at(h, near, b), near, b)
        share(h, 8, at(h, near, b), at(h, near, b))
    fill()
    for h in range(2):
        a, b = mine(h)
        far = wrap(a + 2)
        come(h, 0, 2, at(h, far, b))
        spread(h, 4, 12, at(h, far, b), far, b)
        share(h, 12, at(h, far, b), at(h, far, b))
    fill()
    for group, step in ((1, 0), (2, -1), (3, 1), (4, 2)):
        for h in range(2):
            a, b = mine(h)
            row = wrap(a + step * s)
            near = wrap(b - s)
            come(h, group, 0, at(h, row, near))
            go(h, group, 2, at(h, row, near), at(h, row, near), device(h, a, wrap(b + s)))
            share(h, 4 * (group - 1) + 1, at(h, row, near), at(h, row, near))
            other = wrap(b + s)
            come(h, group, 1, at(h, row, other))
            share(h, 4 * (group - 1) + 2, at(h, row, other), at(h, row, other))
        fill()
    for group, step in ((1, 0), (2, -1), (3, 1), (4, 2)):
        for h in range(2):
            a, b = mine(h)
            row = wrap(a + step * s)
            far = wrap(b + 2)
            come(h, group, 2, at(h, row, far))
            share(h, 4 * (group - 1) + 3, at(h, row, far), at(h, row, far))
    for h in range(2):
        for slot in range(16):
            where = full.at[0, 0, 1 - c, h]
            remote(where, where, dsend.at[h, slot], drecv.at[h, slot], plane_id(z, y, 1 - c)).wait_recv()
    return sent


def gather_sems():
    return [
        pltpu.SemaphoreType.DMA((2, 5, 3)),
        pltpu.SemaphoreType.DMA((2, 5, 3)),
        pltpu.SemaphoreType.DMA((2, 16)),
        pltpu.SemaphoreType.DMA((2, 16)),
    ]


def queries_kernel(pool_bits, page_len, q_hbm, table_hbm, len_hbm, full_ref, list_ref,
                   table_ref, len_ref, lo_ref, hi_ref, part_ref, total_ref, lsem, ssem, rsem, dsend, drecv):
    z, y, c, s = place()
    me = (z * 4 + y) * 2 + c
    loads = [
        pltpu.make_async_copy(src, dst, lsem.at[n])
        for n, (src, dst) in enumerate(
            ((q_hbm, full_ref.at[z, y, c]), (table_hbm, table_ref), (len_hbm, len_ref)))
    ]
    for load in loads:
        load.start()
    greet([plane_id(wrap(z + 1), y, c), plane_id(wrap(z - 1), y, c), plane_id(z, wrap(y + 1), c),
           plane_id(z, wrap(y - 1), c), plane_id(z, y, 1 - c)])
    loads[0].wait()

    def place_pages():
        for load in loads[1:]:
            load.wait()
        slots = table_ref.shape[0]
        slot = lax.broadcasted_iota(jnp.int32, (slots, 128), 0)
        lane = lax.broadcasted_iota(jnp.int32, (slots, 128), 1)
        blocks = table_ref.shape[1] // 128
        mine, tokens, page, owner = [], [], [], []
        for t in range(blocks):
            ids = table_ref[:, t * 128:(t + 1) * 128]
            length = jnp.broadcast_to(len_ref[t:t + 1, :], (slots, 128))
            left = jnp.clip(length - slot * page_len, 0, page_len)
            mine.append(jnp.where(((ids >> pool_bits) == me) & (left > 0), 1.0, 0.0))
            tokens.append(left)
            page.append(ids & ((1 << pool_bits) - 1))
            owner.append(lane + t * 128)
        mine, tokens, page, owner = (jnp.concatenate(v, axis=0) for v in (mine, tokens, page, owner))
        rows = slots * blocks
        mine_h = mine.astype(BF16)
        i = lax.broadcasted_iota(jnp.int32, (rows, rows), 0)
        j = lax.broadcasted_iota(jnp.int32, (rows, rows), 1)
        same = (i // slots) == (j // slots)

        def count(which, what):
            return jnp.dot(jnp.where(which, 1.0, 0.0).astype(BF16), what, preferred_element_type=F32)

        earlier = count(same & (j < i), mine_h)
        column = count(same, mine_h)
        blocks_before = count((j // slots) < (i // slots), mine_h)
        i = lax.broadcasted_iota(jnp.int32, (128, 128), 0)
        j = lax.broadcasted_iota(jnp.int32, (128, 128), 1)
        ahead = jnp.where(i < j, 1.0, 0.0).astype(BF16)
        every = jnp.ones((128, 128), BF16)
        start = jnp.dot(column.astype(BF16), ahead, preferred_element_type=F32)
        start = start + jnp.dot(blocks_before.astype(BF16), every, preferred_element_type=F32)
        rank = (start + earlier).astype(jnp.int32)
        lo_ref[...] = jnp.where(mine > 0.0, rank & 127, -1)
        hi_ref[...] = jnp.where(mine > 0.0, rank >> 7, -1)
        part_ref[0] = (page & 255).astype(F32)
        part_ref[1] = (owner & 255).astype(F32)
        part_ref[2] = ((page >> 8) + ((owner >> 8) << 2) + ((tokens - 1) << 4)).astype(F32)
        part_ref[3] = jnp.where(earlier > 0.0, 0.0, 1.0)
        last = jnp.where(column > 0.0, start + column - 1.0, float(NOTHING)).astype(jnp.int32)
        list_ref[8:16, :] = jnp.concatenate([last[t * slots:t * slots + 1] for t in range(blocks)], axis=0)
        number = (start + column)[rows - 1:rows, 127:128]
        list_ref[16:24, :] = jnp.broadcast_to(number, (8, 128)).astype(jnp.int32)
        total_ref[...] = jnp.zeros_like(total_ref)

    sub = lax.broadcasted_iota(jnp.int32, (128, 128), 0)
    sub8 = lax.broadcasted_iota(jnp.int32, (8, 128), 0)

    def scatter(part):
        def step(n, carry):
            base = pl.multiple_of(n * 8, 8)
            lo8 = lo_ref[pl.ds(base, 8), :]
            hi8 = hi_ref[pl.ds(base, 8), :]
            p8 = [part_ref[k, pl.ds(base, 8), :] for k in range(4)]
            wide, tall = [], []
            for r in range(8):
                wide.append(jnp.where(sub == lo8[r:r + 1, :], 1.0, 0.0).astype(BF16))
                hit = sub8 == hi8[r:r + 1, :]
                tall.append(jnp.concatenate(
                    [jnp.where(hit, p8[k][r:r + 1, :], 0.0) for k in range(4)], axis=0).astype(BF16))
            wide = jnp.concatenate(wide, axis=1)
            tall = jnp.concatenate(tall, axis=1)
            total_ref[...] += lax.dot_general(wide, tall, NT, preferred_element_type=F32)
            return carry

        steps = lo_ref.shape[0] // 32
        lax.fori_loop(part * steps, (part + 1) * steps, step, 0)

    def write_list():
        total = jnp.concatenate([total_ref[...], jnp.zeros((128, 96), F32)], axis=1).T.astype(jnp.int32)
        p0, p1, p2, p3 = (total[8 * k:8 * k + 8, :] for k in range(4))
        page = p0 + ((p2 & 3) << 8)
        owner = p1 + (((p2 >> 2) & 3) << 8)
        tokens = (p2 >> 4) + 1
        list_ref[0:8, :] = page + (owner << 10) + (tokens << 20) + (p3 << 25)

    pieces = [place_pages] + [functools.partial(scatter, n) for n in range(4)] + [write_list]
    for copy in plane_gather(full_ref.at[z, y, c], full_ref, ssem, rsem, dsend, drecv, between=pieces):
        copy.wait_send()


def gather_queries(queries, table, lengths, pool, page_len):
    req = table.shape[1]
    rows = table.shape[0] * req // 128
    mine, heads, dim = queries.shape
    half = mine // 2
    return pl.pallas_call(
        functools.partial(queries_kernel, pool.bit_length() - 1, page_len),
        out_shape=(
            jax.ShapeDtypeStruct((4, 4, 2, 2, half, heads, dim), BF16),
            jax.ShapeDtypeStruct((24, 128), jnp.int32),
        ),
        in_specs=[HBM] * 3,
        out_specs=(VMEM, VMEM),
        scratch_shapes=[
            pltpu.VMEM(table.shape, jnp.int32),
            pltpu.VMEM(lengths.shape, jnp.int32),
            pltpu.VMEM((rows, 128), jnp.int32),
            pltpu.VMEM((rows, 128), jnp.int32),
            pltpu.VMEM((4, rows, 128), F32),
            pltpu.VMEM((128, 32), F32),
            pltpu.SemaphoreType.DMA((3,)),
        ] + gather_sems(),
        compiler_params=pltpu.CompilerParams(collective_id=0, has_side_effects=True, vmem_limit_bytes=8 << 20),
        cost_estimate=pl.CostEstimate(flops=10**10, bytes_accessed=1 << 23, transcendentals=0),
        name="gather_queries",
    )(queries.reshape(2, half, heads, dim), table, lengths)


def pages_kernel(scale, list_ref, q_ref, k_ref, v_ref, acc_ref, sum_ref, top_ref):
    lane = lax.broadcasted_iota(jnp.int32, (16, 128), 1)
    blank = jnp.where(lane < 32, LOW, 0.0)
    sum_ref[NOTHING] = jnp.zeros((16, 128), F32)
    top_ref[NOTHING] = blank

    i = lax.broadcasted_iota(jnp.int32, (16, 128), 0)
    kv_match = (i // 8) == (lane % 2)
    token = (lane % 32) // 2
    token_of = [jnp.where(kv_match & (lane // 32 == n), token, 1 << 20) for n in range(4)]

    def step(n, carry):
        base = n * 16
        entries = []
        for e in range(16):
            word = list_ref[(base + e) >> 7, (base + e) & 127]
            entries.append((word & 1023, (word >> 10) & 1023, (word >> 20) & 31, (word >> 25) & 1))
        results = []
        for g in range(4):
            four = entries[4 * g:4 * g + 4]
            qs = jnp.concatenate([q_ref[r] for _, r, _, _ in four], axis=0)
            ks = jnp.concatenate([k_ref[p] for p, _, _, _ in four], axis=0)
            vs = jnp.concatenate([v_ref[p] for p, _, _, _ in four], axis=0)
            scores = lax.dot_general(qs, ks, NT, preferred_element_type=F32) * scale
            peaks, masses, weights = [], [], []
            for e, (_, _, tokens, _) in enumerate(four):
                valid = token_of[e] < tokens
                sc = jnp.where(valid, scores[16 * e:16 * e + 16], LOW)
                peak = jnp.max(sc, axis=1, keepdims=True)
                w = jnp.where(valid, jnp.exp(sc - peak), 0.0)
                peaks.append(peak)
                masses.append(jnp.sum(w, axis=1, keepdims=True))
                weights.append(w)
            weights = jnp.concatenate(weights, axis=0).astype(BF16)
            out = jnp.dot(weights, vs, preferred_element_type=F32)
            for e in range(4):
                results.append((peaks[e], masses[e], out[16 * e:16 * e + 16]))
        top, mass, acc = carry
        for e, ((_, _, _, first), (p, m, out)) in enumerate(zip(entries, results)):
            old = jnp.where(first == 1, LOW, top)
            p = jnp.broadcast_to(p, (16, 128))
            top = jnp.maximum(old, p)
            f_old = jnp.exp(old - top)
            f_new = jnp.exp(p - top)
            mass = mass * f_old + m * f_new
            acc = acc * f_old + out * f_new
            sum_ref[base + e] = acc
            top_ref[base + e] = jnp.where(lane < 32, top, mass)
        return top, mass, acc

    zero = jnp.zeros((16, 128), F32)
    lax.fori_loop(0, (list_ref[16, 0] + 15) // 16, step, (zero, zero, zero))

    def spread(d, carry):
        tops = blank
        for row in range(32):
            r = d * 32 + row
            last = list_ref[8 + (r >> 7), r & 127]
            acc = sum_ref[last]
            tops = jnp.where((lane == row) | (lane == row + 32), top_ref[last], tops)
            for hh in range(2):
                acc_ref[hh, d, row] = acc[8 * hh:8 * hh + 8]
        for hh in range(2):
            acc_ref[hh, d, 32] = tops[8 * hh:8 * hh + 8]
        return carry

    lax.fori_loop(0, acc_ref.shape[1], spread, 0)


def attend_pages(words, all_queries, keys, values):
    req, heads, dim = all_queries.shape
    return pl.pallas_call(
        functools.partial(pages_kernel, dim ** (-0.5)),
        out_shape=jax.ShapeDtypeStruct((2, req // 32, 33, 8, 128), F32),
        in_specs=[SMEM, VMEM, VMEM, VMEM],
        out_specs=VMEM,
        scratch_shapes=[
            pltpu.VMEM((NOTHING + 1, heads, dim), F32),
            pltpu.VMEM((NOTHING + 1, heads, dim), F32),
        ],
        compiler_params=pltpu.CompilerParams(vmem_limit_bytes=20 << 20),
        name="attend_pages",
    )(words, all_queries, keys, values)


def merge(dst, one, other):
    lane = lax.broadcasted_iota(jnp.int32, (8, 128), 1)
    t1, t2 = one[32], other[32]
    top = jnp.maximum(t1, t2)
    f1 = jnp.exp(t1 - top)
    f2 = jnp.exp(t2 - top)
    mass = t1 * pltpu.roll(f1, 32, 1) + t2 * pltpu.roll(f2, 32, 1)
    for row in range(32):
        dst[row] = one[row] * f1[:, row:row + 1] + other[row] * f2[:, row:row + 1]
    dst[32] = jnp.where(lane < 32, top, mass)


def finish_kernel(part_ref, w_ref, att_ref, proj_ref, unit, pair, far1, near1, next1, far2, near2, next2,
                  tmp, own, full, cols, farx, nearx, nextx,
                  s0, r0, s1, r1, s2, r2, ssem, rsem, dsend, drecv, sx, rx):
    z, y, c, s = place()
    x = lax.axis_index("mp")
    home = plane_id(z, y, c)
    greet([plane_id(wrap(z + 1), y, c), plane_id(wrap(z - 1), y, c), plane_id(z, wrap(y + 1), c),
           plane_id(z, wrap(y - 1), c), plane_id(z, y, 1 - c), {"mp": wrap(x + 1)}, {"mp": wrap(x - 1)}])

    def spot(hh, oa, ob):
        dz = oa + hh * (ob - oa)
        dy = ob + hh * (oa - ob)
        return wrap(z + dz), wrap(y + dy)

    def step_of(n):
        m = n % 3
        return 2 * ((3 - n) // 3) + s * (m * (5 - 3 * m) // 2)

    def swap(hh, zt, yt):
        return remote(part_ref.at[hh, (zt * 4 + yt) * 2 + 1 - c], pair.at[hh, zt, yt], s0.at[hh, zt, yt],
                      r0.at[hh, zt, yt], plane_id(z, y, 1 - c))

    def hop(hh, sign):
        zt, yt = spot(hh, sign * s, 0)
        return plane_id(zt, yt, c)

    def hop2(hh, sign):
        zt, yt = spot(hh, 0, sign * s)
        return plane_id(zt, yt, c)

    order = (0, 2, 1, 3)

    for oa in order:
        def begin(k, carry, oa=oa):
            hh, ob = k % 2, k // 2
            zt, yt = spot(hh, step_of(oa), step_of(ob))
            swap(hh, zt, yt).start()
            return carry
        lax.fori_loop(0, 8, begin, 0)

    def send1(kind, hh, ob, zt, yt):
        dst = (far1, near1, next1)[kind].at[hh, ob]
        return remote(unit.at[hh, zt, yt], dst, s1.at[kind, hh, ob], r1.at[kind, hh, ob], hop(hh, 1 if kind < 2 else -1))

    def both_cores(hh, zt, yt):
        swap(hh, zt, yt).wait_recv()
        merge(unit.at[hh, zt, yt], part_ref.at[hh, (zt * 4 + yt) * 2 + c], pair.at[hh, zt, yt])

    def far_units(k, carry):
        hh, ob = k % 2, k // 2
        zt, yt = spot(hh, 2, step_of(ob))
        both_cores(hh, zt, yt)
        send1(0, hh, ob, zt, yt).start()
        return carry

    def next_units(k, carry):
        hh, ob = k % 2, k // 2
        zt, yt = spot(hh, -s, step_of(ob))
        both_cores(hh, zt, yt)
        send1(2, hh, ob, zt, yt).start()
        return carry

    def near_units(k, carry):
        hh, ob = k % 2, k // 2
        zt, yt = spot(hh, s, step_of(ob))
        both_cores(hh, zt, yt)
        send1(0, hh, ob, zt, yt).wait_recv()
        merge(unit.at[hh, zt, yt], unit.at[hh, zt, yt], far1.at[hh, ob])
        send1(1, hh, ob, zt, yt).start()
        return carry

    def own_units(k, carry):
        hh, ob = k % 2, k // 2
        zt, yt = spot(hh, 0, step_of(ob))
        both_cores(hh, zt, yt)
        return carry

    lax.fori_loop(0, 8, far_units, 0)
    lax.fori_loop(0, 8, next_units, 0)
    lax.fori_loop(0, 8, near_units, 0)
    lax.fori_loop(0, 8, own_units, 0)

    def send2(kind, hh, zt, yt):
        dst = (far2, near2, next2)[kind].at[hh]
        return remote(unit.at[hh, zt, yt], dst, s2.at[kind, hh], r2.at[kind, hh], hop2(hh, 1 if kind < 2 else -1))

    def gathered(hh, ob):
        zt, yt = spot(hh, 0, step_of(ob))
        send1(2, hh, ob, zt, yt).wait_recv()
        merge(unit.at[hh, zt, yt], unit.at[hh, zt, yt], next1.at[hh, ob])
        send1(1, hh, ob, zt, yt).wait_recv()
        merge(unit.at[hh, zt, yt], unit.at[hh, zt, yt], near1.at[hh, ob])
        return zt, yt

    def far_blocks(hh, carry):
        zt, yt = gathered(hh, 0)
        send2(0, hh, zt, yt).start()
        return carry

    def next_blocks(hh, carry):
        zt, yt = gathered(hh, 2)
        send2(2, hh, zt, yt).start()
        return carry

    def near_blocks(hh, carry):
        zt, yt = gathered(hh, 1)
        send2(0, hh, zt, yt).wait_recv()
        merge(unit.at[hh, zt, yt], unit.at[hh, zt, yt], far2.at[hh])
        send2(1, hh, zt, yt).start()
        return carry

    def own_blocks(hh, carry):
        zt, yt = gathered(hh, 3)
        send2(2, hh, zt, yt).wait_recv()
        merge(unit.at[hh, zt, yt], unit.at[hh, zt, yt], next2.at[hh])
        send2(1, hh, zt, yt).wait_recv()
        merge(unit.at[hh, zt, yt], unit.at[hh, zt, yt], near2.at[hh])
        return carry

    for phase in (far_blocks, next_blocks, near_blocks, own_blocks):
        lax.fori_loop(0, 2, phase, 0)

    masses = [unit[hh, z, y, 32] for hh in range(2)]
    for row in range(32):
        both = [unit[hh, z, y, row] / masses[hh][:, 32 + row:33 + row] for hh in range(2)]
        for hh in range(2):
            tmp[hh, row] = both[hh]
        att_ref[row] = jnp.concatenate(both, axis=0).astype(BF16)
    for hh in range(2):
        for head in range(8):
            own[hh, head] = tmp[hh, :, head, :].astype(BF16)
    for hh in range(2):
        full[z, y, c, hh] = own[hh]

    sent = plane_gather(own, full, ssem, rsem, dsend, drecv)

    def project(step):
        t = wrap(x + step)
        rows = [full[t, :, :, hh, head].reshape(256, 128) for hh in range(2) for head in range(8)]
        cols[t] = jnp.dot(jnp.concatenate(rows, axis=1), w_ref[...], preferred_element_type=F32)
        return t

    def sendx(kind, t):
        return remote(cols.at[t], (farx, nearx, nextx)[kind], sx.at[kind], rx.at[kind],
                      {"mp": wrap(x + (s if kind < 2 else -s))})

    t = project(2)
    sendx(0, t).start()
    t = project(-s)
    sendx(2, t).start()
    t = project(s)
    sendx(0, t).wait_recv()
    cols[t] = cols[t] + farx[...]
    sendx(1, t).start()
    t = project(0)
    sendx(2, t).wait_recv()
    total = cols[t] + nextx[...]
    sendx(1, t).wait_recv()
    proj_ref[...] = (total + nearx[...]).astype(BF16)

    for kind in range(3):
        sendx(kind, t).wait_send()
    for copy in sent:
        copy.wait_send()

    def drain(k, carry):
        hh, ob = k % 2, k // 2
        for oa in range(4):
            zt, yt = spot(hh, step_of(oa), step_of(ob))
            swap(hh, zt, yt).wait_send()
        for kind in range(3):
            send1(kind, hh, ob, z, y).wait_send()
        return carry

    lax.fori_loop(0, 8, drain, 0)

    def drain2(hh, carry):
        for kind in range(3):
            send2(kind, hh, z, y).wait_send()
        return carry

    lax.fori_loop(0, 2, drain2, 0)


def finish(parts, weight, rows):
    unit = (33, 8, 128)
    dma = pltpu.SemaphoreType.DMA
    return pl.pallas_call(
        finish_kernel,
        out_shape=(
            jax.ShapeDtypeStruct((rows, 16, 128), BF16),
            jax.ShapeDtypeStruct((256, weight.shape[1]), BF16),
        ),
        in_specs=[VMEM, VMEM],
        out_specs=(VMEM, VMEM),
        scratch_shapes=[
            pltpu.VMEM((2, 4, 4) + unit, F32),
            pltpu.VMEM((2, 4, 4) + unit, F32),
            pltpu.VMEM((2, 4) + unit, F32),
            pltpu.VMEM((2, 4) + unit, F32),
            pltpu.VMEM((2, 4) + unit, F32),
            pltpu.VMEM((2,) + unit, F32),
            pltpu.VMEM((2,) + unit, F32),
            pltpu.VMEM((2,) + unit, F32),
            pltpu.VMEM((2, 32, 8, 128), F32),
            pltpu.VMEM((2, 8, 32, 128), BF16),
            pltpu.VMEM((4, 4, 2, 2, 8, 32, 128), BF16),
            pltpu.VMEM((4, 256, 256), F32),
            pltpu.VMEM((256, 256), F32),
            pltpu.VMEM((256, 256), F32),
            pltpu.VMEM((256, 256), F32),
            dma((2, 4, 4)),
            dma((2, 4, 4)),
            dma((3, 2, 4)),
            dma((3, 2, 4)),
            dma((3, 2)),
            dma((3, 2)),
        ] + gather_sems() + [dma((3,)), dma((3,))],
        compiler_params=pltpu.CompilerParams(collective_id=1, has_side_effects=True, vmem_limit_bytes=24 << 20),
        name="finish",
    )(parts, weight)


def body(queries, lookup_sheets, content_sheets, page_table, context_len, out_weight):
    req = page_table.shape[0]
    pool, page_len, kv, dim = lookup_sheets.shape
    rows, heads, _ = queries.shape
    all_queries, words = gather_queries(
        queries, page_table.T, context_len.reshape(req // 128, 128), pool, page_len
    )
    parts = attend_pages(
        words,
        all_queries.reshape(req, heads, dim),
        lookup_sheets.reshape(pool, page_len * kv, dim),
        content_sheets.reshape(pool, page_len * kv, dim),
    )
    return finish(parts, out_weight, rows)


def solution(mesh):
    finer = Mesh(mesh.devices.reshape(4, 4, 2, mesh.shape["mp"]), ("dp_0", "dp_1", "dp_2", "mp"))
    return jax.shard_map(
        body,
        mesh=finer,
        in_specs=(
            P(DP, "mp", None),
            P(DP, None, "mp", None),
            P(DP, None, "mp", None),
            P(),
            P(),
            P("mp", DP),
        ),
        out_specs=(P(DP, "mp", None), P("mp", DP)),
        check_vma=False,
    )
```

```python
import functools

import jax
import jax.numpy as jnp
from jax import lax
from jax.experimental import pallas as pl
from jax.experimental.pallas import tpu as pltpu
from jax.sharding import Mesh
from jax.sharding import PartitionSpec as P

DP = ("dp_0", "dp_1", "dp_2")
MESH = pl.DeviceIdType.MESH
LOW = -1e30
BATCH = 32
NOTHING = 1056
F32 = jnp.float32
BF16 = jnp.bfloat16
NT = (((1,), (1,)), ((), ()))
VMEM = pl.BlockSpec(memory_space=pltpu.VMEM)
HBM = pl.BlockSpec(memory_space=pltpu.HBM)
SMEM = pl.BlockSpec(memory_space=pltpu.SMEM)


def wrap(value):
    return lax.rem(value + 8, 4)


def place():
    z, y, c = (lax.axis_index(name) for name in DP)
    return z, y, c, 1 - 2 * c


def plane_id(z, y, c):
    return {"dp_0": z, "dp_1": y, "dp_2": c}


def greet(devices):
    barrier = pltpu.get_barrier_semaphore()
    for device in devices:
        pl.semaphore_signal(barrier, inc=1, device_id=device, device_id_type=MESH)
    pl.semaphore_wait(barrier, len(devices))


def remote(src, dst, send_sem, recv_sem, device):
    return pltpu.make_async_remote_copy(
        src_ref=src,
        dst_ref=dst,
        send_sem=send_sem,
        recv_sem=recv_sem,
        device_id=device,
        device_id_type=MESH,
    )


def plane_gather(own, full, ssem, rsem, dsend, drecv, between=()):
    z, y, c, s = place()
    work = list(between)

    def fill():
        if work:
            work.pop(0)()

    def at(h, a, b):
        return full.at[a, b, c, h] if h == 0 else full.at[b, a, c, h]

    def device(h, a, b):
        return plane_id(a, b, c) if h == 0 else plane_id(b, a, c)

    def mine(h):
        return (z, y) if h == 0 else (y, z)

    sent = []

    def go(h, group, m, src, dst, target):
        copy = remote(src, dst, ssem.at[h, group, m], rsem.at[h, group, m], target)
        copy.start()
        sent.append(copy)

    def come(h, group, m, dst):
        remote(dst, dst, ssem.at[h, group, m], rsem.at[h, group, m], plane_id(z, y, c)).wait_recv()

    def share(h, slot, src, dst):
        copy = remote(src, dst, dsend.at[h, slot], drecv.at[h, slot], plane_id(z, y, 1 - c))
        copy.start()
        sent.append(copy)

    def spread(h, group, slot, src, a, b):
        go(h, group, 0, src, at(h, a, b), device(h, mine(h)[0], wrap(b + s)))
        go(h, group, 1, src, at(h, a, b), device(h, mine(h)[0], wrap(b - s)))

    def first(h):
        a, b = mine(h)
        go(h, 0, 0, own.at[h], at(h, a, b), device(h, wrap(a + s), b))
        go(h, 0, 1, own.at[h], at(h, a, b), device(h, wrap(a - s), b))
        go(h, 0, 2, own.at[h], at(h, a, b), device(h, wrap(a + 2), b))

    for h in range(2):
        first(h)
    for h in range(2):
        share(h, 0, own.at[h], at(h, *mine(h)))
        spread(h, 1, 0, own.at[h], *mine(h))
    fill()
    for h in range(2):
        a, b = mine(h)
        near = wrap(a - s)
        come(h, 0, 0, at(h, near, b))
        spread(h, 2, 4, at(h, near, b), near, b)
        share(h, 4, at(h, near, b), at(h, near, b))
    for h in range(2):
        a, b = mine(h)
        near = wrap(a + s)
        come(h, 0, 1, at(h, near, b))
        spread(h, 3, 8, at(h, near, b), near, b)
        share(h, 8, at(h, near, b), at(h, near, b))
    fill()
    for h in range(2):
        a, b = mine(h)
        far = wrap(a + 2)
        come(h, 0, 2, at(h, far, b))
        spread(h, 4, 12, at(h, far, b), far, b)
        share(h, 12, at(h, far, b), at(h, far, b))
    fill()
    for group, step in ((1, 0), (2, -1), (3, 1), (4, 2)):
        for h in range(2):
            a, b = mine(h)
            row = wrap(a + step * s)
            near = wrap(b - s)
            come(h, group, 0, at(h, row, near))
            go(h, group, 2, at(h, row, near), at(h, row, near), device(h, a, wrap(b + s)))
            share(h, 4 * (group - 1) + 1, at(h, row, near), at(h, row, near))
            other = wrap(b + s)
            come(h, group, 1, at(h, row, other))
            share(h, 4 * (group - 1) + 2, at(h, row, other), at(h, row, other))
        fill()
    for group, step in ((1, 0), (2, -1), (3, 1), (4, 2)):
        for h in range(2):
            a, b = mine(h)
            row = wrap(a + step * s)
            far = wrap(b + 2)
            come(h, group, 2, at(h, row, far))
            share(h, 4 * (group - 1) + 3, at(h, row, far), at(h, row, far))
    for h in range(2):
        for slot in range(16):
            where = full.at[0, 0, 1 - c, h]
            remote(where, where, dsend.at[h, slot], drecv.at[h, slot], plane_id(z, y, 1 - c)).wait_recv()
    return sent


def gather_sems():
    return [
        pltpu.SemaphoreType.DMA((2, 5, 3)),
        pltpu.SemaphoreType.DMA((2, 5, 3)),
        pltpu.SemaphoreType.DMA((2, 16)),
        pltpu.SemaphoreType.DMA((2, 16)),
    ]


def queries_kernel(pool_bits, page_len, q_hbm, table_hbm, len_hbm, full_ref, list_ref,
                   table_ref, len_ref, lo_ref, hi_ref, part_ref, total_ref, lsem, ssem, rsem, dsend, drecv):
    z, y, c, s = place()
    me = (z * 4 + y) * 2 + c
    loads = [
        pltpu.make_async_copy(src, dst, lsem.at[n])
        for n, (src, dst) in enumerate(
            ((q_hbm, full_ref.at[z, y, c]), (table_hbm, table_ref), (len_hbm, len_ref)))
    ]
    for load in loads:
        load.start()
    greet([plane_id(wrap(z + 1), y, c), plane_id(wrap(z - 1), y, c), plane_id(z, wrap(y + 1), c),
           plane_id(z, wrap(y - 1), c), plane_id(wrap(z + 2), y, c), plane_id(z, wrap(y + 2), c), plane_id(z, y, 1 - c)])
    loads[0].wait()

    def place_pages():
        for load in loads[1:]:
            load.wait()
        slots = table_ref.shape[0]
        slot = lax.broadcasted_iota(jnp.int32, (slots, 128), 0)
        lane = lax.broadcasted_iota(jnp.int32, (slots, 128), 1)
        blocks = table_ref.shape[1] // 128
        mine, tokens, page, owner = [], [], [], []
        for t in range(blocks):
            ids = table_ref[:, t * 128:(t + 1) * 128]
            length = jnp.broadcast_to(len_ref[t:t + 1, :], (slots, 128))
            left = jnp.clip(length - slot * page_len, 0, page_len)
            mine.append(jnp.where(((ids >> pool_bits) == me) & (left > 0), 1.0, 0.0))
            tokens.append(left)
            page.append(ids & ((1 << pool_bits) - 1))
            owner.append(lane + t * 128)
        mine, tokens, page, owner = (jnp.concatenate(v, axis=0) for v in (mine, tokens, page, owner))
        rows = slots * blocks
        mine_h = mine.astype(BF16)
        i = lax.broadcasted_iota(jnp.int32, (rows, rows), 0)
        j = lax.broadcasted_iota(jnp.int32, (rows, rows), 1)
        same = (i // slots) == (j // slots)

        def count(which, what):
            return jnp.dot(jnp.where(which, 1.0, 0.0).astype(BF16), what, preferred_element_type=F32)

        earlier = count(same & (j < i), mine_h)
        column = count(same, mine_h)
        blocks_before = count((j // slots) < (i // slots), mine_h)
        i = lax.broadcasted_iota(jnp.int32, (128, 128), 0)
        j = lax.broadcasted_iota(jnp.int32, (128, 128), 1)
        ahead = jnp.where(i < j, 1.0, 0.0).astype(BF16)
        every = jnp.ones((128, 128), BF16)
        start = jnp.dot(column.astype(BF16), ahead, preferred_element_type=F32)
        start = start + jnp.dot(blocks_before.astype(BF16), every, preferred_element_type=F32)
        rank = (start + earlier).astype(jnp.int32)
        lo_ref[...] = jnp.where(mine > 0.0, rank & 127, -1)
        hi_ref[...] = jnp.where(mine > 0.0, rank >> 7, -1)
        part_ref[0] = (page & 255).astype(F32)
        part_ref[1] = (owner & 255).astype(F32)
        part_ref[2] = ((page >> 8) + ((owner >> 8) << 2) + ((tokens - 1) << 4)).astype(F32)
        part_ref[3] = jnp.where(earlier > 0.0, 0.0, 1.0)
        last = jnp.where(column > 0.0, start + column - 1.0, float(NOTHING)).astype(jnp.int32)
        list_ref[8:16, :] = jnp.concatenate([last[t * slots:t * slots + 1] for t in range(blocks)], axis=0)
        number = (start + column)[rows - 1:rows, 127:128]
        list_ref[16:24, :] = jnp.broadcast_to(number, (8, 128)).astype(jnp.int32)
        total_ref[...] = jnp.zeros_like(total_ref)

    sub = lax.broadcasted_iota(jnp.int32, (128, 128), 0)
    sub8 = lax.broadcasted_iota(jnp.int32, (8, 128), 0)

    def scatter(part):
        def step(n, carry):
            base = pl.multiple_of(n * 8, 8)
            lo8 = lo_ref[pl.ds(base, 8), :]
            hi8 = hi_ref[pl.ds(base, 8), :]
            p8 = [part_ref[k, pl.ds(base, 8), :] for k in range(4)]
            wide, tall = [], []
            for r in range(8):
                wide.append(jnp.where(sub == lo8[r:r + 1, :], 1.0, 0.0).astype(BF16))
                hit = sub8 == hi8[r:r + 1, :]
                tall.append(jnp.concatenate(
                    [jnp.where(hit, p8[k][r:r + 1, :], 0.0) for k in range(4)], axis=0).astype(BF16))
            wide = jnp.concatenate(wide, axis=1)
            tall = jnp.concatenate(tall, axis=1)
            total_ref[...] += lax.dot_general(wide, tall, NT, preferred_element_type=F32)
            return carry

        steps = lo_ref.shape[0] // 32
        lax.fori_loop(part * steps, (part + 1) * steps, step, 0)

    def write_list():
        total = jnp.concatenate([total_ref[...], jnp.zeros((128, 96), F32)], axis=1).T.astype(jnp.int32)
        p0, p1, p2, p3 = (total[8 * k:8 * k + 8, :] for k in range(4))
        page = p0 + ((p2 & 3) << 8)
        owner = p1 + (((p2 >> 2) & 3) << 8)
        tokens = (p2 >> 4) + 1
        list_ref[0:8, :] = page + (owner << 10) + (tokens << 20) + (p3 << 25)

    pieces = [place_pages] + [functools.partial(scatter, n) for n in range(4)] + [write_list]
    for copy in plane_gather(full_ref.at[z, y, c], full_ref, ssem, rsem, dsend, drecv, between=pieces):
        copy.wait_send()


def gather_queries(queries, table, lengths, pool, page_len):
    req = table.shape[1]
    rows = table.shape[0] * req // 128
    _, half, heads, dim = queries.shape
    return pl.pallas_call(
        functools.partial(queries_kernel, pool.bit_length() - 1, page_len),
        out_shape=(
            jax.ShapeDtypeStruct((4, 4, 2, 2, half, heads, dim), BF16),
            jax.ShapeDtypeStruct((24, 128), jnp.int32),
        ),
        in_specs=[HBM] * 3,
        out_specs=(VMEM, VMEM),
        scratch_shapes=[
            pltpu.VMEM(table.shape, jnp.int32),
            pltpu.VMEM(lengths.shape, jnp.int32),
            pltpu.VMEM((rows, 128), jnp.int32),
            pltpu.VMEM((rows, 128), jnp.int32),
            pltpu.VMEM((4, rows, 128), F32),
            pltpu.VMEM((128, 32), F32),
            pltpu.SemaphoreType.DMA((3,)),
        ] + gather_sems(),
        compiler_params=pltpu.CompilerParams(collective_id=0, has_side_effects=True, vmem_limit_bytes=8 << 20),
        cost_estimate=pl.CostEstimate(flops=10**10, bytes_accessed=1 << 23, transcendentals=0),
        name="gather_queries",
    )(queries, table, lengths)


def pages_kernel(scale, list_ref, q_ref, k_ref, v_ref, acc_ref, sum_ref, top_ref, wait_ref, peak_ref, mass_ref):
    lane = lax.broadcasted_iota(jnp.int32, (16, 128), 1)
    blank = jnp.where(lane < 32, LOW, 0.0)
    zero = jnp.zeros((16, 128), F32)
    sum_ref[NOTHING] = zero
    top_ref[NOTHING] = blank
    wait_ref[...] = jnp.zeros_like(wait_ref)
    peak_ref[...] = jnp.zeros_like(peak_ref)
    mass_ref[...] = jnp.zeros_like(mass_ref)

    i = lax.broadcasted_iota(jnp.int32, (16, 128), 0)
    kv_match = (i // 8) == (lane % 2)
    token = (lane % 32) // 2
    token_of = [jnp.where(kv_match & (lane // 32 == n), token, 1 << 20) for n in range(4)]

    def entry(k):
        word = list_ref[k >> 7, k & 127]
        return word & 1023, (word >> 10) & 1023, (word >> 20) & 31, (word >> 25) & 1

    def step(n, carry):
        past = jnp.maximum(n - 1, 0) * BATCH
        base = n * BATCH
        before = [entry(past + e) for e in range(BATCH)]
        now = [entry(base + e) for e in range(BATCH)]
        outs, scores = [], []
        for g in range(BATCH // 4):
            four = slice(4 * g, 4 * g + 4)
            vs = jnp.concatenate([v_ref[p] for p, _, _, _ in before[four]], axis=0)
            outs.append(jnp.dot(wait_ref[g], vs, preferred_element_type=F32))
            qs = jnp.concatenate([q_ref[r] for _, r, _, _ in now[four]], axis=0)
            ks = jnp.concatenate([k_ref[p] for p, _, _, _ in now[four]], axis=0)
            scores.append(lax.dot_general(qs, ks, NT, preferred_element_type=F32))
        top, mass, acc = carry
        for e, (_, _, _, first) in enumerate(before):
            old = jnp.where(first == 1, LOW, top)
            p = peak_ref[e]
            top = jnp.maximum(old, p)
            f_old = jnp.exp(old - top)
            f_new = jnp.exp(p - top)
            mass = mass * f_old + mass_ref[e] * f_new
            acc = acc * f_old + outs[e // 4][16 * (e % 4):16 * (e % 4) + 16] * f_new
            sum_ref[past + e] = acc
            top_ref[past + e] = jnp.where(lane < 32, top, mass)
        for g in range(BATCH // 4):
            weights = []
            for e in range(4):
                valid = token_of[e] < now[4 * g + e][2]
                sc = jnp.where(valid, scores[g][16 * e:16 * e + 16] * scale, LOW)
                peak = jnp.max(sc, axis=1, keepdims=True)
                w = jnp.where(valid, jnp.exp(sc - peak), 0.0)
                peak_ref[4 * g + e] = jnp.broadcast_to(peak, (16, 128))
                mass_ref[4 * g + e] = jnp.broadcast_to(jnp.sum(w, axis=1, keepdims=True), (16, 128))
                weights.append(w)
            wait_ref[g] = jnp.concatenate(weights, axis=0).astype(BF16)
        return top, mass, acc

    batches = (list_ref[16, 0] + BATCH - 1) // BATCH
    lax.fori_loop(0, batches + 1, step, (zero, zero, zero))

    def spread(d, carry):
        tops = blank
        for row in range(32):
            r = d * 32 + row
            last = list_ref[8 + (r >> 7), r & 127]
            acc = sum_ref[last]
            tops = jnp.where((lane == row) | (lane == row + 32), top_ref[last], tops)
            for hh in range(2):
                acc_ref[hh, d, row] = acc[8 * hh:8 * hh + 8]
        for hh in range(2):
            acc_ref[hh, d, 32] = tops[8 * hh:8 * hh + 8]
        return carry

    lax.fori_loop(0, acc_ref.shape[1], spread, 0)


def attend_pages(words, all_queries, keys, values):
    req, heads, dim = all_queries.shape
    return pl.pallas_call(
        functools.partial(pages_kernel, dim ** (-0.5)),
        out_shape=jax.ShapeDtypeStruct((2, req // 32, 33, 8, 128), F32),
        in_specs=[SMEM, VMEM, VMEM, VMEM],
        out_specs=VMEM,
        scratch_shapes=[
            pltpu.VMEM((NOTHING + 1, heads, dim), F32),
            pltpu.VMEM((NOTHING + 1, heads, dim), F32),
            pltpu.VMEM((BATCH // 4, 4 * heads, dim), BF16),
            pltpu.VMEM((BATCH, heads, dim), F32),
            pltpu.VMEM((BATCH, heads, dim), F32),
        ],
        compiler_params=pltpu.CompilerParams(vmem_limit_bytes=20 << 20),
        name="attend_pages",
    )(words, all_queries, keys, values)


def merge(dst, one, other):
    lane = lax.broadcasted_iota(jnp.int32, (8, 128), 1)
    t1, t2 = one[32], other[32]
    top = jnp.maximum(t1, t2)
    f1 = jnp.exp(t1 - top)
    f2 = jnp.exp(t2 - top)
    mass = t1 * pltpu.roll(f1, 32, 1) + t2 * pltpu.roll(f2, 32, 1)
    for row in range(32):
        dst[row] = one[row] * f1[:, row:row + 1] + other[row] * f2[:, row:row + 1]
    dst[32] = jnp.where(lane < 32, top, mass)


def finish_kernel(part_ref, w_ref, att_ref, proj_ref, unit, pair, far1, near1, next1, far2, near2, next2,
                  tmp, own, full, cols, farx, nearx, nextx,
                  s0, r0, s1, r1, s2, r2, ssem, rsem, dsend, drecv, sx, rx):
    z, y, c, s = place()
    x = lax.axis_index("mp")
    home = plane_id(z, y, c)
    greet([plane_id(wrap(z + 1), y, c), plane_id(wrap(z - 1), y, c), plane_id(z, wrap(y + 1), c),
           plane_id(z, wrap(y - 1), c), plane_id(wrap(z + 2), y, c), plane_id(z, wrap(y + 2), c), plane_id(z, y, 1 - c), {"mp": wrap(x + 1)}, {"mp": wrap(x - 1)}])

    def spot(hh, oa, ob):
        dz = oa + hh * (ob - oa)
        dy = ob + hh * (oa - ob)
        return wrap(z + dz), wrap(y + dy)

    def step_of(n):
        m = n % 3
        return 2 * ((3 - n) // 3) + s * (m * (5 - 3 * m) // 2)

    def swap(hh, zt, yt):
        return remote(part_ref.at[hh, (zt * 4 + yt) * 2 + 1 - c], pair.at[hh, zt, yt], s0.at[hh, zt, yt],
                      r0.at[hh, zt, yt], plane_id(z, y, 1 - c))

    def hop(hh, sign):
        zt, yt = spot(hh, sign * s, 0)
        return plane_id(zt, yt, c)

    def hop2(hh, sign):
        zt, yt = spot(hh, 0, sign * s)
        return plane_id(zt, yt, c)

    order = (0, 2, 1, 3)

    for oa in order:
        def begin(k, carry, oa=oa):
            hh, ob = k % 2, k // 2
            zt, yt = spot(hh, step_of(oa), step_of(ob))
            swap(hh, zt, yt).start()
            return carry
        lax.fori_loop(0, 8, begin, 0)

    def send1(kind, hh, ob, zt, yt):
        dst = (far1, near1, next1)[kind].at[hh, ob]
        return remote(unit.at[hh, zt, yt], dst, s1.at[kind, hh, ob], r1.at[kind, hh, ob], hop(hh, 1 if kind < 2 else -1))

    def both_cores(hh, zt, yt):
        swap(hh, zt, yt).wait_recv()
        merge(unit.at[hh, zt, yt], part_ref.at[hh, (zt * 4 + yt) * 2 + c], pair.at[hh, zt, yt])

    def far_units(k, carry):
        hh, ob = k % 2, k // 2
        zt, yt = spot(hh, 2, step_of(ob))
        both_cores(hh, zt, yt)
        send1(0, hh, ob, zt, yt).start()
        return carry

    def next_units(k, carry):
        hh, ob = k % 2, k // 2
        zt, yt = spot(hh, -s, step_of(ob))
        both_cores(hh, zt, yt)
        send1(2, hh, ob, zt, yt).start()
        return carry

    def near_units(k, carry):
        hh, ob = k % 2, k // 2
        zt, yt = spot(hh, s, step_of(ob))
        both_cores(hh, zt, yt)
        send1(0, hh, ob, zt, yt).wait_recv()
        merge(unit.at[hh, zt, yt], unit.at[hh, zt, yt], far1.at[hh, ob])
        send1(1, hh, ob, zt, yt).start()
        return carry

    def own_units(k, carry):
        hh, ob = k % 2, k // 2
        zt, yt = spot(hh, 0, step_of(ob))
        both_cores(hh, zt, yt)
        return carry

    lax.fori_loop(0, 8, far_units, 0)
    lax.fori_loop(0, 8, next_units, 0)
    lax.fori_loop(0, 8, near_units, 0)
    lax.fori_loop(0, 8, own_units, 0)

    def send2(kind, hh, zt, yt):
        dst = (far2, near2, next2)[kind].at[hh]
        return remote(unit.at[hh, zt, yt], dst, s2.at[kind, hh], r2.at[kind, hh], hop2(hh, 1 if kind < 2 else -1))

    def gathered(hh, ob):
        zt, yt = spot(hh, 0, step_of(ob))
        send1(2, hh, ob, zt, yt).wait_recv()
        merge(unit.at[hh, zt, yt], unit.at[hh, zt, yt], next1.at[hh, ob])
        send1(1, hh, ob, zt, yt).wait_recv()
        merge(unit.at[hh, zt, yt], unit.at[hh, zt, yt], near1.at[hh, ob])
        return zt, yt

    def far_blocks(hh, carry):
        zt, yt = gathered(hh, 0)
        send2(0, hh, zt, yt).start()
        return carry

    def next_blocks(hh, carry):
        zt, yt = gathered(hh, 2)
        send2(2, hh, zt, yt).start()
        return carry

    def near_blocks(hh, carry):
        zt, yt = gathered(hh, 1)
        send2(0, hh, zt, yt).wait_recv()
        merge(unit.at[hh, zt, yt], unit.at[hh, zt, yt], far2.at[hh])
        send2(1, hh, zt, yt).start()
        return carry

    def own_blocks(hh, carry):
        zt, yt = gathered(hh, 3)
        send2(2, hh, zt, yt).wait_recv()
        merge(unit.at[hh, zt, yt], unit.at[hh, zt, yt], next2.at[hh])
        send2(1, hh, zt, yt).wait_recv()
        merge(unit.at[hh, zt, yt], unit.at[hh, zt, yt], near2.at[hh])
        return carry

    for phase in (far_blocks, next_blocks, near_blocks, own_blocks):
        lax.fori_loop(0, 2, phase, 0)

    masses = [unit[hh, z, y, 32] for hh in range(2)]
    for row in range(32):
        both = [unit[hh, z, y, row] / masses[hh][:, 32 + row:33 + row] for hh in range(2)]
        for hh in range(2):
            tmp[hh, row] = both[hh]
        att_ref[row] = jnp.concatenate(both, axis=0).astype(BF16)
    for hh in range(2):
        for head in range(8):
            own[hh, head] = tmp[hh, :, head, :].astype(BF16)
    for hh in range(2):
        full[z, y, c, hh] = own[hh]

    sent = plane_gather(own, full, ssem, rsem, dsend, drecv)

    def project(step):
        t = wrap(x + step)
        rows = [full[t, :, :, hh, head].reshape(256, 128) for hh in range(2) for head in range(8)]
        cols[t] = jnp.dot(jnp.concatenate(rows, axis=1), w_ref[...], preferred_element_type=F32)
        return t

    def sendx(kind, t):
        return remote(cols.at[t], (farx, nearx, nextx)[kind], sx.at[kind], rx.at[kind],
                      {"mp": wrap(x + (s if kind < 2 else -s))})

    t = project(2)
    sendx(0, t).start()
    t = project(-s)
    sendx(2, t).start()
    t = project(s)
    sendx(0, t).wait_recv()
    cols[t] = cols[t] + farx[...]
    sendx(1, t).start()
    t = project(0)
    sendx(2, t).wait_recv()
    total = cols[t] + nextx[...]
    sendx(1, t).wait_recv()
    proj_ref[...] = (total + nearx[...]).astype(BF16)

    for kind in range(3):
        sendx(kind, t).wait_send()
    for copy in sent:
        copy.wait_send()

    def drain(k, carry):
        hh, ob = k % 2, k // 2
        for oa in range(4):
            zt, yt = spot(hh, step_of(oa), step_of(ob))
            swap(hh, zt, yt).wait_send()
        for kind in range(3):
            send1(kind, hh, ob, z, y).wait_send()
        return carry

    lax.fori_loop(0, 8, drain, 0)

    def drain2(hh, carry):
        for kind in range(3):
            send2(kind, hh, z, y).wait_send()
        return carry

    lax.fori_loop(0, 2, drain2, 0)


def finish(parts, weight, rows):
    unit = (33, 8, 128)
    dma = pltpu.SemaphoreType.DMA
    return pl.pallas_call(
        finish_kernel,
        out_shape=(
            jax.ShapeDtypeStruct((rows, 16, 128), BF16),
            jax.ShapeDtypeStruct((256, weight.shape[1]), BF16),
        ),
        in_specs=[VMEM, VMEM],
        out_specs=(VMEM, VMEM),
        scratch_shapes=[
            pltpu.VMEM((2, 4, 4) + unit, F32),
            pltpu.VMEM((2, 4, 4) + unit, F32),
            pltpu.VMEM((2, 4) + unit, F32),
            pltpu.VMEM((2, 4) + unit, F32),
            pltpu.VMEM((2, 4) + unit, F32),
            pltpu.VMEM((2,) + unit, F32),
            pltpu.VMEM((2,) + unit, F32),
            pltpu.VMEM((2,) + unit, F32),
            pltpu.VMEM((2, 32, 8, 128), F32),
            pltpu.VMEM((2, 8, 32, 128), BF16),
            pltpu.VMEM((4, 4, 2, 2, 8, 32, 128), BF16),
            pltpu.VMEM((4, 256, 256), F32),
            pltpu.VMEM((256, 256), F32),
            pltpu.VMEM((256, 256), F32),
            pltpu.VMEM((256, 256), F32),
            dma((2, 4, 4)),
            dma((2, 4, 4)),
            dma((3, 2, 4)),
            dma((3, 2, 4)),
            dma((3, 2)),
            dma((3, 2)),
        ] + gather_sems() + [dma((3,)), dma((3,))],
        compiler_params=pltpu.CompilerParams(collective_id=1, has_side_effects=True, vmem_limit_bytes=24 << 20),
        name="finish",
    )(parts, weight)


def body(queries, lookup_sheets, content_sheets, page_table, context_len, out_weight):
    req = page_table.shape[0]
    pool, page_len, kv, dim = lookup_sheets.shape
    rows, heads, _ = queries.shape
    all_queries, words = gather_queries(
        *(pltpu.with_memory_space_constraint(a, pltpu.HBM)
          for a in (queries.reshape(2, rows // 2, heads, dim), page_table.T, context_len.reshape(req // 128, 128))),
        pool,
        page_len,
    )
    parts = attend_pages(
        words,
        all_queries.reshape(req, heads, dim),
        lookup_sheets.reshape(pool, page_len * kv, dim),
        content_sheets.reshape(pool, page_len * kv, dim),
    )
    return finish(parts, out_weight, rows)


def solution(mesh):
    finer = Mesh(mesh.devices.reshape(4, 4, 2, mesh.shape["mp"]), ("dp_0", "dp_1", "dp_2", "mp"))
    return jax.shard_map(
        body,
        mesh=finer,
        in_specs=(
            P(DP, "mp", None),
            P(DP, None, "mp", None),
            P(DP, None, "mp", None),
            P(),
            P(),
            P("mp", DP),
        ),
        out_specs=(P(DP, "mp", None), P("mp", DP)),
        check_vma=False,
    )
```

```python
import functools

import jax
import jax.numpy as jnp
from jax import lax
from jax.experimental import pallas as pl
from jax.experimental.pallas import tpu as pltpu
from jax.sharding import Mesh
from jax.sharding import PartitionSpec as P

DP = ("dp_0", "dp_1", "dp_2")
MESH = pl.DeviceIdType.MESH
LOW = -1e30
QUARTER = 64
BATCH = 32
NOTHING = 1056
F32 = jnp.float32
BF16 = jnp.bfloat16
NT = (((1,), (1,)), ((), ()))
VMEM = pl.BlockSpec(memory_space=pltpu.VMEM)
HBM = pl.BlockSpec(memory_space=pltpu.HBM)
SMEM = pl.BlockSpec(memory_space=pltpu.SMEM)


def wrap(value):
    return lax.rem(value + 8, 4)


def place():
    z, y, c = (lax.axis_index(name) for name in DP)
    return z, y, c, 1 - 2 * c


def plane_id(z, y, c):
    return {"dp_0": z, "dp_1": y, "dp_2": c}


def greet(devices):
    barrier = pltpu.get_barrier_semaphore()
    for device in devices:
        pl.semaphore_signal(barrier, inc=1, device_id=device, device_id_type=MESH)
    pl.semaphore_wait(barrier, len(devices))


def remote(src, dst, send_sem, recv_sem, device):
    return pltpu.make_async_remote_copy(
        src_ref=src,
        dst_ref=dst,
        send_sem=send_sem,
        recv_sem=recv_sem,
        device_id=device,
        device_id_type=MESH,
    )


def plane_gather(own, full, ssem, rsem, dsend, drecv, between=(), row_done=None):
    z, y, c, s = place()
    work = list(between)

    def fill():
        piece = work.pop(0) if work else None
        if piece is not None:
            piece()

    def at(h, a, b):
        return full.at[a, b, c, h] if h == 0 else full.at[b, a, c, h]

    def device(h, a, b):
        return plane_id(a, b, c) if h == 0 else plane_id(b, a, c)

    def mine(h):
        return (z, y) if h == 0 else (y, z)

    sent = []

    def go(h, group, m, src, dst, target):
        copy = remote(src, dst, ssem.at[h, group, m], rsem.at[h, group, m], target)
        copy.start()
        sent.append(copy)

    def come(h, group, m, dst):
        remote(dst, dst, ssem.at[h, group, m], rsem.at[h, group, m], plane_id(z, y, c)).wait_recv()

    def share(h, slot, src, dst):
        copy = remote(src, dst, dsend.at[h, slot], drecv.at[h, slot], plane_id(z, y, 1 - c))
        copy.start()
        sent.append(copy)

    def spread(h, group, slot, src, a, b):
        go(h, group, 0, src, at(h, a, b), device(h, mine(h)[0], wrap(b + s)))
        go(h, group, 1, src, at(h, a, b), device(h, mine(h)[0], wrap(b - s)))

    def first(h):
        a, b = mine(h)
        go(h, 0, 0, own.at[h], at(h, a, b), device(h, wrap(a + s), b))
        go(h, 0, 1, own.at[h], at(h, a, b), device(h, wrap(a - s), b))
        go(h, 0, 2, own.at[h], at(h, a, b), device(h, wrap(a + 2), b))

    for h in range(2):
        first(h)
    for h in range(2):
        share(h, 0, own.at[h], at(h, *mine(h)))
        spread(h, 1, 0, own.at[h], *mine(h))
    fill()
    for h in range(2):
        a, b = mine(h)
        near = wrap(a - s)
        come(h, 0, 0, at(h, near, b))
        spread(h, 2, 4, at(h, near, b), near, b)
        share(h, 4, at(h, near, b), at(h, near, b))
    for h in range(2):
        a, b = mine(h)
        near = wrap(a + s)
        come(h, 0, 1, at(h, near, b))
        spread(h, 3, 8, at(h, near, b), near, b)
        share(h, 8, at(h, near, b), at(h, near, b))
    fill()
    for h in range(2):
        a, b = mine(h)
        far = wrap(a + 2)
        come(h, 0, 2, at(h, far, b))
        spread(h, 4, 12, at(h, far, b), far, b)
        share(h, 12, at(h, far, b), at(h, far, b))
    fill()
    steps = (0, 0, -1, 1, 2)

    def sides(group):
        for h in range(2):
            a, b = mine(h)
            row = wrap(a + steps[group] * s)
            near = wrap(b - s)
            come(h, group, 0, at(h, row, near))
            go(h, group, 2, at(h, row, near), at(h, row, near), device(h, a, wrap(b + s)))
            share(h, 4 * (group - 1) + 1, at(h, row, near), at(h, row, near))
            other = wrap(b + s)
            come(h, group, 1, at(h, row, other))
            share(h, 4 * (group - 1) + 2, at(h, row, other), at(h, row, other))
        fill()

    def far(group):
        for h in range(2):
            a, b = mine(h)
            row = wrap(a + steps[group] * s)
            opposite = wrap(b + 2)
            come(h, group, 2, at(h, row, opposite))
            share(h, 4 * (group - 1) + 3, at(h, row, opposite), at(h, row, opposite))

    across = (0, 2, 1, 3)

    def from_pair(k, n):
        for h, slot in ((0, 4 * across[k] + across[n]), (1, 4 * across[n] + across[k])):
            where = full.at[0, 0, 1 - c, h]
            remote(where, where, dsend.at[h, slot], drecv.at[h, slot], plane_id(z, y, 1 - c)).wait_recv()

    def arrived(k, columns=(0, 1, 2, 3)):
        for n in columns:
            from_pair(k, n)
        if row_done is not None:
            row_done(k, columns)

    for group in range(1, 5):
        sides(group)
    far(1)
    if row_done is not None:
        arrived(0)
    far(2)
    far(3)
    if row_done is not None:
        arrived(1)
        arrived(2)
    far(4)
    if row_done is not None:
        arrived(3, (0, 1, 2))
        arrived(3, (3,))
    else:
        for k in range(4):
            arrived(k)
    return sent


def gather_sems():
    return [
        pltpu.SemaphoreType.DMA((2, 5, 3)),
        pltpu.SemaphoreType.DMA((2, 5, 3)),
        pltpu.SemaphoreType.DMA((2, 16)),
        pltpu.SemaphoreType.DMA((2, 16)),
    ]


def queries_kernel(pool_bits, page_len, q_hbm, table_hbm, len_hbm, full_ref, list_ref,
                   table_ref, len_ref, lo_ref, hi_ref, part_ref, total_ref, lsem, ssem, rsem, dsend, drecv):
    z, y, c, s = place()
    me = (z * 4 + y) * 2 + c
    loads = [
        pltpu.make_async_copy(src, dst, lsem.at[n])
        for n, (src, dst) in enumerate(
            ((q_hbm, full_ref.at[z, y, c]), (table_hbm, table_ref), (len_hbm, len_ref)))
    ]
    for load in loads:
        load.start()
    greet([plane_id(wrap(z + 1), y, c), plane_id(wrap(z - 1), y, c), plane_id(z, wrap(y + 1), c),
           plane_id(z, wrap(y - 1), c), plane_id(wrap(z + 2), y, c), plane_id(z, wrap(y + 2), c), plane_id(z, y, 1 - c)])
    loads[0].wait()

    def place_pages():
        for load in loads[1:]:
            load.wait()
        slots = table_ref.shape[0]
        slot = lax.broadcasted_iota(jnp.int32, (slots, 128), 0)
        lane = lax.broadcasted_iota(jnp.int32, (slots, 128), 1)
        blocks = table_ref.shape[1] // 128
        mine, tokens, page, owner = [], [], [], []
        for t in range(blocks):
            ids = table_ref[:, t * 128:(t + 1) * 128]
            length = jnp.broadcast_to(len_ref[t:t + 1, :], (slots, 128))
            left = jnp.clip(length - slot * page_len, 0, page_len)
            mine.append(jnp.where(((ids >> pool_bits) == me) & (left > 0), 1.0, 0.0))
            tokens.append(left)
            page.append(ids & ((1 << pool_bits) - 1))
            owner.append(lane + t * 128)
        mine, tokens, page, owner = (jnp.concatenate(v, axis=0) for v in (mine, tokens, page, owner))
        rows = slots * blocks
        mine_h = mine.astype(BF16)
        i = lax.broadcasted_iota(jnp.int32, (rows, rows), 0)
        j = lax.broadcasted_iota(jnp.int32, (rows, rows), 1)
        same = (i // slots) == (j // slots)

        def count(which, what):
            return jnp.dot(jnp.where(which, 1.0, 0.0).astype(BF16), what, preferred_element_type=F32)

        earlier = count(same & (j < i), mine_h)
        column = count(same, mine_h)
        blocks_before = count((j // slots) < (i // slots), mine_h)
        i = lax.broadcasted_iota(jnp.int32, (128, 128), 0)
        j = lax.broadcasted_iota(jnp.int32, (128, 128), 1)
        ahead = jnp.where(i < j, 1.0, 0.0).astype(BF16)
        every = jnp.ones((128, 128), BF16)
        start = jnp.dot(column.astype(BF16), ahead, preferred_element_type=F32)
        start = start + jnp.dot(blocks_before.astype(BF16), every, preferred_element_type=F32)
        rank = (start + earlier).astype(jnp.int32)
        lo_ref[...] = jnp.where(mine > 0.0, rank & 127, -1)
        hi_ref[...] = jnp.where(mine > 0.0, rank >> 7, -1)
        part_ref[0] = (page & 255).astype(F32)
        part_ref[1] = (owner & 255).astype(F32)
        part_ref[2] = ((page >> 8) + ((owner >> 8) << 2) + ((tokens - 1) << 4)).astype(F32)
        part_ref[3] = jnp.where(earlier > 0.0, 0.0, 1.0)
        last = jnp.where(column > 0.0, start + column - 1.0, float(NOTHING)).astype(jnp.int32)
        list_ref[8:16, :] = jnp.concatenate([last[t * slots:t * slots + 1] for t in range(blocks)], axis=0)
        number = (start + column)[rows - 1:rows, 127:128]
        list_ref[16:24, :] = jnp.broadcast_to(number, (8, 128)).astype(jnp.int32)
        total_ref[...] = jnp.zeros_like(total_ref)

    sub = lax.broadcasted_iota(jnp.int32, (128, 128), 0).astype(F32).astype(BF16)
    one, nil = jnp.ones((128, 128), BF16), jnp.zeros((128, 128), BF16)
    sub8 = lax.broadcasted_iota(jnp.int32, (8, 128), 0)

    def scatter(part):
        def step(n, carry):
            base = pl.multiple_of(n * 8, 8)
            lo8 = lo_ref[pl.ds(base, 8), :].astype(F32)
            hi8 = hi_ref[pl.ds(base, 8), :]
            p8 = [part_ref[k, pl.ds(base, 8), :] for k in range(4)]
            wide, tall = [], []
            for r in range(8):
                wide.append(jnp.where(sub == jnp.broadcast_to(lo8[r:r + 1, :], (128, 128)).astype(BF16), one, nil))
                hit = sub8 == hi8[r:r + 1, :]
                tall.append(jnp.concatenate(
                    [jnp.where(hit, p8[k][r:r + 1, :], 0.0) for k in range(4)], axis=0).astype(BF16))
            wide = jnp.concatenate(wide, axis=1)
            tall = jnp.concatenate(tall, axis=1)
            total_ref[...] += lax.dot_general(wide, tall, NT, preferred_element_type=F32)
            return carry

        steps = lo_ref.shape[0] // 32
        lax.fori_loop(part * steps, (part + 1) * steps, step, 0)

    def write_list():
        total = jnp.concatenate([total_ref[...], jnp.zeros((128, 96), F32)], axis=1).T.astype(jnp.int32)
        p0, p1, p2, p3 = (total[8 * k:8 * k + 8, :] for k in range(4))
        page = p0 + ((p2 & 3) << 8)
        owner = p1 + (((p2 >> 2) & 3) << 8)
        tokens = (p2 >> 4) + 1
        list_ref[0:8, :] = page + (owner << 10) + (tokens << 20) + (p3 << 25)

    def start_list():
        place_pages()
        scatter(0)

    def end_list():
        scatter(3)
        write_list()

    pieces = [start_list, None, functools.partial(scatter, 1), None, functools.partial(scatter, 2), None, end_list]
    for copy in plane_gather(full_ref.at[z, y, c], full_ref, ssem, rsem, dsend, drecv, between=pieces):
        copy.wait_send()


def gather_queries(queries, table, lengths, pool, page_len):
    req = table.shape[1]
    rows = table.shape[0] * req // 128
    _, half, heads, dim = queries.shape
    return pl.pallas_call(
        functools.partial(queries_kernel, pool.bit_length() - 1, page_len),
        out_shape=(
            jax.ShapeDtypeStruct((4, 4, 2, 2, half, heads, dim), BF16),
            jax.ShapeDtypeStruct((24, 128), jnp.int32),
        ),
        in_specs=[HBM] * 3,
        out_specs=(VMEM, VMEM),
        scratch_shapes=[
            pltpu.VMEM(table.shape, jnp.int32),
            pltpu.VMEM(lengths.shape, jnp.int32),
            pltpu.VMEM((rows, 128), jnp.int32),
            pltpu.VMEM((rows, 128), jnp.int32),
            pltpu.VMEM((4, rows, 128), F32),
            pltpu.VMEM((128, 32), F32),
            pltpu.SemaphoreType.DMA((3,)),
        ] + gather_sems(),
        compiler_params=pltpu.CompilerParams(collective_id=0, has_side_effects=True, vmem_limit_bytes=8 << 20),
        cost_estimate=pl.CostEstimate(flops=10**10, bytes_accessed=1 << 23, transcendentals=0),
        name="gather_queries",
    )(queries, table, lengths)


def pages_kernel(scale, list_ref, q_ref, k_ref, v_ref, acc_ref, sum_ref, top_ref, wait_ref, peak_ref, mass_ref):
    lane = lax.broadcasted_iota(jnp.int32, (16, 128), 1)
    blank = jnp.where(lane < 32, LOW, 0.0)
    zero = jnp.zeros((16, 128), F32)
    sum_ref[NOTHING] = zero
    top_ref[NOTHING] = blank
    wait_ref[...] = jnp.zeros_like(wait_ref)
    peak_ref[...] = jnp.zeros_like(peak_ref)
    mass_ref[...] = jnp.zeros_like(mass_ref)

    i = lax.broadcasted_iota(jnp.int32, (16, 128), 0)
    kv_match = (i // 8) == (lane % 2)
    token = (lane % 32) // 2
    token_of = [jnp.where(kv_match & (lane // 32 == n), token, 1 << 20) for n in range(4)]

    def entry(k):
        word = list_ref[k >> 7, k & 127]
        return word & 1023, (word >> 10) & 1023, (word >> 20) & 31, (word >> 25) & 1

    def step(n, carry):
        past = jnp.maximum(n - 1, 0) * BATCH
        base = n * BATCH
        before = [entry(past + e) for e in range(BATCH)]
        now = [entry(base + e) for e in range(BATCH)]
        outs, scores = [], []
        for g in range(BATCH // 4):
            four = slice(4 * g, 4 * g + 4)
            vs = jnp.concatenate([v_ref[p] for p, _, _, _ in before[four]], axis=0)
            outs.append(jnp.dot(wait_ref[g], vs, preferred_element_type=F32))
            qs = jnp.concatenate([q_ref[r] for _, r, _, _ in now[four]], axis=0)
            ks = jnp.concatenate([k_ref[p] for p, _, _, _ in now[four]], axis=0)
            scores.append(lax.dot_general(qs, ks, NT, preferred_element_type=F32))
        top, mass, acc = carry
        for e, (_, _, _, first) in enumerate(before):
            old = jnp.where(first == 1, LOW, top)
            p = peak_ref[e]
            top = jnp.maximum(old, p)
            f_old = jnp.exp(old - top)
            f_new = jnp.exp(p - top)
            mass = mass * f_old + mass_ref[e] * f_new
            acc = acc * f_old + outs[e // 4][16 * (e % 4):16 * (e % 4) + 16] * f_new
            sum_ref[past + e] = acc
            top_ref[past + e] = jnp.where(lane < 32, top, mass)
        for g in range(BATCH // 4):
            weights = []
            for e in range(4):
                valid = token_of[e] < now[4 * g + e][2]
                sc = jnp.where(valid, scores[g][16 * e:16 * e + 16] * scale, LOW)
                peak = jnp.max(sc, axis=1, keepdims=True)
                w = jnp.where(valid, jnp.exp(sc - peak), 0.0)
                peak_ref[4 * g + e] = jnp.broadcast_to(peak, (16, 128))
                mass_ref[4 * g + e] = jnp.broadcast_to(jnp.sum(w, axis=1, keepdims=True), (16, 128))
                weights.append(w)
            wait_ref[g] = jnp.concatenate(weights, axis=0).astype(BF16)
        return top, mass, acc

    batches = (list_ref[16, 0] + BATCH - 1) // BATCH
    lax.fori_loop(0, batches + 1, step, (zero, zero, zero))

    def spread(d, carry):
        tops = blank
        for row in range(32):
            r = d * 32 + row
            last = list_ref[8 + (r >> 7), r & 127]
            acc = sum_ref[last]
            tops = jnp.where((lane == row) | (lane == row + 32), top_ref[last], tops)
            for hh in range(2):
                acc_ref[hh, d, row] = acc[8 * hh:8 * hh + 8]
        for hh in range(2):
            acc_ref[hh, d, 32] = tops[8 * hh:8 * hh + 8]
        return carry

    lax.fori_loop(0, acc_ref.shape[1], spread, 0)


def attend_pages(words, all_queries, keys, values):
    req, heads, dim = all_queries.shape
    return pl.pallas_call(
        functools.partial(pages_kernel, dim ** (-0.5)),
        out_shape=jax.ShapeDtypeStruct((2, req // 32, 33, 8, 128), F32),
        in_specs=[SMEM, VMEM, VMEM, VMEM],
        out_specs=VMEM,
        scratch_shapes=[
            pltpu.VMEM((NOTHING + 1, heads, dim), F32),
            pltpu.VMEM((NOTHING + 1, heads, dim), F32),
            pltpu.VMEM((BATCH // 4, 4 * heads, dim), BF16),
            pltpu.VMEM((BATCH, heads, dim), F32),
            pltpu.VMEM((BATCH, heads, dim), F32),
        ],
        compiler_params=pltpu.CompilerParams(vmem_limit_bytes=20 << 20),
        name="attend_pages",
    )(words, all_queries, keys, values)


def merge(dst, one, other):
    lane = lax.broadcasted_iota(jnp.int32, (8, 128), 1)
    t1, t2 = one[32], other[32]
    top = jnp.maximum(t1, t2)
    f1 = jnp.exp(t1 - top)
    f2 = jnp.exp(t2 - top)
    mass = t1 * pltpu.roll(f1, 32, 1) + t2 * pltpu.roll(f2, 32, 1)
    for row in range(32):
        dst[row] = one[row] * f1[:, row:row + 1] + other[row] * f2[:, row:row + 1]
    dst[32] = jnp.where(lane < 32, top, mass)


def finish_kernel(part_ref, w_ref, att_ref, proj_ref, unit, pair, far1, near1, next1, far2, near2, next2,
                  tmp, own, full, cols, farx, nearx, nextx,
                  s0, r0, s1, r1, s2, r2, ssem, rsem, dsend, drecv, sx, rx):
    z, y, c, s = place()
    x = lax.axis_index("mp")
    home = plane_id(z, y, c)
    greet([plane_id(wrap(z + 1), y, c), plane_id(wrap(z - 1), y, c), plane_id(z, wrap(y + 1), c),
           plane_id(z, wrap(y - 1), c), plane_id(wrap(z + 2), y, c), plane_id(z, wrap(y + 2), c), plane_id(z, y, 1 - c), {"mp": wrap(x + 1)}, {"mp": wrap(x - 1)}])

    def spot(hh, oa, ob):
        dz = oa + hh * (ob - oa)
        dy = ob + hh * (oa - ob)
        return wrap(z + dz), wrap(y + dy)

    def step_of(n):
        m = n % 3
        return 2 * ((3 - n) // 3) + s * (m * (5 - 3 * m) // 2)

    def swap(hh, zt, yt):
        return remote(part_ref.at[hh, (zt * 4 + yt) * 2 + 1 - c], pair.at[hh, zt, yt], s0.at[hh, zt, yt],
                      r0.at[hh, zt, yt], plane_id(z, y, 1 - c))

    def hop(hh, sign):
        zt, yt = spot(hh, sign * s, 0)
        return plane_id(zt, yt, c)

    def hop2(hh, sign):
        zt, yt = spot(hh, 0, sign * s)
        return plane_id(zt, yt, c)

    def far_place(n):
        m, odd = (n + 1) // 2, n % 2
        return wrap(z + step_of((1 - odd) * m)), wrap(y + step_of(odd * m))

    def rest_place(n):
        m, k = n // 3, n % 3
        return wrap(z + step_of(2 - m + 3 * (m // 2))), wrap(y + step_of(2 - k + 3 * (k // 2)))

    def give(where):
        def step(n, carry):
            zt, yt = where(n)
            for hh in range(2):
                swap(hh, zt, yt).start()
            return carry
        return step

    def send1(kind, hh, ob, zt, yt):
        dst = (far1, near1, next1)[kind].at[hh, ob]
        return remote(unit.at[hh, zt, yt], dst, s1.at[kind, hh, ob], r1.at[kind, hh, ob], hop(hh, 1 if kind < 2 else -1))

    def both_cores(hh, zt, yt):
        swap(hh, zt, yt).wait_recv()
        merge(unit.at[hh, zt, yt], part_ref.at[hh, (zt * 4 + yt) * 2 + c], pair.at[hh, zt, yt])

    def far_units(k, carry):
        hh, ob = k % 2, k // 2
        zt, yt = spot(hh, 2, step_of(ob))
        both_cores(hh, zt, yt)
        send1(0, hh, ob, zt, yt).start()
        return carry

    def next_units(k, carry):
        hh, ob = k % 2, k // 2
        zt, yt = spot(hh, -s, step_of(ob))
        both_cores(hh, zt, yt)
        send1(2, hh, ob, zt, yt).start()
        return carry

    def near_units(k, carry):
        hh, ob = k % 2, k // 2
        zt, yt = spot(hh, s, step_of(ob))
        both_cores(hh, zt, yt)
        send1(0, hh, ob, zt, yt).wait_recv()
        merge(unit.at[hh, zt, yt], unit.at[hh, zt, yt], far1.at[hh, ob])
        send1(1, hh, ob, zt, yt).start()
        return carry

    def own_units(k, carry):
        hh, ob = k % 2, k // 2
        zt, yt = spot(hh, 0, step_of(ob))
        both_cores(hh, zt, yt)
        return carry

    lax.fori_loop(0, 7, give(far_place), 0)
    lax.fori_loop(0, 9, give(rest_place), 0)
    lax.fori_loop(0, 8, far_units, 0)
    lax.fori_loop(0, 8, next_units, 0)
    lax.fori_loop(0, 8, near_units, 0)
    lax.fori_loop(0, 8, own_units, 0)

    def send2(kind, hh, zt, yt):
        dst = (far2, near2, next2)[kind].at[hh]
        return remote(unit.at[hh, zt, yt], dst, s2.at[kind, hh], r2.at[kind, hh], hop2(hh, 1 if kind < 2 else -1))

    def gathered(hh, ob):
        zt, yt = spot(hh, 0, step_of(ob))
        send1(2, hh, ob, zt, yt).wait_recv()
        merge(unit.at[hh, zt, yt], unit.at[hh, zt, yt], next1.at[hh, ob])
        send1(1, hh, ob, zt, yt).wait_recv()
        merge(unit.at[hh, zt, yt], unit.at[hh, zt, yt], near1.at[hh, ob])
        return zt, yt

    def far_blocks(hh, carry):
        zt, yt = gathered(hh, 0)
        send2(0, hh, zt, yt).start()
        return carry

    def next_blocks(hh, carry):
        zt, yt = gathered(hh, 2)
        send2(2, hh, zt, yt).start()
        return carry

    def near_blocks(hh, carry):
        zt, yt = gathered(hh, 1)
        send2(0, hh, zt, yt).wait_recv()
        merge(unit.at[hh, zt, yt], unit.at[hh, zt, yt], far2.at[hh])
        send2(1, hh, zt, yt).start()
        return carry

    def own_blocks(hh, carry):
        zt, yt = gathered(hh, 3)
        send2(2, hh, zt, yt).wait_recv()
        merge(unit.at[hh, zt, yt], unit.at[hh, zt, yt], next2.at[hh])
        send2(1, hh, zt, yt).wait_recv()
        merge(unit.at[hh, zt, yt], unit.at[hh, zt, yt], near2.at[hh])
        return carry

    for phase in (far_blocks, next_blocks, near_blocks, own_blocks):
        lax.fori_loop(0, 2, phase, 0)

    masses = [unit[hh, z, y, 32] for hh in range(2)]
    for row in range(32):
        both = [unit[hh, z, y, row] / masses[hh][:, 32 + row:33 + row] for hh in range(2)]
        for hh in range(2):
            tmp[hh, row] = both[hh]
        att_ref[row] = jnp.concatenate(both, axis=0).astype(BF16)
    for hh in range(2):
        for head in range(8):
            own[hh, head] = tmp[hh, :, head, :].astype(BF16)
    for hh in range(2):
        full[z, y, c, hh] = own[hh]

    def sendx(kind, t, q):
        rows = pl.ds(pl.multiple_of(q * QUARTER, QUARTER) if not isinstance(q, int) else q * QUARTER, QUARTER)
        dst = (farx, nearx, nextx)[kind].at[rows]
        return remote(cols.at[t, rows], dst, sx.at[kind, q], rx.at[kind, q],
                      {"mp": wrap(x + (s if kind < 2 else -s))})

    targets = [wrap(z + step) for step in (0, -s, s, 2)]
    columns_of = [wrap(y + step) for step in (0, -s, s, 2)]

    def pass_on(k):
        t = targets[k]

        @pl.when(wrap(t - x - s) == 0)
        def _():
            for q in columns_of:
                rows = pl.ds(pl.multiple_of(q * QUARTER, QUARTER), QUARTER)
                sendx(0, t, q).wait_recv()
                cols[t, rows] = cols[t, rows] + farx[rows]
                sendx(1, t, q).start()

    def send_on(t, quarters):
        @pl.when(wrap(t - x - 2) == 0)
        def _():
            for q in quarters:
                sendx(0, t, q).start()

        @pl.when(wrap(t - x + s) == 0)
        def _():
            for q in quarters:
                sendx(2, t, q).start()

    def project(k, columns):
        t = targets[k]
        if len(columns) == 4:
            rows = [full[t, :, :, hh, head].reshape(256, 128) for hh in range(2) for head in range(8)]
            cols[t] = jnp.dot(jnp.concatenate(rows, axis=1), w_ref[...], preferred_element_type=F32)
            send_on(t, columns_of)
            return
        for n in columns:
            q = columns_of[n]
            rows = [full[t, q, :, hh, head].reshape(QUARTER, 128) for hh in range(2) for head in range(8)]
            cols[t, pl.ds(pl.multiple_of(q * QUARTER, QUARTER), QUARTER)] = jnp.dot(
                jnp.concatenate(rows, axis=1), w_ref[...], preferred_element_type=F32)
            send_on(t, [q])

    sent = plane_gather(own, full, ssem, rsem, dsend, drecv, row_done=project)
    for k in range(4):
        pass_on(k)
    for q in range(4):
        rows = pl.ds(q * QUARTER, QUARTER)
        sendx(2, x, q).wait_recv()
        sendx(1, x, q).wait_recv()
        proj_ref[rows] = (cols[x, rows] + nextx[rows] + nearx[rows]).astype(BF16)

    for kind in range(3):
        for q in range(4):
            sendx(kind, x, q).wait_send()
    for copy in sent:
        copy.wait_send()

    def drain(k, carry):
        hh, ob = k % 2, k // 2
        for oa in range(4):
            zt, yt = spot(hh, step_of(oa), step_of(ob))
            swap(hh, zt, yt).wait_send()
        for kind in range(3):
            send1(kind, hh, ob, z, y).wait_send()
        return carry

    lax.fori_loop(0, 8, drain, 0)

    def drain2(hh, carry):
        for kind in range(3):
            send2(kind, hh, z, y).wait_send()
        return carry

    lax.fori_loop(0, 2, drain2, 0)


def finish(parts, weight, rows):
    unit = (33, 8, 128)
    dma = pltpu.SemaphoreType.DMA
    return pl.pallas_call(
        finish_kernel,
        out_shape=(
            jax.ShapeDtypeStruct((rows, 16, 128), BF16),
            jax.ShapeDtypeStruct((256, weight.shape[1]), BF16),
        ),
        in_specs=[VMEM, VMEM],
        out_specs=(VMEM, VMEM),
        scratch_shapes=[
            pltpu.VMEM((2, 4, 4) + unit, F32),
            pltpu.VMEM((2, 4, 4) + unit, F32),
            pltpu.VMEM((2, 4) + unit, F32),
            pltpu.VMEM((2, 4) + unit, F32),
            pltpu.VMEM((2, 4) + unit, F32),
            pltpu.VMEM((2,) + unit, F32),
            pltpu.VMEM((2,) + unit, F32),
            pltpu.VMEM((2,) + unit, F32),
            pltpu.VMEM((2, 32, 8, 128), F32),
            pltpu.VMEM((2, 8, 32, 128), BF16),
            pltpu.VMEM((4, 4, 2, 2, 8, 32, 128), BF16),
            pltpu.VMEM((4, 256, 256), F32),
            pltpu.VMEM((256, 256), F32),
            pltpu.VMEM((256, 256), F32),
            pltpu.VMEM((256, 256), F32),
            dma((2, 4, 4)),
            dma((2, 4, 4)),
            dma((3, 2, 4)),
            dma((3, 2, 4)),
            dma((3, 2)),
            dma((3, 2)),
        ] + gather_sems() + [dma((3, 4)), dma((3, 4))],
        compiler_params=pltpu.CompilerParams(collective_id=1, has_side_effects=True, vmem_limit_bytes=24 << 20),
        name="finish",
    )(parts, weight)


def body(queries, lookup_sheets, content_sheets, page_table, context_len, out_weight):
    req = page_table.shape[0]
    pool, page_len, kv, dim = lookup_sheets.shape
    rows, heads, _ = queries.shape
    all_queries, words = gather_queries(
        *(pltpu.with_memory_space_constraint(a, pltpu.HBM)
          for a in (queries.reshape(2, rows // 2, heads, dim), page_table.T, context_len.reshape(req // 128, 128))),
        pool,
        page_len,
    )
    parts = attend_pages(
        words,
        all_queries.reshape(req, heads, dim),
        lookup_sheets.reshape(pool, page_len * kv, dim),
        content_sheets.reshape(pool, page_len * kv, dim),
    )
    return finish(parts, out_weight, rows)


def solution(mesh):
    finer = Mesh(mesh.devices.reshape(4, 4, 2, mesh.shape["mp"]), ("dp_0", "dp_1", "dp_2", "mp"))
    return jax.shard_map(
        body,
        mesh=finer,
        in_specs=(
            P(DP, "mp", None),
            P(DP, None, "mp", None),
            P(DP, None, "mp", None),
            P(),
            P(),
            P("mp", DP),
        ),
        out_specs=(P(DP, "mp", None), P("mp", DP)),
        check_vma=False,
    )
```

```python
import functools

import jax
import jax.numpy as jnp
from jax import lax
from jax.experimental import pallas as pl
from jax.experimental.pallas import tpu as pltpu
from jax.sharding import Mesh
from jax.sharding import PartitionSpec as P

DP = ("dp_0", "dp_1", "dp_2")
MESH = pl.DeviceIdType.MESH
LOW = -1e30
QUARTER = 64
BATCH = 32
NOTHING = 1056
F32 = jnp.float32
BF16 = jnp.bfloat16
NT = (((1,), (1,)), ((), ()))
VMEM = pl.BlockSpec(memory_space=pltpu.VMEM)
HBM = pl.BlockSpec(memory_space=pltpu.HBM)
SMEM = pl.BlockSpec(memory_space=pltpu.SMEM)


def wrap(value):
    return lax.rem(value + 8, 4)


def place():
    z, y, c = (lax.axis_index(name) for name in DP)
    return z, y, c, 1 - 2 * c


def plane_id(z, y, c):
    return {"dp_0": z, "dp_1": y, "dp_2": c}


def greet(devices):
    barrier = pltpu.get_barrier_semaphore()
    for device in devices:
        pl.semaphore_signal(barrier, inc=1, device_id=device, device_id_type=MESH)
    pl.semaphore_wait(barrier, len(devices))


def remote(src, dst, send_sem, recv_sem, device):
    return pltpu.make_async_remote_copy(
        src_ref=src,
        dst_ref=dst,
        send_sem=send_sem,
        recv_sem=recv_sem,
        device_id=device,
        device_id_type=MESH,
    )


def plane_gather(own, full, ssem, rsem, dsend, drecv, between=(), row_done=None):
    z, y, c, s = place()
    work = list(between)

    def fill():
        piece = work.pop(0) if work else None
        if piece is not None:
            piece()

    def at(h, a, b):
        return full.at[a, b, c, h] if h == 0 else full.at[b, a, c, h]

    def device(h, a, b):
        return plane_id(a, b, c) if h == 0 else plane_id(b, a, c)

    def mine(h):
        return (z, y) if h == 0 else (y, z)

    sent = []

    def go(h, group, m, src, dst, target):
        copy = remote(src, dst, ssem.at[h, group, m], rsem.at[h, group, m], target)
        copy.start()
        sent.append(copy)

    def come(h, group, m, dst):
        remote(dst, dst, ssem.at[h, group, m], rsem.at[h, group, m], plane_id(z, y, c)).wait_recv()

    def share(h, slot, src, dst):
        copy = remote(src, dst, dsend.at[h, slot], drecv.at[h, slot], plane_id(z, y, 1 - c))
        copy.start()
        sent.append(copy)

    def spread(h, group, slot, src, a, b):
        go(h, group, 0, src, at(h, a, b), device(h, mine(h)[0], wrap(b + s)))
        go(h, group, 1, src, at(h, a, b), device(h, mine(h)[0], wrap(b - s)))

    def first(h):
        a, b = mine(h)
        go(h, 0, 0, own.at[h], at(h, a, b), device(h, wrap(a + s), b))
        go(h, 0, 1, own.at[h], at(h, a, b), device(h, wrap(a - s), b))
        go(h, 0, 2, own.at[h], at(h, a, b), device(h, wrap(a + 2), b))

    for h in range(2):
        first(h)
    for h in range(2):
        share(h, 0, own.at[h], at(h, *mine(h)))
        spread(h, 1, 0, own.at[h], *mine(h))
    fill()
    for h in range(2):
        a, b = mine(h)
        near = wrap(a - s)
        come(h, 0, 0, at(h, near, b))
        spread(h, 2, 4, at(h, near, b), near, b)
        share(h, 4, at(h, near, b), at(h, near, b))
    for h in range(2):
        a, b = mine(h)
        near = wrap(a + s)
        come(h, 0, 1, at(h, near, b))
        spread(h, 3, 8, at(h, near, b), near, b)
        share(h, 8, at(h, near, b), at(h, near, b))
    fill()
    for h in range(2):
        a, b = mine(h)
        far = wrap(a + 2)
        come(h, 0, 2, at(h, far, b))
        spread(h, 4, 12, at(h, far, b), far, b)
        share(h, 12, at(h, far, b), at(h, far, b))
    fill()
    steps = (0, 0, -1, 1, 2)

    def near(group):
        for h in range(2):
            a, b = mine(h)
            row = wrap(a + steps[group] * s)
            side = wrap(b - s)
            come(h, group, 0, at(h, row, side))
            go(h, group, 2, at(h, row, side), at(h, row, side), device(h, a, wrap(b + s)))
            share(h, 4 * (group - 1) + 1, at(h, row, side), at(h, row, side))
        fill()

    def other(group):
        for h in range(2):
            a, b = mine(h)
            row = wrap(a + steps[group] * s)
            side = wrap(b + s)
            come(h, group, 1, at(h, row, side))
            share(h, 4 * (group - 1) + 2, at(h, row, side), at(h, row, side))

    def far(group):
        for h in range(2):
            a, b = mine(h)
            row = wrap(a + steps[group] * s)
            opposite = wrap(b + 2)
            come(h, group, 2, at(h, row, opposite))
            share(h, 4 * (group - 1) + 3, at(h, row, opposite), at(h, row, opposite))

    across = (0, 2, 1, 3)

    def from_pair(k, n):
        for h, slot in ((0, 4 * across[k] + across[n]), (1, 4 * across[n] + across[k])):
            where = full.at[0, 0, 1 - c, h]
            remote(where, where, dsend.at[h, slot], drecv.at[h, slot], plane_id(z, y, 1 - c)).wait_recv()

    def arrived(k, columns=(0, 1, 2, 3)):
        for n in columns:
            from_pair(k, n)
        if row_done is not None:
            row_done(k, columns)

    near(1)
    near(2)
    other(1)
    near(3)
    other(2)
    near(4)
    other(3)
    other(4)
    far(1)
    if row_done is not None:
        arrived(0)
    far(2)
    far(3)
    if row_done is not None:
        arrived(1)
        arrived(2)
    far(4)
    if row_done is not None:
        arrived(3, (0, 1, 2))
        arrived(3, (3,))
    else:
        for k in range(4):
            arrived(k)
    return sent


def gather_sems():
    return [
        pltpu.SemaphoreType.DMA((2, 5, 3)),
        pltpu.SemaphoreType.DMA((2, 5, 3)),
        pltpu.SemaphoreType.DMA((2, 16)),
        pltpu.SemaphoreType.DMA((2, 16)),
    ]


def queries_kernel(pool_bits, page_len, q_hbm, table_hbm, len_hbm, full_ref, list_ref,
                   table_ref, len_ref, lo_ref, hi_ref, part_ref, total_ref, lsem, ssem, rsem, dsend, drecv):
    z, y, c, s = place()
    me = (z * 4 + y) * 2 + c
    loads = [
        pltpu.make_async_copy(src, dst, lsem.at[n])
        for n, (src, dst) in enumerate(
            ((q_hbm, full_ref.at[z, y, c]), (table_hbm, table_ref), (len_hbm, len_ref)))
    ]
    for load in loads:
        load.start()
    greet([plane_id(wrap(z + 1), y, c), plane_id(wrap(z - 1), y, c), plane_id(z, wrap(y + 1), c),
           plane_id(z, wrap(y - 1), c), plane_id(wrap(z + 2), y, c), plane_id(z, wrap(y + 2), c), plane_id(z, y, 1 - c)])
    loads[0].wait()

    def place_pages():
        for load in loads[1:]:
            load.wait()
        slots = table_ref.shape[0]
        slot = lax.broadcasted_iota(jnp.int32, (slots, 128), 0)
        lane = lax.broadcasted_iota(jnp.int32, (slots, 128), 1)
        blocks = table_ref.shape[1] // 128
        mine, tokens, page, owner = [], [], [], []
        for t in range(blocks):
            ids = table_ref[:, t * 128:(t + 1) * 128]
            length = jnp.broadcast_to(len_ref[t:t + 1, :], (slots, 128))
            left = jnp.clip(length - slot * page_len, 0, page_len)
            mine.append(jnp.where(((ids >> pool_bits) == me) & (left > 0), 1.0, 0.0))
            tokens.append(left)
            page.append(ids & ((1 << pool_bits) - 1))
            owner.append(lane + t * 128)
        mine, tokens, page, owner = (jnp.concatenate(v, axis=0) for v in (mine, tokens, page, owner))
        rows = slots * blocks
        mine_h = mine.astype(BF16)
        i = lax.broadcasted_iota(jnp.int32, (rows, rows), 0)
        j = lax.broadcasted_iota(jnp.int32, (rows, rows), 1)
        same = (i // slots) == (j // slots)

        def count(which, what):
            return jnp.dot(jnp.where(which, 1.0, 0.0).astype(BF16), what, preferred_element_type=F32)

        earlier = count(same & (j < i), mine_h)
        column = count(same, mine_h)
        blocks_before = count((j // slots) < (i // slots), mine_h)
        i = lax.broadcasted_iota(jnp.int32, (128, 128), 0)
        j = lax.broadcasted_iota(jnp.int32, (128, 128), 1)
        ahead = jnp.where(i < j, 1.0, 0.0).astype(BF16)
        every = jnp.ones((128, 128), BF16)
        start = jnp.dot(column.astype(BF16), ahead, preferred_element_type=F32)
        start = start + jnp.dot(blocks_before.astype(BF16), every, preferred_element_type=F32)
        rank = (start + earlier).astype(jnp.int32)
        lo_ref[...] = jnp.where(mine > 0.0, rank & 127, -1)
        hi_ref[...] = jnp.where(mine > 0.0, rank >> 7, -1)
        part_ref[0] = (page & 255).astype(F32)
        part_ref[1] = (owner & 255).astype(F32)
        part_ref[2] = ((page >> 8) + ((owner >> 8) << 2) + ((tokens - 1) << 4)).astype(F32)
        part_ref[3] = jnp.where(earlier > 0.0, 0.0, 1.0)
        last = jnp.where(column > 0.0, start + column - 1.0, float(NOTHING)).astype(jnp.int32)
        list_ref[8:16, :] = jnp.concatenate([last[t * slots:t * slots + 1] for t in range(blocks)], axis=0)
        number = (start + column)[rows - 1:rows, 127:128]
        list_ref[16:24, :] = jnp.broadcast_to(number, (8, 128)).astype(jnp.int32)
        total_ref[...] = jnp.zeros_like(total_ref)

    sub = lax.broadcasted_iota(jnp.int32, (128, 128), 0).astype(F32).astype(BF16)
    one, nil = jnp.ones((128, 128), BF16), jnp.zeros((128, 128), BF16)
    sub8 = lax.broadcasted_iota(jnp.int32, (8, 128), 0)

    def scatter(part):
        def step(n, carry):
            base = pl.multiple_of(n * 8, 8)
            lo8 = lo_ref[pl.ds(base, 8), :].astype(F32)
            hi8 = hi_ref[pl.ds(base, 8), :]
            p8 = [part_ref[k, pl.ds(base, 8), :] for k in range(4)]
            wide, tall = [], []
            for r in range(8):
                wide.append(jnp.where(sub == jnp.broadcast_to(lo8[r:r + 1, :], (128, 128)).astype(BF16), one, nil))
                hit = sub8 == hi8[r:r + 1, :]
                tall.append(jnp.concatenate(
                    [jnp.where(hit, p8[k][r:r + 1, :], 0.0) for k in range(4)], axis=0).astype(BF16))
            wide = jnp.concatenate(wide, axis=1)
            tall = jnp.concatenate(tall, axis=1)
            total_ref[...] += lax.dot_general(wide, tall, NT, preferred_element_type=F32)
            return carry

        steps = lo_ref.shape[0] // 32
        lax.fori_loop(part * steps, (part + 1) * steps, step, 0)

    def write_list():
        total = jnp.concatenate([total_ref[...], jnp.zeros((128, 96), F32)], axis=1).T.astype(jnp.int32)
        p0, p1, p2, p3 = (total[8 * k:8 * k + 8, :] for k in range(4))
        page = p0 + ((p2 & 3) << 8)
        owner = p1 + (((p2 >> 2) & 3) << 8)
        tokens = (p2 >> 4) + 1
        list_ref[0:8, :] = page + (owner << 10) + (tokens << 20) + (p3 << 25)

    def start_list():
        place_pages()
        scatter(0)

    def end_list():
        scatter(3)
        write_list()

    pieces = [start_list, None, functools.partial(scatter, 1), None, functools.partial(scatter, 2), None, end_list]
    for copy in plane_gather(full_ref.at[z, y, c], full_ref, ssem, rsem, dsend, drecv, between=pieces):
        copy.wait_send()


def gather_queries(queries, table, lengths, pool, page_len):
    req = table.shape[1]
    rows = table.shape[0] * req // 128
    _, half, heads, dim = queries.shape
    return pl.pallas_call(
        functools.partial(queries_kernel, pool.bit_length() - 1, page_len),
        out_shape=(
            jax.ShapeDtypeStruct((4, 4, 2, 2, half, heads, dim), BF16),
            jax.ShapeDtypeStruct((24, 128), jnp.int32),
        ),
        in_specs=[HBM] * 3,
        out_specs=(VMEM, VMEM),
        scratch_shapes=[
            pltpu.VMEM(table.shape, jnp.int32),
            pltpu.VMEM(lengths.shape, jnp.int32),
            pltpu.VMEM((rows, 128), jnp.int32),
            pltpu.VMEM((rows, 128), jnp.int32),
            pltpu.VMEM((4, rows, 128), F32),
            pltpu.VMEM((128, 32), F32),
            pltpu.SemaphoreType.DMA((3,)),
        ] + gather_sems(),
        compiler_params=pltpu.CompilerParams(collective_id=0, has_side_effects=True, vmem_limit_bytes=8 << 20),
        cost_estimate=pl.CostEstimate(flops=10**10, bytes_accessed=1 << 23, transcendentals=0),
        name="gather_queries",
    )(queries, table, lengths)


def pages_kernel(scale, list_ref, q_ref, k_ref, v_ref, acc_ref, sum_ref, top_ref, wait_ref, peak_ref, mass_ref):
    lane = lax.broadcasted_iota(jnp.int32, (16, 128), 1)
    blank = jnp.where(lane < 32, LOW, 0.0)
    zero = jnp.zeros((16, 128), F32)
    sum_ref[NOTHING] = zero
    top_ref[NOTHING] = blank
    wait_ref[...] = jnp.zeros_like(wait_ref)
    peak_ref[...] = jnp.zeros_like(peak_ref)
    mass_ref[...] = jnp.zeros_like(mass_ref)

    i = lax.broadcasted_iota(jnp.int32, (16, 128), 0)
    kv_match = (i // 8) == (lane % 2)
    token = (lane % 32) // 2
    token_of = [jnp.where(kv_match & (lane // 32 == n), token, 1 << 20) for n in range(4)]

    def entry(base, e):
        word = list_ref[base // 128, base % 128 + e]
        return word & 1023, (word >> 10) & 1023, (word >> 20) & 31, (word >> 25) & 1

    def step(n, carry):
        past = jnp.maximum(n - 1, 0) * BATCH
        base = n * BATCH
        before = [entry(past, e) for e in range(BATCH)]
        now = [entry(base, e) for e in range(BATCH)]
        outs, scores = [], []
        for g in range(BATCH // 4):
            four = slice(4 * g, 4 * g + 4)
            vs = jnp.concatenate([v_ref[p] for p, _, _, _ in before[four]], axis=0)
            outs.append(jnp.dot(wait_ref[g], vs, preferred_element_type=F32))
            qs = jnp.concatenate([q_ref[r] for _, r, _, _ in now[four]], axis=0)
            ks = jnp.concatenate([k_ref[p] for p, _, _, _ in now[four]], axis=0)
            scores.append(lax.dot_general(qs, ks, NT, preferred_element_type=F32))
        top, mass, acc = carry
        for e, (_, _, _, first) in enumerate(before):
            old = jnp.where(first == 1, LOW, top)
            p = peak_ref[e]
            top = jnp.maximum(old, p)
            f_old = jnp.exp(old - top)
            f_new = jnp.exp(p - top)
            mass = mass * f_old + mass_ref[e] * f_new
            acc = acc * f_old + outs[e // 4][16 * (e % 4):16 * (e % 4) + 16] * f_new
            sum_ref[past + e] = acc
            top_ref[past + e] = jnp.where(lane < 32, top, mass)
        for g in range(BATCH // 4):
            weights = []
            for e in range(4):
                valid = token_of[e] < now[4 * g + e][2]
                sc = jnp.where(valid, scores[g][16 * e:16 * e + 16] * scale, LOW)
                peak = jnp.max(sc, axis=1, keepdims=True)
                w = jnp.where(valid, jnp.exp(sc - peak), 0.0)
                peak_ref[4 * g + e] = jnp.broadcast_to(peak, (16, 128))
                mass_ref[4 * g + e] = jnp.broadcast_to(jnp.sum(w, axis=1, keepdims=True), (16, 128))
                weights.append(w)
            wait_ref[g] = jnp.concatenate(weights, axis=0).astype(BF16)
        return top, mass, acc

    batches = (list_ref[16, 0] + BATCH - 1) // BATCH
    lax.fori_loop(0, batches + 1, step, (zero, zero, zero))

    def spread(d, carry):
        tops = blank
        line, first = 8 + d // 4, (d % 4) * 32
        for row in range(32):
            last = list_ref[line, first + row]
            acc = sum_ref[last]
            tops = jnp.where((lane == row) | (lane == row + 32), top_ref[last], tops)
            for hh in range(2):
                acc_ref[hh, d, row] = acc[8 * hh:8 * hh + 8]
        for hh in range(2):
            acc_ref[hh, d, 32] = tops[8 * hh:8 * hh + 8]
        return carry

    lax.fori_loop(0, acc_ref.shape[1], spread, 0)


def attend_pages(words, all_queries, keys, values):
    req, heads, dim = all_queries.shape
    return pl.pallas_call(
        functools.partial(pages_kernel, dim ** (-0.5)),
        out_shape=jax.ShapeDtypeStruct((2, req // 32, 33, 8, 128), F32),
        in_specs=[SMEM, VMEM, VMEM, VMEM],
        out_specs=VMEM,
        scratch_shapes=[
            pltpu.VMEM((NOTHING + 1, heads, dim), F32),
            pltpu.VMEM((NOTHING + 1, heads, dim), F32),
            pltpu.VMEM((BATCH // 4, 4 * heads, dim), BF16),
            pltpu.VMEM((BATCH, heads, dim), F32),
            pltpu.VMEM((BATCH, heads, dim), F32),
        ],
        compiler_params=pltpu.CompilerParams(vmem_limit_bytes=20 << 20),
        name="attend_pages",
    )(words, all_queries, keys, values)


def merge(dst, one, other):
    lane = lax.broadcasted_iota(jnp.int32, (8, 128), 1)
    t1, t2 = one[32], other[32]
    top = jnp.maximum(t1, t2)
    f1 = jnp.exp(t1 - top)
    f2 = jnp.exp(t2 - top)
    mass = t1 * pltpu.roll(f1, 32, 1) + t2 * pltpu.roll(f2, 32, 1)
    for row in range(32):
        dst[row] = one[row] * f1[:, row:row + 1] + other[row] * f2[:, row:row + 1]
    dst[32] = jnp.where(lane < 32, top, mass)


def finish_kernel(part_ref, w_ref, att_ref, proj_ref, unit, pair, far1, near1, next1, far2, near2, next2,
                  tmp, own, full, cols, farx, nearx, nextx,
                  s0, r0, s1, r1, s2, r2, ssem, rsem, dsend, drecv, sx, rx):
    z, y, c, s = place()
    x = lax.axis_index("mp")
    home = plane_id(z, y, c)
    greet([plane_id(wrap(z + 1), y, c), plane_id(wrap(z - 1), y, c), plane_id(z, wrap(y + 1), c),
           plane_id(z, wrap(y - 1), c), plane_id(wrap(z + 2), y, c), plane_id(z, wrap(y + 2), c), plane_id(z, y, 1 - c), {"mp": wrap(x + 1)}, {"mp": wrap(x - 1)}])

    def spot(hh, oa, ob):
        dz = oa + hh * (ob - oa)
        dy = ob + hh * (oa - ob)
        return wrap(z + dz), wrap(y + dy)

    def step_of(n):
        m = n % 3
        return 2 * ((3 - n) // 3) + s * (m * (5 - 3 * m) // 2)

    def swap(hh, zt, yt):
        return remote(part_ref.at[hh, (zt * 4 + yt) * 2 + 1 - c], pair.at[hh, zt, yt], s0.at[hh, zt, yt],
                      r0.at[hh, zt, yt], plane_id(z, y, 1 - c))

    def hop(hh, sign):
        zt, yt = spot(hh, sign * s, 0)
        return plane_id(zt, yt, c)

    def hop2(hh, sign):
        zt, yt = spot(hh, 0, sign * s)
        return plane_id(zt, yt, c)

    def far_place(n):
        m, odd = (n + 1) // 2, n % 2
        return wrap(z + step_of((1 - odd) * m)), wrap(y + step_of(odd * m))

    def rest_place(n):
        m, k = n // 3, n % 3
        return wrap(z + step_of(2 - m + 3 * (m // 2))), wrap(y + step_of(2 - k + 3 * (k // 2)))

    def give(where):
        def step(n, carry):
            zt, yt = where(n)
            for hh in range(2):
                swap(hh, zt, yt).start()
            return carry
        return step

    def send1(kind, hh, ob, zt, yt):
        dst = (far1, near1, next1)[kind].at[hh, ob]
        return remote(unit.at[hh, zt, yt], dst, s1.at[kind, hh, ob], r1.at[kind, hh, ob], hop(hh, 1 if kind < 2 else -1))

    def both_cores(hh, zt, yt):
        swap(hh, zt, yt).wait_recv()
        merge(unit.at[hh, zt, yt], part_ref.at[hh, (zt * 4 + yt) * 2 + c], pair.at[hh, zt, yt])

    def far_units(k, carry):
        hh, ob = k % 2, k // 2
        zt, yt = spot(hh, 2, step_of(ob))
        both_cores(hh, zt, yt)
        send1(0, hh, ob, zt, yt).start()
        return carry

    def next_units(k, carry):
        hh, ob = k % 2, k // 2
        zt, yt = spot(hh, -s, step_of(ob))
        both_cores(hh, zt, yt)
        send1(2, hh, ob, zt, yt).start()
        return carry

    def near_units(k, carry):
        hh, ob = k % 2, k // 2
        zt, yt = spot(hh, s, step_of(ob))
        both_cores(hh, zt, yt)
        send1(0, hh, ob, zt, yt).wait_recv()
        merge(unit.at[hh, zt, yt], unit.at[hh, zt, yt], far1.at[hh, ob])
        send1(1, hh, ob, zt, yt).start()
        return carry

    def own_units(k, carry):
        hh, ob = k % 2, k // 2
        zt, yt = spot(hh, 0, step_of(ob))
        both_cores(hh, zt, yt)
        return carry

    lax.fori_loop(0, 7, give(far_place), 0)
    lax.fori_loop(0, 9, give(rest_place), 0)
    lax.fori_loop(0, 8, far_units, 0)
    lax.fori_loop(0, 8, next_units, 0)
    lax.fori_loop(0, 8, near_units, 0)
    lax.fori_loop(0, 8, own_units, 0)

    def send2(kind, hh, zt, yt):
        dst = (far2, near2, next2)[kind].at[hh]
        return remote(unit.at[hh, zt, yt], dst, s2.at[kind, hh], r2.at[kind, hh], hop2(hh, 1 if kind < 2 else -1))

    def gathered(hh, ob):
        zt, yt = spot(hh, 0, step_of(ob))
        send1(2, hh, ob, zt, yt).wait_recv()
        merge(unit.at[hh, zt, yt], unit.at[hh, zt, yt], next1.at[hh, ob])
        send1(1, hh, ob, zt, yt).wait_recv()
        merge(unit.at[hh, zt, yt], unit.at[hh, zt, yt], near1.at[hh, ob])
        return zt, yt

    def far_blocks(hh, carry):
        zt, yt = gathered(hh, 0)
        send2(0, hh, zt, yt).start()
        return carry

    def next_blocks(hh, carry):
        zt, yt = gathered(hh, 2)
        send2(2, hh, zt, yt).start()
        return carry

    def near_blocks(hh, carry):
        zt, yt = gathered(hh, 1)
        send2(0, hh, zt, yt).wait_recv()
        merge(unit.at[hh, zt, yt], unit.at[hh, zt, yt], far2.at[hh])
        send2(1, hh, zt, yt).start()
        return carry

    def own_blocks(hh, carry):
        zt, yt = gathered(hh, 3)
        send2(2, hh, zt, yt).wait_recv()
        merge(unit.at[hh, zt, yt], unit.at[hh, zt, yt], next2.at[hh])
        send2(1, hh, zt, yt).wait_recv()
        merge(unit.at[hh, zt, yt], unit.at[hh, zt, yt], near2.at[hh])
        return carry

    for phase in (far_blocks, next_blocks, near_blocks, own_blocks):
        lax.fori_loop(0, 2, phase, 0)

    masses = [unit[hh, z, y, 32] for hh in range(2)]
    for row in range(32):
        both = [unit[hh, z, y, row] / masses[hh][:, 32 + row:33 + row] for hh in range(2)]
        for hh in range(2):
            tmp[hh, row] = both[hh]
        att_ref[row] = jnp.concatenate(both, axis=0).astype(BF16)
    for hh in range(2):
        for head in range(8):
            own[hh, head] = tmp[hh, :, head, :].astype(BF16)
    for hh in range(2):
        full[z, y, c, hh] = own[hh]

    def sendx(kind, t, q):
        rows = pl.ds(pl.multiple_of(q * QUARTER, QUARTER) if not isinstance(q, int) else q * QUARTER, QUARTER)
        dst = (farx, nearx, nextx)[kind].at[rows]
        return remote(cols.at[t, rows], dst, sx.at[kind, q], rx.at[kind, q],
                      {"mp": wrap(x + (s if kind < 2 else -s))})

    targets = [wrap(z + step) for step in (0, -s, s, 2)]
    columns_of = [wrap(y + step) for step in (0, -s, s, 2)]

    def pass_on(k):
        t = targets[k]

        @pl.when(wrap(t - x - s) == 0)
        def _():
            for q in columns_of:
                rows = pl.ds(pl.multiple_of(q * QUARTER, QUARTER), QUARTER)
                sendx(0, t, q).wait_recv()
                cols[t, rows] = cols[t, rows] + farx[rows]
                sendx(1, t, q).start()

    def send_on(t, quarters):
        @pl.when(wrap(t - x - 2) == 0)
        def _():
            for q in quarters:
                sendx(0, t, q).start()

        @pl.when(wrap(t - x + s) == 0)
        def _():
            for q in quarters:
                sendx(2, t, q).start()

    def project(k, columns):
        t = targets[k]
        if len(columns) == 4:
            rows = [full[t, :, :, hh, head].reshape(256, 128) for hh in range(2) for head in range(8)]
            cols[t] = jnp.dot(jnp.concatenate(rows, axis=1), w_ref[...], preferred_element_type=F32)
            send_on(t, columns_of)
            return
        for n in columns:
            q = columns_of[n]
            rows = [full[t, q, :, hh, head].reshape(QUARTER, 128) for hh in range(2) for head in range(8)]
            cols[t, pl.ds(pl.multiple_of(q * QUARTER, QUARTER), QUARTER)] = jnp.dot(
                jnp.concatenate(rows, axis=1), w_ref[...], preferred_element_type=F32)
            send_on(t, [q])

    sent = plane_gather(own, full, ssem, rsem, dsend, drecv, row_done=project)
    for k in range(4):
        pass_on(k)
    for q in range(4):
        rows = pl.ds(q * QUARTER, QUARTER)
        sendx(2, x, q).wait_recv()
        sendx(1, x, q).wait_recv()
        proj_ref[rows] = (cols[x, rows] + nextx[rows] + nearx[rows]).astype(BF16)

    for kind in range(3):
        for q in range(4):
            sendx(kind, x, q).wait_send()
    for copy in sent:
        copy.wait_send()

    def drain(k, carry):
        hh, ob = k % 2, k // 2
        for oa in range(4):
            zt, yt = spot(hh, step_of(oa), step_of(ob))
            swap(hh, zt, yt).wait_send()
        for kind in range(3):
            send1(kind, hh, ob, z, y).wait_send()
        return carry

    lax.fori_loop(0, 8, drain, 0)

    def drain2(hh, carry):
        for kind in range(3):
            send2(kind, hh, z, y).wait_send()
        return carry

    lax.fori_loop(0, 2, drain2, 0)


def finish(parts, weight, rows):
    unit = (33, 8, 128)
    dma = pltpu.SemaphoreType.DMA
    return pl.pallas_call(
        finish_kernel,
        out_shape=(
            jax.ShapeDtypeStruct((rows, 16, 128), BF16),
            jax.ShapeDtypeStruct((256, weight.shape[1]), BF16),
        ),
        in_specs=[VMEM, VMEM],
        out_specs=(VMEM, VMEM),
        scratch_shapes=[
            pltpu.VMEM((2, 4, 4) + unit, F32),
            pltpu.VMEM((2, 4, 4) + unit, F32),
            pltpu.VMEM((2, 4) + unit, F32),
            pltpu.VMEM((2, 4) + unit, F32),
            pltpu.VMEM((2, 4) + unit, F32),
            pltpu.VMEM((2,) + unit, F32),
            pltpu.VMEM((2,) + unit, F32),
            pltpu.VMEM((2,) + unit, F32),
            pltpu.VMEM((2, 32, 8, 128), F32),
            pltpu.VMEM((2, 8, 32, 128), BF16),
            pltpu.VMEM((4, 4, 2, 2, 8, 32, 128), BF16),
            pltpu.VMEM((4, 256, 256), F32),
            pltpu.VMEM((256, 256), F32),
            pltpu.VMEM((256, 256), F32),
            pltpu.VMEM((256, 256), F32),
            dma((2, 4, 4)),
            dma((2, 4, 4)),
            dma((3, 2, 4)),
            dma((3, 2, 4)),
            dma((3, 2)),
            dma((3, 2)),
        ] + gather_sems() + [dma((3, 4)), dma((3, 4))],
        compiler_params=pltpu.CompilerParams(collective_id=1, has_side_effects=True, vmem_limit_bytes=24 << 20),
        name="finish",
    )(parts, weight)


def body(queries, lookup_sheets, content_sheets, page_table, context_len, out_weight):
    req = page_table.shape[0]
    pool, page_len, kv, dim = lookup_sheets.shape
    rows, heads, _ = queries.shape
    all_queries, words = gather_queries(
        *(pltpu.with_memory_space_constraint(a, pltpu.HBM)
          for a in (queries.reshape(2, rows // 2, heads, dim), page_table.T, context_len.reshape(req // 128, 128))),
        pool,
        page_len,
    )
    parts = attend_pages(
        words,
        all_queries.reshape(req, heads, dim),
        lookup_sheets.reshape(pool, page_len * kv, dim),
        content_sheets.reshape(pool, page_len * kv, dim),
    )
    return finish(parts, out_weight, rows)


def solution(mesh):
    finer = Mesh(mesh.devices.reshape(4, 4, 2, mesh.shape["mp"]), ("dp_0", "dp_1", "dp_2", "mp"))
    return jax.shard_map(
        body,
        mesh=finer,
        in_specs=(
            P(DP, "mp", None),
            P(DP, None, "mp", None),
            P(DP, None, "mp", None),
            P(),
            P(),
            P("mp", DP),
        ),
        out_specs=(P(DP, "mp", None), P("mp", DP)),
        check_vma=False,
    )
```

```python
import functools

import jax
import jax.numpy as jnp
from jax import lax
from jax.experimental import pallas as pl
from jax.experimental.pallas import tpu as pltpu
from jax.sharding import Mesh
from jax.sharding import PartitionSpec as P

DP = ("dp_0", "dp_1", "dp_2")
MESH = pl.DeviceIdType.MESH
LOW = -1e30
QUARTER = 64
BATCH = 32
NOTHING = 1056
F32 = jnp.float32
BF16 = jnp.bfloat16
NT = (((1,), (1,)), ((), ()))
VMEM = pl.BlockSpec(memory_space=pltpu.VMEM)
HBM = pl.BlockSpec(memory_space=pltpu.HBM)
SMEM = pl.BlockSpec(memory_space=pltpu.SMEM)


def wrap(value):
    return lax.rem(value + 8, 4)


def place():
    z, y, c = (lax.axis_index(name) for name in DP)
    return z, y, c, 1 - 2 * c


def plane_id(z, y, c):
    return {"dp_0": z, "dp_1": y, "dp_2": c}


def greet(devices):
    barrier = pltpu.get_barrier_semaphore()
    for device in devices:
        pl.semaphore_signal(barrier, inc=1, device_id=device, device_id_type=MESH)
    pl.semaphore_wait(barrier, len(devices))


def remote(src, dst, send_sem, recv_sem, device):
    return pltpu.make_async_remote_copy(
        src_ref=src,
        dst_ref=dst,
        send_sem=send_sem,
        recv_sem=recv_sem,
        device_id=device,
        device_id_type=MESH,
    )


def plane_gather(own, full, ssem, rsem, dsend, drecv, between=(), row_done=None):
    z, y, c, s = place()
    work = list(between)

    def fill():
        piece = work.pop(0) if work else None
        if piece is not None:
            piece()

    def at(h, a, b):
        return full.at[a, b, c, h] if h == 0 else full.at[b, a, c, h]

    def device(h, a, b):
        return plane_id(a, b, c) if h == 0 else plane_id(b, a, c)

    def mine(h):
        return (z, y) if h == 0 else (y, z)

    sent = []

    def go(h, group, m, src, dst, target):
        copy = remote(src, dst, ssem.at[h, group, m], rsem.at[h, group, m], target)
        copy.start()
        sent.append(copy)

    def come(h, group, m, dst):
        remote(dst, dst, ssem.at[h, group, m], rsem.at[h, group, m], plane_id(z, y, c)).wait_recv()

    def share(h, slot, src, dst):
        copy = remote(src, dst, dsend.at[h, slot], drecv.at[h, slot], plane_id(z, y, 1 - c))
        copy.start()
        sent.append(copy)

    def spread(h, group, slot, src, a, b):
        go(h, group, 0, src, at(h, a, b), device(h, mine(h)[0], wrap(b + s)))
        go(h, group, 1, src, at(h, a, b), device(h, mine(h)[0], wrap(b - s)))

    def first(h):
        a, b = mine(h)
        go(h, 0, 0, own.at[h], at(h, a, b), device(h, wrap(a + s), b))
        go(h, 0, 1, own.at[h], at(h, a, b), device(h, wrap(a - s), b))
        go(h, 0, 2, own.at[h], at(h, a, b), device(h, wrap(a + 2), b))

    for h in range(2):
        first(h)
    for h in range(2):
        share(h, 0, own.at[h], at(h, *mine(h)))
        spread(h, 1, 0, own.at[h], *mine(h))
    fill()
    for h in range(2):
        a, b = mine(h)
        near = wrap(a - s)
        come(h, 0, 0, at(h, near, b))
        spread(h, 2, 4, at(h, near, b), near, b)
        share(h, 4, at(h, near, b), at(h, near, b))
    for h in range(2):
        a, b = mine(h)
        near = wrap(a + s)
        come(h, 0, 1, at(h, near, b))
        spread(h, 3, 8, at(h, near, b), near, b)
        share(h, 8, at(h, near, b), at(h, near, b))
    fill()
    for h in range(2):
        a, b = mine(h)
        far = wrap(a + 2)
        come(h, 0, 2, at(h, far, b))
        spread(h, 4, 12, at(h, far, b), far, b)
        share(h, 12, at(h, far, b), at(h, far, b))
    fill()
    steps = (0, 0, -1, 1, 2)

    def near(group):
        for h in range(2):
            a, b = mine(h)
            row = wrap(a + steps[group] * s)
            side = wrap(b - s)
            come(h, group, 0, at(h, row, side))
            go(h, group, 2, at(h, row, side), at(h, row, side), device(h, a, wrap(b + s)))
            share(h, 4 * (group - 1) + 1, at(h, row, side), at(h, row, side))
        fill()

    def other(group):
        for h in range(2):
            a, b = mine(h)
            row = wrap(a + steps[group] * s)
            side = wrap(b + s)
            come(h, group, 1, at(h, row, side))
            share(h, 4 * (group - 1) + 2, at(h, row, side), at(h, row, side))

    def far(group):
        for h in range(2):
            a, b = mine(h)
            row = wrap(a + steps[group] * s)
            opposite = wrap(b + 2)
            come(h, group, 2, at(h, row, opposite))
            share(h, 4 * (group - 1) + 3, at(h, row, opposite), at(h, row, opposite))

    across = (0, 2, 1, 3)

    def from_pair(k, n):
        for h, slot in ((0, 4 * across[k] + across[n]), (1, 4 * across[n] + across[k])):
            where = full.at[0, 0, 1 - c, h]
            remote(where, where, dsend.at[h, slot], drecv.at[h, slot], plane_id(z, y, 1 - c)).wait_recv()

    def arrived(k, columns=(0, 1, 2, 3)):
        for n in columns:
            from_pair(k, n)
        if row_done is not None:
            row_done(k, columns)

    near(1)
    near(2)
    other(1)
    near(3)
    other(2)
    near(4)
    other(3)
    other(4)
    far(1)
    if row_done is not None:
        arrived(0)
    far(2)
    far(3)
    if row_done is not None:
        arrived(1)
        arrived(2)
    far(4)
    if row_done is not None:
        arrived(3, (0, 1, 2))
        arrived(3, (3,))
    else:
        for k in range(4):
            arrived(k)
    return sent


def gather_sems():
    return [
        pltpu.SemaphoreType.DMA((2, 5, 3)),
        pltpu.SemaphoreType.DMA((2, 5, 3)),
        pltpu.SemaphoreType.DMA((2, 16)),
        pltpu.SemaphoreType.DMA((2, 16)),
    ]


def queries_kernel(pool_bits, page_len, q_hbm, table_hbm, len_hbm, full_ref, list_ref,
                   table_ref, len_ref, lo_ref, hi_ref, part_ref, total_ref, lsem, ssem, rsem, dsend, drecv):
    z, y, c, s = place()
    me = (z * 4 + y) * 2 + c
    loads = [
        pltpu.make_async_copy(src, dst, lsem.at[n])
        for n, (src, dst) in enumerate(
            ((q_hbm, full_ref.at[z, y, c]), (table_hbm, table_ref), (len_hbm, len_ref)))
    ]
    for load in loads:
        load.start()
    greet([plane_id(wrap(z + 1), y, c), plane_id(wrap(z - 1), y, c), plane_id(z, wrap(y + 1), c),
           plane_id(z, wrap(y - 1), c), plane_id(wrap(z + 2), y, c), plane_id(z, wrap(y + 2), c), plane_id(z, y, 1 - c)])
    loads[0].wait()

    def place_pages():
        for load in loads[1:]:
            load.wait()
        slots = table_ref.shape[0]
        slot = lax.broadcasted_iota(jnp.int32, (slots, 128), 0)
        lane = lax.broadcasted_iota(jnp.int32, (slots, 128), 1)
        blocks = table_ref.shape[1] // 128
        mine, tokens, page, owner = [], [], [], []
        for t in range(blocks):
            ids = table_ref[:, t * 128:(t + 1) * 128]
            length = jnp.broadcast_to(len_ref[t:t + 1, :], (slots, 128))
            left = jnp.clip(length - slot * page_len, 0, page_len)
            mine.append(jnp.where(((ids >> pool_bits) == me) & (left > 0), 1.0, 0.0))
            tokens.append(left)
            page.append(ids & ((1 << pool_bits) - 1))
            owner.append(lane + t * 128)
        mine, tokens, page, owner = (jnp.concatenate(v, axis=0) for v in (mine, tokens, page, owner))
        rows = slots * blocks
        mine_h = mine.astype(BF16)
        i = lax.broadcasted_iota(jnp.int32, (rows, rows), 0)
        j = lax.broadcasted_iota(jnp.int32, (rows, rows), 1)
        same = (i // slots) == (j // slots)

        def count(which, what):
            return jnp.dot(jnp.where(which, 1.0, 0.0).astype(BF16), what, preferred_element_type=F32)

        earlier = count(same & (j < i), mine_h)
        column = count(same, mine_h)
        blocks_before = count((j // slots) < (i // slots), mine_h)
        i = lax.broadcasted_iota(jnp.int32, (128, 128), 0)
        j = lax.broadcasted_iota(jnp.int32, (128, 128), 1)
        ahead = jnp.where(i < j, 1.0, 0.0).astype(BF16)
        every = jnp.ones((128, 128), BF16)
        start = jnp.dot(column.astype(BF16), ahead, preferred_element_type=F32)
        start = start + jnp.dot(blocks_before.astype(BF16), every, preferred_element_type=F32)
        rank = (start + earlier).astype(jnp.int32)
        lo_ref[...] = jnp.where(mine > 0.0, rank & 127, -1)
        hi_ref[...] = jnp.where(mine > 0.0, rank >> 7, -1)
        part_ref[0] = (page & 255).astype(F32)
        part_ref[1] = (owner & 255).astype(F32)
        part_ref[2] = ((page >> 8) + ((owner >> 8) << 2) + ((tokens - 1) << 4)).astype(F32)
        part_ref[3] = jnp.where(earlier > 0.0, 0.0, 1.0)
        last = jnp.where(column > 0.0, start + column - 1.0, float(NOTHING)).astype(jnp.int32)
        list_ref[8:16, :] = jnp.concatenate([last[t * slots:t * slots + 1] for t in range(blocks)], axis=0)
        number = (start + column)[rows - 1:rows, 127:128]
        list_ref[16:24, :] = jnp.broadcast_to(number, (8, 128)).astype(jnp.int32)
        total_ref[...] = jnp.zeros_like(total_ref)

    sub = lax.broadcasted_iota(jnp.int32, (128, 128), 0).astype(F32).astype(BF16)
    one, nil = jnp.ones((128, 128), BF16), jnp.zeros((128, 128), BF16)
    sub8 = lax.broadcasted_iota(jnp.int32, (8, 128), 0)

    def scatter(part):
        def step(n, carry):
            base = pl.multiple_of(n * 8, 8)
            lo8 = lo_ref[pl.ds(base, 8), :].astype(F32)
            hi8 = hi_ref[pl.ds(base, 8), :]
            p8 = [part_ref[k, pl.ds(base, 8), :] for k in range(4)]
            wide, tall = [], []
            for r in range(8):
                wide.append(jnp.where(sub == jnp.broadcast_to(lo8[r:r + 1, :], (128, 128)).astype(BF16), one, nil))
                hit = sub8 == hi8[r:r + 1, :]
                tall.append(jnp.concatenate(
                    [jnp.where(hit, p8[k][r:r + 1, :], 0.0) for k in range(4)], axis=0).astype(BF16))
            wide = jnp.concatenate(wide, axis=1)
            tall = jnp.concatenate(tall, axis=1)
            total_ref[...] += lax.dot_general(wide, tall, NT, preferred_element_type=F32)
            return carry

        steps = lo_ref.shape[0] // 32
        lax.fori_loop(part * steps, (part + 1) * steps, step, 0)

    def write_list():
        total = jnp.concatenate([total_ref[...], jnp.zeros((128, 96), F32)], axis=1).T.astype(jnp.int32)
        p0, p1, p2, p3 = (total[8 * k:8 * k + 8, :] for k in range(4))
        page = p0 + ((p2 & 3) << 8)
        owner = p1 + (((p2 >> 2) & 3) << 8)
        tokens = (p2 >> 4) + 1
        list_ref[0:8, :] = page + (owner << 10) + (tokens << 20) + (p3 << 25)

    def start_list():
        place_pages()
        scatter(0)
        scatter(1)

    pieces = [start_list, None, functools.partial(scatter, 2), functools.partial(scatter, 3), None, None, write_list]
    for copy in plane_gather(full_ref.at[z, y, c], full_ref, ssem, rsem, dsend, drecv, between=pieces):
        copy.wait_send()


def gather_queries(queries, table, lengths, pool, page_len):
    req = table.shape[1]
    rows = table.shape[0] * req // 128
    _, half, heads, dim = queries.shape
    return pl.pallas_call(
        functools.partial(queries_kernel, pool.bit_length() - 1, page_len),
        out_shape=(
            jax.ShapeDtypeStruct((4, 4, 2, 2, half, heads, dim), BF16),
            jax.ShapeDtypeStruct((24, 128), jnp.int32),
        ),
        in_specs=[HBM] * 3,
        out_specs=(VMEM, VMEM),
        scratch_shapes=[
            pltpu.VMEM(table.shape, jnp.int32),
            pltpu.VMEM(lengths.shape, jnp.int32),
            pltpu.VMEM((rows, 128), jnp.int32),
            pltpu.VMEM((rows, 128), jnp.int32),
            pltpu.VMEM((4, rows, 128), F32),
            pltpu.VMEM((128, 32), F32),
            pltpu.SemaphoreType.DMA((3,)),
        ] + gather_sems(),
        compiler_params=pltpu.CompilerParams(collective_id=0, has_side_effects=True, vmem_limit_bytes=8 << 20),
        cost_estimate=pl.CostEstimate(flops=10**10, bytes_accessed=1 << 23, transcendentals=0),
        name="gather_queries",
    )(queries, table, lengths)


def pages_kernel(scale, list_ref, q_ref, k_ref, v_ref, acc_ref, sum_ref, top_ref, wait_ref, peak_ref, mass_ref):
    lane = lax.broadcasted_iota(jnp.int32, (16, 128), 1)
    blank = jnp.where(lane < 32, LOW, 0.0)
    zero = jnp.zeros((16, 128), F32)
    sum_ref[NOTHING] = zero
    top_ref[NOTHING] = blank
    wait_ref[...] = jnp.zeros_like(wait_ref)
    peak_ref[...] = jnp.zeros_like(peak_ref)
    mass_ref[...] = jnp.zeros_like(mass_ref)

    i = lax.broadcasted_iota(jnp.int32, (16, 128), 0)
    kv_match = (i // 8) == (lane % 2)
    token = (lane % 32) // 2
    token_of = [jnp.where(kv_match & (lane // 32 == n), token, 1 << 20) for n in range(4)]

    def entry(base, e):
        word = list_ref[base // 128, base % 128 + e]
        return word & 1023, (word >> 10) & 1023, (word >> 20) & 31, (word >> 25) & 1

    def step(n, carry):
        past = jnp.maximum(n - 1, 0) * BATCH
        base = n * BATCH
        before = [entry(past, e) for e in range(BATCH)]
        now = [entry(base, e) for e in range(BATCH)]
        outs, scores = [], []
        for g in range(BATCH // 4):
            four = slice(4 * g, 4 * g + 4)
            vs = jnp.concatenate([v_ref[p] for p, _, _, _ in before[four]], axis=0)
            outs.append(jnp.dot(wait_ref[g], vs, preferred_element_type=F32))
            qs = jnp.concatenate([q_ref[r] for _, r, _, _ in now[four]], axis=0)
            ks = jnp.concatenate([k_ref[p] for p, _, _, _ in now[four]], axis=0)
            scores.append(lax.dot_general(qs, ks, NT, preferred_element_type=F32))
        top, mass, acc = carry
        for e, (_, _, _, first) in enumerate(before):
            old = jnp.where(first == 1, LOW, top)
            p = peak_ref[e]
            top = jnp.maximum(old, p)
            f_old = jnp.exp(old - top)
            f_new = jnp.exp(p - top)
            mass = mass * f_old + mass_ref[e] * f_new
            acc = acc * f_old + outs[e // 4][16 * (e % 4):16 * (e % 4) + 16] * f_new
            sum_ref[past + e] = acc
            top_ref[past + e] = jnp.where(lane < 32, top, mass)
        for g in range(BATCH // 4):
            weights = []
            for e in range(4):
                valid = token_of[e] < now[4 * g + e][2]
                sc = jnp.where(valid, scores[g][16 * e:16 * e + 16] * scale, LOW)
                peak = jnp.max(sc, axis=1, keepdims=True)
                w = jnp.where(valid, jnp.exp(sc - peak), 0.0)
                peak_ref[4 * g + e] = jnp.broadcast_to(peak, (16, 128))
                mass_ref[4 * g + e] = jnp.broadcast_to(jnp.sum(w, axis=1, keepdims=True), (16, 128))
                weights.append(w)
            wait_ref[g] = jnp.concatenate(weights, axis=0).astype(BF16)
        return top, mass, acc

    batches = (list_ref[16, 0] + BATCH - 1) // BATCH
    lax.fori_loop(0, batches + 1, step, (zero, zero, zero))

    def spread(d, carry):
        tops = blank
        line, first = 8 + d // 4, (d % 4) * 32
        for row in range(32):
            last = list_ref[line, first + row]
            acc = sum_ref[last]
            tops = jnp.where((lane == row) | (lane == row + 32), top_ref[last], tops)
            for hh in range(2):
                acc_ref[hh, d, row] = acc[8 * hh:8 * hh + 8]
        for hh in range(2):
            acc_ref[hh, d, 32] = tops[8 * hh:8 * hh + 8]
        return carry

    lax.fori_loop(0, acc_ref.shape[1], spread, 0)


def attend_pages(words, all_queries, keys, values):
    req, heads, dim = all_queries.shape
    return pl.pallas_call(
        functools.partial(pages_kernel, dim ** (-0.5)),
        out_shape=jax.ShapeDtypeStruct((2, req // 32, 33, 8, 128), F32),
        in_specs=[SMEM, VMEM, VMEM, VMEM],
        out_specs=VMEM,
        scratch_shapes=[
            pltpu.VMEM((NOTHING + 1, heads, dim), F32),
            pltpu.VMEM((NOTHING + 1, heads, dim), F32),
            pltpu.VMEM((BATCH // 4, 4 * heads, dim), BF16),
            pltpu.VMEM((BATCH, heads, dim), F32),
            pltpu.VMEM((BATCH, heads, dim), F32),
        ],
        compiler_params=pltpu.CompilerParams(vmem_limit_bytes=20 << 20),
        name="attend_pages",
    )(words, all_queries, keys, values)


def merge(dst, one, other):
    lane = lax.broadcasted_iota(jnp.int32, (8, 128), 1)
    t1, t2 = one[32], other[32]
    top = jnp.maximum(t1, t2)
    f1 = jnp.exp(t1 - top)
    f2 = jnp.exp(t2 - top)
    mass = t1 * pltpu.roll(f1, 32, 1) + t2 * pltpu.roll(f2, 32, 1)
    for row in range(32):
        dst[row] = one[row] * f1[:, row:row + 1] + other[row] * f2[:, row:row + 1]
    dst[32] = jnp.where(lane < 32, top, mass)


def finish_kernel(part_ref, w_ref, att_ref, proj_ref, unit, pair, far1, near1, next1, far2, near2, next2,
                  tmp, own, full, cols, farx, nearx, nextx,
                  s0, r0, s1, r1, s2, r2, ssem, rsem, dsend, drecv, sx, rx):
    z, y, c, s = place()
    x = lax.axis_index("mp")
    home = plane_id(z, y, c)
    greet([plane_id(wrap(z + 1), y, c), plane_id(wrap(z - 1), y, c), plane_id(z, wrap(y + 1), c),
           plane_id(z, wrap(y - 1), c), plane_id(wrap(z + 2), y, c), plane_id(z, wrap(y + 2), c), plane_id(z, y, 1 - c), {"mp": wrap(x + 1)}, {"mp": wrap(x - 1)}])

    def spot(hh, oa, ob):
        dz = oa + hh * (ob - oa)
        dy = ob + hh * (oa - ob)
        return wrap(z + dz), wrap(y + dy)

    def step_of(n):
        m = n % 3
        return 2 * ((3 - n) // 3) + s * (m * (5 - 3 * m) // 2)

    def swap(hh, zt, yt):
        return remote(part_ref.at[hh, (zt * 4 + yt) * 2 + 1 - c], pair.at[hh, zt, yt], s0.at[hh, zt, yt],
                      r0.at[hh, zt, yt], plane_id(z, y, 1 - c))

    def hop(hh, sign):
        zt, yt = spot(hh, sign * s, 0)
        return plane_id(zt, yt, c)

    def hop2(hh, sign):
        zt, yt = spot(hh, 0, sign * s)
        return plane_id(zt, yt, c)

    def far_place(n):
        m, odd = (n + 1) // 2, n % 2
        return wrap(z + step_of((1 - odd) * m)), wrap(y + step_of(odd * m))

    def rest_place(n):
        m, k = n // 3, n % 3
        return wrap(z + step_of(2 - m + 3 * (m // 2))), wrap(y + step_of(2 - k + 3 * (k // 2)))

    def give(where):
        def step(n, carry):
            zt, yt = where(n)
            for hh in range(2):
                swap(hh, zt, yt).start()
            return carry
        return step

    def send1(kind, hh, ob, zt, yt):
        dst = (far1, near1, next1)[kind].at[hh, ob]
        return remote(unit.at[hh, zt, yt], dst, s1.at[kind, hh, ob], r1.at[kind, hh, ob], hop(hh, 1 if kind < 2 else -1))

    def both_cores(hh, zt, yt):
        swap(hh, zt, yt).wait_recv()
        merge(unit.at[hh, zt, yt], part_ref.at[hh, (zt * 4 + yt) * 2 + c], pair.at[hh, zt, yt])

    def far_units(k, carry):
        hh, ob = k % 2, k // 2
        zt, yt = spot(hh, 2, step_of(ob))
        both_cores(hh, zt, yt)
        send1(0, hh, ob, zt, yt).start()
        return carry

    def next_units(k, carry):
        hh, ob = k % 2, k // 2
        zt, yt = spot(hh, -s, step_of(ob))
        both_cores(hh, zt, yt)
        send1(2, hh, ob, zt, yt).start()
        return carry

    def near_units(k, carry):
        hh, ob = k % 2, k // 2
        zt, yt = spot(hh, s, step_of(ob))
        both_cores(hh, zt, yt)
        send1(0, hh, ob, zt, yt).wait_recv()
        merge(unit.at[hh, zt, yt], unit.at[hh, zt, yt], far1.at[hh, ob])
        send1(1, hh, ob, zt, yt).start()
        return carry

    def own_units(k, carry):
        hh, ob = k % 2, k // 2
        zt, yt = spot(hh, 0, step_of(ob))
        both_cores(hh, zt, yt)
        return carry

    lax.fori_loop(0, 7, give(far_place), 0)
    lax.fori_loop(0, 9, give(rest_place), 0)
    lax.fori_loop(0, 8, far_units, 0)
    lax.fori_loop(0, 8, next_units, 0)
    lax.fori_loop(0, 8, near_units, 0)
    lax.fori_loop(0, 8, own_units, 0)

    def send2(kind, hh, zt, yt):
        dst = (far2, near2, next2)[kind].at[hh]
        return remote(unit.at[hh, zt, yt], dst, s2.at[kind, hh], r2.at[kind, hh], hop2(hh, 1 if kind < 2 else -1))

    def gathered(hh, ob):
        zt, yt = spot(hh, 0, step_of(ob))
        send1(2, hh, ob, zt, yt).wait_recv()
        merge(unit.at[hh, zt, yt], unit.at[hh, zt, yt], next1.at[hh, ob])
        send1(1, hh, ob, zt, yt).wait_recv()
        merge(unit.at[hh, zt, yt], unit.at[hh, zt, yt], near1.at[hh, ob])
        return zt, yt

    def far_blocks(hh, carry):
        zt, yt = gathered(hh, 0)
        send2(0, hh, zt, yt).start()
        return carry

    def next_blocks(hh, carry):
        zt, yt = gathered(hh, 2)
        send2(2, hh, zt, yt).start()
        return carry

    def near_sums(hh, carry):
        gathered(hh, 1)
        return carry

    def near_blocks(hh, carry):
        zt, yt = spot(hh, 0, s)
        send2(0, hh, zt, yt).wait_recv()
        merge(unit.at[hh, zt, yt], unit.at[hh, zt, yt], far2.at[hh])
        send2(1, hh, zt, yt).start()
        return carry

    def own_blocks(hh, carry):
        zt, yt = gathered(hh, 3)
        send2(2, hh, zt, yt).wait_recv()
        merge(unit.at[hh, zt, yt], unit.at[hh, zt, yt], next2.at[hh])
        send2(1, hh, zt, yt).wait_recv()
        merge(unit.at[hh, zt, yt], unit.at[hh, zt, yt], near2.at[hh])
        return carry

    for phase in (far_blocks, near_sums, next_blocks, near_blocks, own_blocks):
        lax.fori_loop(0, 2, phase, 0)

    masses = [unit[hh, z, y, 32] for hh in range(2)]
    for row in range(32):
        both = [unit[hh, z, y, row] / masses[hh][:, 32 + row:33 + row] for hh in range(2)]
        for hh in range(2):
            tmp[hh, row] = both[hh]
        att_ref[row] = jnp.concatenate(both, axis=0).astype(BF16)
    for hh in range(2):
        for head in range(8):
            own[hh, head] = tmp[hh, :, head, :].astype(BF16)
    for hh in range(2):
        full[z, y, c, hh] = own[hh]

    def sendx(kind, t, q):
        rows = pl.ds(pl.multiple_of(q * QUARTER, QUARTER) if not isinstance(q, int) else q * QUARTER, QUARTER)
        dst = (farx, nearx, nextx)[kind].at[rows]
        return remote(cols.at[t, rows], dst, sx.at[kind, q], rx.at[kind, q],
                      {"mp": wrap(x + (s if kind < 2 else -s))})

    targets = [wrap(z + step) for step in (0, -s, s, 2)]
    columns_of = [wrap(y + step) for step in (0, -s, s, 2)]

    def pass_on(k):
        t = targets[k]

        @pl.when(wrap(t - x - s) == 0)
        def _():
            for q in columns_of:
                rows = pl.ds(pl.multiple_of(q * QUARTER, QUARTER), QUARTER)
                sendx(0, t, q).wait_recv()
                cols[t, rows] = cols[t, rows] + farx[rows]
                sendx(1, t, q).start()

    def send_on(t, quarters):
        @pl.when(wrap(t - x - 2) == 0)
        def _():
            for q in quarters:
                sendx(0, t, q).start()

        @pl.when(wrap(t - x + s) == 0)
        def _():
            for q in quarters:
                sendx(2, t, q).start()

    def project(k, columns):
        t = targets[k]
        if len(columns) == 4:
            rows = [full[t, :, :, hh, head].reshape(256, 128) for hh in range(2) for head in range(8)]
            cols[t] = jnp.dot(jnp.concatenate(rows, axis=1), w_ref[...], preferred_element_type=F32)
            send_on(t, columns_of)
            return
        for n in columns:
            q = columns_of[n]
            rows = [full[t, q, :, hh, head].reshape(QUARTER, 128) for hh in range(2) for head in range(8)]
            cols[t, pl.ds(pl.multiple_of(q * QUARTER, QUARTER), QUARTER)] = jnp.dot(
                jnp.concatenate(rows, axis=1), w_ref[...], preferred_element_type=F32)
            send_on(t, [q])

    sent = plane_gather(own, full, ssem, rsem, dsend, drecv, row_done=project)
    for k in range(4):
        pass_on(k)
    for q in columns_of:
        rows = pl.ds(pl.multiple_of(q * QUARTER, QUARTER), QUARTER)
        sendx(2, x, q).wait_recv()
        sendx(1, x, q).wait_recv()
        proj_ref[rows] = (cols[x, rows] + nextx[rows] + nearx[rows]).astype(BF16)

    for kind in range(3):
        for q in range(4):
            sendx(kind, x, q).wait_send()
    for copy in sent:
        copy.wait_send()

    def drain(k, carry):
        hh, ob = k % 2, k // 2
        for oa in range(4):
            zt, yt = spot(hh, step_of(oa), step_of(ob))
            swap(hh, zt, yt).wait_send()
        for kind in range(3):
            send1(kind, hh, ob, z, y).wait_send()
        return carry

    lax.fori_loop(0, 8, drain, 0)

    def drain2(hh, carry):
        for kind in range(3):
            send2(kind, hh, z, y).wait_send()
        return carry

    lax.fori_loop(0, 2, drain2, 0)


def finish(parts, weight, rows):
    unit = (33, 8, 128)
    dma = pltpu.SemaphoreType.DMA
    return pl.pallas_call(
        finish_kernel,
        out_shape=(
            jax.ShapeDtypeStruct((rows, 16, 128), BF16),
            jax.ShapeDtypeStruct((256, weight.shape[1]), BF16),
        ),
        in_specs=[VMEM, VMEM],
        out_specs=(VMEM, VMEM),
        scratch_shapes=[
            pltpu.VMEM((2, 4, 4) + unit, F32),
            pltpu.VMEM((2, 4, 4) + unit, F32),
            pltpu.VMEM((2, 4) + unit, F32),
            pltpu.VMEM((2, 4) + unit, F32),
            pltpu.VMEM((2, 4) + unit, F32),
            pltpu.VMEM((2,) + unit, F32),
            pltpu.VMEM((2,) + unit, F32),
            pltpu.VMEM((2,) + unit, F32),
            pltpu.VMEM((2, 32, 8, 128), F32),
            pltpu.VMEM((2, 8, 32, 128), BF16),
            pltpu.VMEM((4, 4, 2, 2, 8, 32, 128), BF16),
            pltpu.VMEM((4, 256, 256), F32),
            pltpu.VMEM((256, 256), F32),
            pltpu.VMEM((256, 256), F32),
            pltpu.VMEM((256, 256), F32),
            dma((2, 4, 4)),
            dma((2, 4, 4)),
            dma((3, 2, 4)),
            dma((3, 2, 4)),
            dma((3, 2)),
            dma((3, 2)),
        ] + gather_sems() + [dma((3, 4)), dma((3, 4))],
        compiler_params=pltpu.CompilerParams(collective_id=1, has_side_effects=True, vmem_limit_bytes=24 << 20),
        name="finish",
    )(parts, weight)


def body(queries, lookup_sheets, content_sheets, page_table, context_len, out_weight):
    req = page_table.shape[0]
    pool, page_len, kv, dim = lookup_sheets.shape
    rows, heads, _ = queries.shape
    all_queries, words = gather_queries(
        *(pltpu.with_memory_space_constraint(a, pltpu.HBM)
          for a in (queries.reshape(2, rows // 2, heads, dim), page_table.T, context_len.reshape(req // 128, 128))),
        pool,
        page_len,
    )
    parts = attend_pages(
        words,
        all_queries.reshape(req, heads, dim),
        lookup_sheets.reshape(pool, page_len * kv, dim),
        content_sheets.reshape(pool, page_len * kv, dim),
    )
    return finish(parts, out_weight, rows)


def solution(mesh):
    finer = Mesh(mesh.devices.reshape(4, 4, 2, mesh.shape["mp"]), ("dp_0", "dp_1", "dp_2", "mp"))
    return jax.shard_map(
        body,
        mesh=finer,
        in_specs=(
            P(DP, "mp", None),
            P(DP, None, "mp", None),
            P(DP, None, "mp", None),
            P(),
            P(),
            P("mp", DP),
        ),
        out_specs=(P(DP, "mp", None), P("mp", DP)),
        check_vma=False,
    )
```

```python
import functools

import jax
import jax.numpy as jnp
from jax import lax
from jax.experimental import pallas as pl
from jax.experimental.pallas import tpu as pltpu
from jax.sharding import Mesh
from jax.sharding import PartitionSpec as P

DP = ("dp_0", "dp_1", "dp_2")
MESH = pl.DeviceIdType.MESH
LOW = -1e30
QUARTER = 64
BATCH = 32
NOTHING = 1056
F32 = jnp.float32
BF16 = jnp.bfloat16
NT = (((1,), (1,)), ((), ()))
VMEM = pl.BlockSpec(memory_space=pltpu.VMEM)
HBM = pl.BlockSpec(memory_space=pltpu.HBM)
SMEM = pl.BlockSpec(memory_space=pltpu.SMEM)


def wrap(value):
    return lax.rem(value + 8, 4)


def place():
    z, y, c = (lax.axis_index(name) for name in DP)
    return z, y, c, 1 - 2 * c


def plane_id(z, y, c):
    return {"dp_0": z, "dp_1": y, "dp_2": c}


def greet(devices):
    barrier = pltpu.get_barrier_semaphore()
    for device in devices:
        pl.semaphore_signal(barrier, inc=1, device_id=device, device_id_type=MESH)
    pl.semaphore_wait(barrier, len(devices))


def remote(src, dst, send_sem, recv_sem, device):
    return pltpu.make_async_remote_copy(
        src_ref=src,
        dst_ref=dst,
        send_sem=send_sem,
        recv_sem=recv_sem,
        device_id=device,
        device_id_type=MESH,
    )


def plane_gather(own, full, ssem, rsem, dsend, drecv, between=(), row_done=None):
    z, y, c, s = place()
    work = list(between)

    def fill():
        piece = work.pop(0) if work else None
        if piece is not None:
            piece()

    def at(h, a, b):
        return full.at[a, b, c, h] if h == 0 else full.at[b, a, c, h]

    def device(h, a, b):
        return plane_id(a, b, c) if h == 0 else plane_id(b, a, c)

    def mine(h):
        return (z, y) if h == 0 else (y, z)

    sent = []

    def go(h, group, m, src, dst, target):
        copy = remote(src, dst, ssem.at[h, group, m], rsem.at[h, group, m], target)
        copy.start()
        sent.append(copy)

    def come(h, group, m, dst):
        remote(dst, dst, ssem.at[h, group, m], rsem.at[h, group, m], plane_id(z, y, c)).wait_recv()

    def share(h, slot, src, dst):
        copy = remote(src, dst, dsend.at[h, slot], drecv.at[h, slot], plane_id(z, y, 1 - c))
        copy.start()
        sent.append(copy)

    def spread(h, group, slot, src, a, b):
        go(h, group, 0, src, at(h, a, b), device(h, mine(h)[0], wrap(b + s)))
        go(h, group, 1, src, at(h, a, b), device(h, mine(h)[0], wrap(b - s)))

    def first(h):
        a, b = mine(h)
        go(h, 0, 0, own.at[h], at(h, a, b), device(h, wrap(a + s), b))
        go(h, 0, 1, own.at[h], at(h, a, b), device(h, wrap(a - s), b))
        go(h, 0, 2, own.at[h], at(h, a, b), device(h, wrap(a + 2), b))

    for h in range(2):
        first(h)
    for h in range(2):
        share(h, 0, own.at[h], at(h, *mine(h)))
        spread(h, 1, 0, own.at[h], *mine(h))
    fill()
    for h in range(2):
        a, b = mine(h)
        near = wrap(a - s)
        come(h, 0, 0, at(h, near, b))
        spread(h, 2, 4, at(h, near, b), near, b)
        share(h, 4, at(h, near, b), at(h, near, b))
    for h in range(2):
        a, b = mine(h)
        near = wrap(a + s)
        come(h, 0, 1, at(h, near, b))
        spread(h, 3, 8, at(h, near, b), near, b)
        share(h, 8, at(h, near, b), at(h, near, b))
    fill()
    for h in range(2):
        a, b = mine(h)
        far = wrap(a + 2)
        come(h, 0, 2, at(h, far, b))
        spread(h, 4, 12, at(h, far, b), far, b)
        share(h, 12, at(h, far, b), at(h, far, b))
    fill()
    steps = (0, 0, -1, 1, 2)

    def near(group):
        for h in range(2):
            a, b = mine(h)
            row = wrap(a + steps[group] * s)
            side = wrap(b - s)
            come(h, group, 0, at(h, row, side))
            go(h, group, 2, at(h, row, side), at(h, row, side), device(h, a, wrap(b + s)))
            share(h, 4 * (group - 1) + 1, at(h, row, side), at(h, row, side))
        fill()

    def other(group):
        for h in range(2):
            a, b = mine(h)
            row = wrap(a + steps[group] * s)
            side = wrap(b + s)
            come(h, group, 1, at(h, row, side))
            share(h, 4 * (group - 1) + 2, at(h, row, side), at(h, row, side))

    def far(group):
        for h in range(2):
            a, b = mine(h)
            row = wrap(a + steps[group] * s)
            opposite = wrap(b + 2)
            come(h, group, 2, at(h, row, opposite))
            share(h, 4 * (group - 1) + 3, at(h, row, opposite), at(h, row, opposite))

    across = (0, 2, 1, 3)

    def from_pair(k, n):
        for h, slot in ((0, 4 * across[k] + across[n]), (1, 4 * across[n] + across[k])):
            where = full.at[0, 0, 1 - c, h]
            remote(where, where, dsend.at[h, slot], drecv.at[h, slot], plane_id(z, y, 1 - c)).wait_recv()

    def arrived(k, columns=(0, 1, 2, 3)):
        for n in columns:
            from_pair(k, n)
        if row_done is not None:
            row_done(k, columns)

    near(1)
    near(2)
    other(1)
    near(3)
    other(2)
    near(4)
    other(3)
    other(4)
    far(1)
    if row_done is not None:
        arrived(0)
    far(2)
    far(3)
    if row_done is not None:
        arrived(1)
        arrived(2)
    far(4)
    if row_done is not None:
        arrived(3, (0, 1, 2))
        arrived(3, (3,))
    else:
        for k in range(4):
            arrived(k)
    return sent


def gather_sems():
    return [
        pltpu.SemaphoreType.DMA((2, 5, 3)),
        pltpu.SemaphoreType.DMA((2, 5, 3)),
        pltpu.SemaphoreType.DMA((2, 16)),
        pltpu.SemaphoreType.DMA((2, 16)),
    ]


def queries_kernel(pool_bits, page_len, q_hbm, table_hbm, len_hbm, full_ref, list_ref,
                   table_ref, len_ref, lo_ref, hi_ref, part_ref, total_ref, lsem, ssem, rsem, dsend, drecv):
    z, y, c, s = place()
    me = (z * 4 + y) * 2 + c
    loads = [
        pltpu.make_async_copy(src, dst, lsem.at[n])
        for n, (src, dst) in enumerate(
            ((q_hbm, full_ref.at[z, y, c]), (table_hbm, table_ref), (len_hbm, len_ref)))
    ]
    for load in loads:
        load.start()
    greet([plane_id(wrap(z + 1), y, c), plane_id(wrap(z - 1), y, c), plane_id(z, wrap(y + 1), c),
           plane_id(z, wrap(y - 1), c), plane_id(wrap(z + 2), y, c), plane_id(z, wrap(y + 2), c), plane_id(z, y, 1 - c)])
    loads[0].wait()

    def place_pages():
        for load in loads[1:]:
            load.wait()
        slots = table_ref.shape[0]
        slot = lax.broadcasted_iota(jnp.int32, (slots, 128), 0)
        lane = lax.broadcasted_iota(jnp.int32, (slots, 128), 1)
        blocks = table_ref.shape[1] // 128
        mine, tokens, page, owner = [], [], [], []
        for t in range(blocks):
            ids = table_ref[:, t * 128:(t + 1) * 128]
            length = jnp.broadcast_to(len_ref[t:t + 1, :], (slots, 128))
            left = jnp.clip(length - slot * page_len, 0, page_len)
            mine.append(jnp.where(((ids >> pool_bits) == me) & (left > 0), 1.0, 0.0))
            tokens.append(left)
            page.append(ids & ((1 << pool_bits) - 1))
            owner.append(lane + t * 128)
        mine, tokens, page, owner = (jnp.concatenate(v, axis=0) for v in (mine, tokens, page, owner))
        rows = slots * blocks
        mine_h = mine.astype(BF16)
        i = lax.broadcasted_iota(jnp.int32, (rows, rows), 0)
        j = lax.broadcasted_iota(jnp.int32, (rows, rows), 1)
        same = (i // slots) == (j // slots)

        def count(which, what):
            return jnp.dot(jnp.where(which, 1.0, 0.0).astype(BF16), what, preferred_element_type=F32)

        earlier = count(same & (j < i), mine_h)
        column = count(same, mine_h)
        blocks_before = count((j // slots) < (i // slots), mine_h)
        i = lax.broadcasted_iota(jnp.int32, (128, 128), 0)
        j = lax.broadcasted_iota(jnp.int32, (128, 128), 1)
        ahead = jnp.where(i < j, 1.0, 0.0).astype(BF16)
        every = jnp.ones((128, 128), BF16)
        start = jnp.dot(column.astype(BF16), ahead, preferred_element_type=F32)
        start = start + jnp.dot(blocks_before.astype(BF16), every, preferred_element_type=F32)
        rank = (start + earlier).astype(jnp.int32)
        lo_ref[...] = jnp.where(mine > 0.0, rank & 127, -1)
        hi_ref[...] = jnp.where(mine > 0.0, rank >> 7, -1)
        part_ref[0] = (page & 255).astype(F32)
        part_ref[1] = (owner & 255).astype(F32)
        part_ref[2] = ((page >> 8) + ((owner >> 8) << 2) + ((tokens - 1) << 4)).astype(F32)
        part_ref[3] = jnp.where(earlier > 0.0, 0.0, 1.0)
        last = jnp.where(column > 0.0, start + column - 1.0, float(NOTHING)).astype(jnp.int32)
        list_ref[8:16, :] = jnp.concatenate([last[t * slots:t * slots + 1] for t in range(blocks)], axis=0)
        number = (start + column)[rows - 1:rows, 127:128]
        list_ref[16:24, :] = jnp.broadcast_to(number, (8, 128)).astype(jnp.int32)
        total_ref[...] = jnp.zeros_like(total_ref)

    sub = lax.broadcasted_iota(jnp.int32, (128, 128), 0).astype(F32).astype(BF16)
    one, nil = jnp.ones((128, 128), BF16), jnp.zeros((128, 128), BF16)
    sub8 = lax.broadcasted_iota(jnp.int32, (8, 128), 0)

    def scatter(part):
        def step(n, carry):
            base = pl.multiple_of(n * 8, 8)
            lo8 = lo_ref[pl.ds(base, 8), :].astype(F32)
            hi8 = hi_ref[pl.ds(base, 8), :]
            p8 = [part_ref[k, pl.ds(base, 8), :] for k in range(4)]
            wide, tall = [], []
            for r in range(8):
                wide.append(jnp.where(sub == jnp.broadcast_to(lo8[r:r + 1, :], (128, 128)).astype(BF16), one, nil))
                hit = sub8 == hi8[r:r + 1, :]
                tall.append(jnp.concatenate(
                    [jnp.where(hit, p8[k][r:r + 1, :], 0.0) for k in range(4)], axis=0).astype(BF16))
            wide = jnp.concatenate(wide, axis=1)
            tall = jnp.concatenate(tall, axis=1)
            total_ref[...] += lax.dot_general(wide, tall, NT, preferred_element_type=F32)
            return carry

        steps = lo_ref.shape[0] // 32
        lax.fori_loop(part * steps, (part + 1) * steps, step, 0)

    def write_list():
        total = jnp.concatenate([total_ref[...], jnp.zeros((128, 96), F32)], axis=1).T.astype(jnp.int32)
        p0, p1, p2, p3 = (total[8 * k:8 * k + 8, :] for k in range(4))
        page = p0 + ((p2 & 3) << 8)
        owner = p1 + (((p2 >> 2) & 3) << 8)
        tokens = (p2 >> 4) + 1
        list_ref[0:8, :] = page + (owner << 10) + (tokens << 20) + (p3 << 25)

    def start_list():
        place_pages()
        scatter(0)
        scatter(1)

    pieces = [start_list, None, functools.partial(scatter, 2), functools.partial(scatter, 3), None, None, write_list]
    for copy in plane_gather(full_ref.at[z, y, c], full_ref, ssem, rsem, dsend, drecv, between=pieces):
        copy.wait_send()


def gather_queries(queries, table, lengths, pool, page_len):
    req = table.shape[1]
    rows = table.shape[0] * req // 128
    _, half, heads, dim = queries.shape
    return pl.pallas_call(
        functools.partial(queries_kernel, pool.bit_length() - 1, page_len),
        out_shape=(
            jax.ShapeDtypeStruct((4, 4, 2, 2, half, heads, dim), BF16),
            jax.ShapeDtypeStruct((24, 128), jnp.int32),
        ),
        in_specs=[HBM] * 3,
        out_specs=(VMEM, VMEM),
        scratch_shapes=[
            pltpu.VMEM(table.shape, jnp.int32),
            pltpu.VMEM(lengths.shape, jnp.int32),
            pltpu.VMEM((rows, 128), jnp.int32),
            pltpu.VMEM((rows, 128), jnp.int32),
            pltpu.VMEM((4, rows, 128), F32),
            pltpu.VMEM((128, 32), F32),
            pltpu.SemaphoreType.DMA((3,)),
        ] + gather_sems(),
        compiler_params=pltpu.CompilerParams(collective_id=0, has_side_effects=True, vmem_limit_bytes=8 << 20),
        cost_estimate=pl.CostEstimate(flops=10**10, bytes_accessed=1 << 23, transcendentals=0),
        name="gather_queries",
    )(queries, table, lengths)


def pages_kernel(scale, list_ref, q_ref, k_ref, v_ref, acc_ref, sum_ref, top_ref, wait_ref, peak_ref, mass_ref):
    lane = lax.broadcasted_iota(jnp.int32, (16, 128), 1)
    blank = jnp.where(lane < 32, LOW, 0.0)
    zero = jnp.zeros((16, 128), F32)
    sum_ref[NOTHING] = zero
    top_ref[NOTHING] = blank
    wait_ref[...] = jnp.zeros_like(wait_ref)
    peak_ref[...] = jnp.zeros_like(peak_ref)
    mass_ref[...] = jnp.zeros_like(mass_ref)

    i = lax.broadcasted_iota(jnp.int32, (16, 128), 0)
    kv_match = (i // 8) == (lane % 2)
    token = (lane % 32) // 2
    token_of = [jnp.where(kv_match & (lane // 32 == n), token, 1 << 20) for n in range(4)]

    def entry(base, e):
        word = list_ref[base // 128, base % 128 + e]
        return word & 1023, (word >> 10) & 1023, (word >> 20) & 31, (word >> 25) & 1

    def step(n, carry):
        past = jnp.maximum(n - 1, 0) * BATCH
        base = n * BATCH
        before = [entry(past, e) for e in range(BATCH)]
        now = [entry(base, e) for e in range(BATCH)]
        outs, scores = [], []
        for g in range(BATCH // 4):
            four = slice(4 * g, 4 * g + 4)
            vs = jnp.concatenate([v_ref[p] for p, _, _, _ in before[four]], axis=0)
            outs.append(jnp.dot(wait_ref[g], vs, preferred_element_type=F32))
            qs = jnp.concatenate([q_ref[r] for _, r, _, _ in now[four]], axis=0)
            ks = jnp.concatenate([k_ref[p] for p, _, _, _ in now[four]], axis=0)
            scores.append(lax.dot_general(qs, ks, NT, preferred_element_type=F32))
        top, mass, acc = carry
        for e, (_, _, _, first) in enumerate(before):
            old = jnp.where(first == 1, LOW, top)
            p = peak_ref[e]
            top = jnp.maximum(old, p)
            f_old = jnp.exp(old - top)
            f_new = jnp.exp(p - top)
            mass = mass * f_old + mass_ref[e] * f_new
            acc = acc * f_old + outs[e // 4][16 * (e % 4):16 * (e % 4) + 16] * f_new
            sum_ref[past + e] = acc
            top_ref[past + e] = jnp.where(lane < 32, top, mass)
        for g in range(BATCH // 4):
            weights = []
            for e in range(4):
                valid = token_of[e] < now[4 * g + e][2]
                sc = jnp.where(valid, scores[g][16 * e:16 * e + 16] * scale, LOW)
                peak = jnp.max(sc, axis=1, keepdims=True)
                w = jnp.where(valid, jnp.exp(sc - peak), 0.0)
                peak_ref[4 * g + e] = jnp.broadcast_to(peak, (16, 128))
                mass_ref[4 * g + e] = jnp.broadcast_to(jnp.sum(w, axis=1, keepdims=True), (16, 128))
                weights.append(w)
            wait_ref[g] = jnp.concatenate(weights, axis=0).astype(BF16)
        return top, mass, acc

    batches = (list_ref[16, 0] + BATCH - 1) // BATCH
    lax.fori_loop(0, batches + 1, step, (zero, zero, zero))

    def spread(d, carry):
        tops = blank
        line, first = 8 + d // 4, (d % 4) * 32
        for row in range(32):
            last = list_ref[line, first + row]
            acc = sum_ref[last]
            tops = jnp.where((lane == row) | (lane == row + 32), top_ref[last], tops)
            for hh in range(2):
                acc_ref[hh, d, row] = acc[8 * hh:8 * hh + 8]
        for hh in range(2):
            acc_ref[hh, d, 32] = tops[8 * hh:8 * hh + 8]
        return carry

    lax.fori_loop(0, acc_ref.shape[1], spread, 0)


def attend_pages(words, all_queries, keys, values):
    req, heads, dim = all_queries.shape
    return pl.pallas_call(
        functools.partial(pages_kernel, dim ** (-0.5)),
        out_shape=jax.ShapeDtypeStruct((2, req // 32, 33, 8, 128), F32),
        in_specs=[SMEM, VMEM, VMEM, VMEM],
        out_specs=VMEM,
        scratch_shapes=[
            pltpu.VMEM((NOTHING + 1, heads, dim), F32),
            pltpu.VMEM((NOTHING + 1, heads, dim), F32),
            pltpu.VMEM((BATCH // 4, 4 * heads, dim), BF16),
            pltpu.VMEM((BATCH, heads, dim), F32),
            pltpu.VMEM((BATCH, heads, dim), F32),
        ],
        compiler_params=pltpu.CompilerParams(vmem_limit_bytes=20 << 20),
        name="attend_pages",
    )(words, all_queries, keys, values)


def merge(dst, one, other):
    lane = lax.broadcasted_iota(jnp.int32, (8, 128), 1)
    t1, t2 = one[32], other[32]
    top = jnp.maximum(t1, t2)
    f1 = jnp.exp(t1 - top)
    f2 = jnp.exp(t2 - top)
    mass = t1 * pltpu.roll(f1, 32, 1) + t2 * pltpu.roll(f2, 32, 1)
    for row in range(32):
        dst[row] = one[row] * f1[:, row:row + 1] + other[row] * f2[:, row:row + 1]
    dst[32] = jnp.where(lane < 32, top, mass)


def finish_kernel(part_ref, w_ref, att_ref, proj_ref, unit, pair, far1, near1, next1, far2, near2, next2,
                  tmp, own, full, cols, farx, nearx, nextx,
                  s0, r0, s1, r1, s2, r2, ssem, rsem, dsend, drecv, sx, rx):
    z, y, c, s = place()
    x = lax.axis_index("mp")
    home = plane_id(z, y, c)
    greet([plane_id(wrap(z + 1), y, c), plane_id(wrap(z - 1), y, c), plane_id(z, wrap(y + 1), c),
           plane_id(z, wrap(y - 1), c), plane_id(wrap(z + 2), y, c), plane_id(z, wrap(y + 2), c), plane_id(z, y, 1 - c), {"mp": wrap(x + 1)}, {"mp": wrap(x - 1)}])

    def spot(hh, oa, ob):
        dz = oa + hh * (ob - oa)
        dy = ob + hh * (oa - ob)
        return wrap(z + dz), wrap(y + dy)

    def step_of(n):
        m = n % 3
        return 2 * ((3 - n) // 3) + s * (m * (5 - 3 * m) // 2)

    def swap(hh, zt, yt):
        return remote(part_ref.at[hh, (zt * 4 + yt) * 2 + 1 - c], pair.at[hh, zt, yt], s0.at[hh, zt, yt],
                      r0.at[hh, zt, yt], plane_id(z, y, 1 - c))

    def hop(hh, sign):
        zt, yt = spot(hh, sign * s, 0)
        return plane_id(zt, yt, c)

    def hop2(hh, sign):
        zt, yt = spot(hh, 0, sign * s)
        return plane_id(zt, yt, c)

    def far_place(n):
        m, odd = (n + 1) // 2, n % 2
        return wrap(z + step_of((1 - odd) * m)), wrap(y + step_of(odd * m))

    def rest_place(n):
        m, k = n // 3, n % 3
        return wrap(z + step_of(2 - m + 3 * (m // 2))), wrap(y + step_of(2 - k + 3 * (k // 2)))

    def give(where):
        def step(n, carry):
            zt, yt = where(n)
            for hh in range(2):
                swap(hh, zt, yt).start()
            return carry
        return step

    def send1(kind, hh, ob, zt, yt):
        dst = (far1, near1, next1)[kind].at[hh, ob]
        return remote(unit.at[hh, zt, yt], dst, s1.at[kind, hh, ob], r1.at[kind, hh, ob], hop(hh, 1 if kind < 2 else -1))

    def both_cores(hh, zt, yt):
        swap(hh, zt, yt).wait_recv()
        merge(unit.at[hh, zt, yt], part_ref.at[hh, (zt * 4 + yt) * 2 + c], pair.at[hh, zt, yt])

    def far_units(k, carry):
        hh, ob = k % 2, k // 2
        zt, yt = spot(hh, 2, step_of(ob))
        both_cores(hh, zt, yt)
        send1(0, hh, ob, zt, yt).start()
        return carry

    def next_units(k, carry):
        hh, ob = k % 2, k // 2
        zt, yt = spot(hh, -s, step_of(ob))
        both_cores(hh, zt, yt)
        send1(2, hh, ob, zt, yt).start()
        return carry

    def near_units(k, carry):
        hh, ob = k % 2, k // 2
        zt, yt = spot(hh, s, step_of(ob))
        both_cores(hh, zt, yt)
        send1(0, hh, ob, zt, yt).wait_recv()
        merge(unit.at[hh, zt, yt], unit.at[hh, zt, yt], far1.at[hh, ob])
        send1(1, hh, ob, zt, yt).start()
        return carry

    def own_units(k, carry):
        hh, ob = k % 2, k // 2
        zt, yt = spot(hh, 0, step_of(ob))
        both_cores(hh, zt, yt)
        return carry

    lax.fori_loop(0, 7, give(far_place), 0)
    lax.fori_loop(0, 9, give(rest_place), 0)
    lax.fori_loop(0, 8, far_units, 0)
    lax.fori_loop(0, 8, next_units, 0)
    lax.fori_loop(0, 8, near_units, 0)
    lax.fori_loop(0, 8, own_units, 0)

    def send2(kind, hh, zt, yt):
        dst = (far2, near2, next2)[kind].at[hh]
        return remote(unit.at[hh, zt, yt], dst, s2.at[kind, hh], r2.at[kind, hh], hop2(hh, -1 if kind < 2 else 1))

    def gathered(hh, ob):
        zt, yt = spot(hh, 0, step_of(ob))
        send1(2, hh, ob, zt, yt).wait_recv()
        merge(unit.at[hh, zt, yt], unit.at[hh, zt, yt], next1.at[hh, ob])
        send1(1, hh, ob, zt, yt).wait_recv()
        merge(unit.at[hh, zt, yt], unit.at[hh, zt, yt], near1.at[hh, ob])
        return zt, yt

    def far_blocks(hh, carry):
        zt, yt = gathered(hh, 0)
        send2(0, hh, zt, yt).start()
        return carry

    def next_blocks(hh, carry):
        zt, yt = gathered(hh, 1)
        send2(2, hh, zt, yt).start()
        return carry

    def near_sums(hh, carry):
        gathered(hh, 2)
        return carry

    def near_blocks(hh, carry):
        zt, yt = spot(hh, 0, -s)
        send2(0, hh, zt, yt).wait_recv()
        merge(unit.at[hh, zt, yt], unit.at[hh, zt, yt], far2.at[hh])
        send2(1, hh, zt, yt).start()
        return carry

    def own_blocks(hh, carry):
        zt, yt = gathered(hh, 3)
        send2(2, hh, zt, yt).wait_recv()
        merge(unit.at[hh, zt, yt], unit.at[hh, zt, yt], next2.at[hh])
        send2(1, hh, zt, yt).wait_recv()
        merge(unit.at[hh, zt, yt], unit.at[hh, zt, yt], near2.at[hh])
        return carry

    for phase in (far_blocks, next_blocks, near_sums, near_blocks, own_blocks):
        lax.fori_loop(0, 2, phase, 0)

    masses = [unit[hh, z, y, 32] for hh in range(2)]
    for row in range(32):
        both = [unit[hh, z, y, row] / masses[hh][:, 32 + row:33 + row] for hh in range(2)]
        for hh in range(2):
            tmp[hh, row] = both[hh]
        att_ref[row] = jnp.concatenate(both, axis=0).astype(BF16)
    for hh in range(2):
        for head in range(8):
            own[hh, head] = tmp[hh, :, head, :].astype(BF16)
    for hh in range(2):
        full[z, y, c, hh] = own[hh]

    def sendx(kind, t, q):
        rows = pl.ds(pl.multiple_of(q * QUARTER, QUARTER) if not isinstance(q, int) else q * QUARTER, QUARTER)
        dst = (farx, nearx, nextx)[kind].at[rows]
        return remote(cols.at[t, rows], dst, sx.at[kind, q], rx.at[kind, q],
                      {"mp": wrap(x + (s if kind < 2 else -s))})

    targets = [wrap(z + step) for step in (0, -s, s, 2)]
    columns_of = [wrap(y + step) for step in (0, -s, s, 2)]

    def pass_on(k):
        t = targets[k]

        @pl.when(wrap(t - x - s) == 0)
        def _():
            for q in columns_of:
                rows = pl.ds(pl.multiple_of(q * QUARTER, QUARTER), QUARTER)
                sendx(0, t, q).wait_recv()
                cols[t, rows] = cols[t, rows] + farx[rows]
                sendx(1, t, q).start()

    def send_on(t, quarters):
        @pl.when(wrap(t - x - 2) == 0)
        def _():
            for q in quarters:
                sendx(0, t, q).start()

        @pl.when(wrap(t - x + s) == 0)
        def _():
            for q in quarters:
                sendx(2, t, q).start()

    def project(k, columns):
        t = targets[k]
        if len(columns) == 4:
            rows = [full[t, :, :, hh, head].reshape(256, 128) for hh in range(2) for head in range(8)]
            cols[t] = jnp.dot(jnp.concatenate(rows, axis=1), w_ref[...], preferred_element_type=F32)
            send_on(t, columns_of)
            return
        for n in columns:
            q = columns_of[n]
            rows = [full[t, q, :, hh, head].reshape(QUARTER, 128) for hh in range(2) for head in range(8)]
            cols[t, pl.ds(pl.multiple_of(q * QUARTER, QUARTER), QUARTER)] = jnp.dot(
                jnp.concatenate(rows, axis=1), w_ref[...], preferred_element_type=F32)
            send_on(t, [q])

    sent = plane_gather(own, full, ssem, rsem, dsend, drecv, row_done=project)
    for k in range(4):
        pass_on(k)
    for q in columns_of:
        rows = pl.ds(pl.multiple_of(q * QUARTER, QUARTER), QUARTER)
        sendx(2, x, q).wait_recv()
        sendx(1, x, q).wait_recv()
        proj_ref[rows] = (cols[x, rows] + nextx[rows] + nearx[rows]).astype(BF16)

    for kind in range(3):
        for q in range(4):
            sendx(kind, x, q).wait_send()
    for copy in sent:
        copy.wait_send()

    def drain(k, carry):
        hh, ob = k % 2, k // 2
        for oa in range(4):
            zt, yt = spot(hh, step_of(oa), step_of(ob))
            swap(hh, zt, yt).wait_send()
        for kind in range(3):
            send1(kind, hh, ob, z, y).wait_send()
        return carry

    lax.fori_loop(0, 8, drain, 0)

    def drain2(hh, carry):
        for kind in range(3):
            send2(kind, hh, z, y).wait_send()
        return carry

    lax.fori_loop(0, 2, drain2, 0)


def finish(parts, weight, rows):
    unit = (33, 8, 128)
    dma = pltpu.SemaphoreType.DMA
    return pl.pallas_call(
        finish_kernel,
        out_shape=(
            jax.ShapeDtypeStruct((rows, 16, 128), BF16),
            jax.ShapeDtypeStruct((256, weight.shape[1]), BF16),
        ),
        in_specs=[VMEM, VMEM],
        out_specs=(VMEM, VMEM),
        scratch_shapes=[
            pltpu.VMEM((2, 4, 4) + unit, F32),
            pltpu.VMEM((2, 4, 4) + unit, F32),
            pltpu.VMEM((2, 4) + unit, F32),
            pltpu.VMEM((2, 4) + unit, F32),
            pltpu.VMEM((2, 4) + unit, F32),
            pltpu.VMEM((2,) + unit, F32),
            pltpu.VMEM((2,) + unit, F32),
            pltpu.VMEM((2,) + unit, F32),
            pltpu.VMEM((2, 32, 8, 128), F32),
            pltpu.VMEM((2, 8, 32, 128), BF16),
            pltpu.VMEM((4, 4, 2, 2, 8, 32, 128), BF16),
            pltpu.VMEM((4, 256, 256), F32),
            pltpu.VMEM((256, 256), F32),
            pltpu.VMEM((256, 256), F32),
            pltpu.VMEM((256, 256), F32),
            dma((2, 4, 4)),
            dma((2, 4, 4)),
            dma((3, 2, 4)),
            dma((3, 2, 4)),
            dma((3, 2)),
            dma((3, 2)),
        ] + gather_sems() + [dma((3, 4)), dma((3, 4))],
        compiler_params=pltpu.CompilerParams(collective_id=1, has_side_effects=True, vmem_limit_bytes=24 << 20),
        name="finish",
    )(parts, weight)


def body(queries, lookup_sheets, content_sheets, page_table, context_len, out_weight):
    req = page_table.shape[0]
    pool, page_len, kv, dim = lookup_sheets.shape
    rows, heads, _ = queries.shape
    all_queries, words = gather_queries(
        *(pltpu.with_memory_space_constraint(a, pltpu.HBM)
          for a in (queries.reshape(2, rows // 2, heads, dim), page_table.T, context_len.reshape(req // 128, 128))),
        pool,
        page_len,
    )
    parts = attend_pages(
        words,
        all_queries.reshape(req, heads, dim),
        lookup_sheets.reshape(pool, page_len * kv, dim),
        content_sheets.reshape(pool, page_len * kv, dim),
    )
    return finish(parts, out_weight, rows)


def solution(mesh):
    finer = Mesh(mesh.devices.reshape(4, 4, 2, mesh.shape["mp"]), ("dp_0", "dp_1", "dp_2", "mp"))
    return jax.shard_map(
        body,
        mesh=finer,
        in_specs=(
            P(DP, "mp", None),
            P(DP, None, "mp", None),
            P(DP, None, "mp", None),
            P(),
            P(),
            P("mp", DP),
        ),
        out_specs=(P(DP, "mp", None), P("mp", DP)),
        check_vma=False,
    )
```

```python
import functools

import jax
import jax.numpy as jnp
from jax import lax
from jax.experimental import pallas as pl
from jax.experimental.pallas import tpu as pltpu
from jax.sharding import Mesh
from jax.sharding import PartitionSpec as P

DP = ("dp_0", "dp_1", "dp_2")
MESH = pl.DeviceIdType.MESH
LOW = -1e30
QUARTER = 64
BATCH = 32
NOTHING = 1056
F32 = jnp.float32
BF16 = jnp.bfloat16
NT = (((1,), (1,)), ((), ()))
VMEM = pl.BlockSpec(memory_space=pltpu.VMEM)
HBM = pl.BlockSpec(memory_space=pltpu.HBM)
SMEM = pl.BlockSpec(memory_space=pltpu.SMEM)


def wrap(value):
    return lax.rem(value + 8, 4)


def place():
    z, y, c = (lax.axis_index(name) for name in DP)
    return z, y, c, 1 - 2 * c


def plane_id(z, y, c):
    return {"dp_0": z, "dp_1": y, "dp_2": c}


def greet(devices):
    barrier = pltpu.get_barrier_semaphore()
    for device in devices:
        pl.semaphore_signal(barrier, inc=1, device_id=device, device_id_type=MESH)
    pl.semaphore_wait(barrier, len(devices))


def remote(src, dst, send_sem, recv_sem, device):
    return pltpu.make_async_remote_copy(
        src_ref=src,
        dst_ref=dst,
        send_sem=send_sem,
        recv_sem=recv_sem,
        device_id=device,
        device_id_type=MESH,
    )


def plane_gather(own, full, ssem, rsem, dsend, drecv, between=(), row_done=None):
    z, y, c, s = place()
    work = list(between)

    def fill():
        piece = work.pop(0) if work else None
        if piece is not None:
            piece()

    def at(h, a, b):
        return full.at[a, b, c, h] if h == 0 else full.at[b, a, c, h]

    def device(h, a, b):
        return plane_id(a, b, c) if h == 0 else plane_id(b, a, c)

    def mine(h):
        return (z, y) if h == 0 else (y, z)

    sent = []

    def go(h, group, m, src, dst, target):
        copy = remote(src, dst, ssem.at[h, group, m], rsem.at[h, group, m], target)
        copy.start()
        sent.append(copy)

    def come(h, group, m, dst):
        remote(dst, dst, ssem.at[h, group, m], rsem.at[h, group, m], plane_id(z, y, c)).wait_recv()

    def share(h, slot, src, dst):
        copy = remote(src, dst, dsend.at[h, slot], drecv.at[h, slot], plane_id(z, y, 1 - c))
        copy.start()
        sent.append(copy)

    def spread(h, group, slot, src, a, b):
        go(h, group, 0, src, at(h, a, b), device(h, mine(h)[0], wrap(b + s)))
        go(h, group, 1, src, at(h, a, b), device(h, mine(h)[0], wrap(b - s)))

    def first(h):
        a, b = mine(h)
        go(h, 0, 0, own.at[h], at(h, a, b), device(h, wrap(a + s), b))
        go(h, 0, 1, own.at[h], at(h, a, b), device(h, wrap(a - s), b))
        go(h, 0, 2, own.at[h], at(h, a, b), device(h, wrap(a + 2), b))

    for h in range(2):
        first(h)
    for h in range(2):
        share(h, 0, own.at[h], at(h, *mine(h)))
        spread(h, 1, 0, own.at[h], *mine(h))
    fill()
    for h in range(2):
        a, b = mine(h)
        near = wrap(a - s)
        come(h, 0, 0, at(h, near, b))
        spread(h, 2, 4, at(h, near, b), near, b)
        share(h, 4, at(h, near, b), at(h, near, b))
    for h in range(2):
        a, b = mine(h)
        near = wrap(a + s)
        come(h, 0, 1, at(h, near, b))
        spread(h, 3, 8, at(h, near, b), near, b)
        share(h, 8, at(h, near, b), at(h, near, b))
    fill()
    for h in range(2):
        a, b = mine(h)
        far = wrap(a + 2)
        come(h, 0, 2, at(h, far, b))
        spread(h, 4, 12, at(h, far, b), far, b)
        share(h, 12, at(h, far, b), at(h, far, b))
    fill()
    steps = (0, 0, -1, 1, 2)

    def near(group):
        for h in range(2):
            a, b = mine(h)
            row = wrap(a + steps[group] * s)
            side = wrap(b - s)
            come(h, group, 0, at(h, row, side))
            go(h, group, 2, at(h, row, side), at(h, row, side), device(h, a, wrap(b + s)))
            share(h, 4 * (group - 1) + 1, at(h, row, side), at(h, row, side))
        fill()

    def other(group):
        for h in range(2):
            a, b = mine(h)
            row = wrap(a + steps[group] * s)
            side = wrap(b + s)
            come(h, group, 1, at(h, row, side))
            share(h, 4 * (group - 1) + 2, at(h, row, side), at(h, row, side))

    def far(group):
        for h in range(2):
            a, b = mine(h)
            row = wrap(a + steps[group] * s)
            opposite = wrap(b + 2)
            come(h, group, 2, at(h, row, opposite))
            share(h, 4 * (group - 1) + 3, at(h, row, opposite), at(h, row, opposite))

    across = (0, 2, 1, 3)

    def from_pair(k, n):
        for h, slot in ((0, 4 * across[k] + across[n]), (1, 4 * across[n] + across[k])):
            where = full.at[0, 0, 1 - c, h]
            remote(where, where, dsend.at[h, slot], drecv.at[h, slot], plane_id(z, y, 1 - c)).wait_recv()

    def arrived(k, columns=(0, 1, 2, 3)):
        for n in columns:
            from_pair(k, n)
        if row_done is not None:
            row_done(k, columns)

    near(1)
    near(2)
    other(1)
    near(3)
    other(2)
    near(4)
    other(3)
    other(4)
    far(1)
    if row_done is not None:
        arrived(0)
    far(2)
    far(3)
    if row_done is not None:
        arrived(1)
        arrived(2)
    far(4)
    if row_done is not None:
        arrived(3, (0, 1, 2))
        arrived(3, (3,))
    else:
        for k in range(4):
            arrived(k)
    return sent


def gather_sems():
    return [
        pltpu.SemaphoreType.DMA((2, 5, 3)),
        pltpu.SemaphoreType.DMA((2, 5, 3)),
        pltpu.SemaphoreType.DMA((2, 16)),
        pltpu.SemaphoreType.DMA((2, 16)),
    ]


def queries_kernel(pool_bits, page_len, q_hbm, table_hbm, len_hbm, full_ref, list_ref,
                   table_ref, len_ref, lo_ref, hi_ref, part_ref, total_ref, lsem, ssem, rsem, dsend, drecv):
    z, y, c, s = place()
    me = (z * 4 + y) * 2 + c
    loads = [
        pltpu.make_async_copy(src, dst, lsem.at[n])
        for n, (src, dst) in enumerate(
            ((q_hbm, full_ref.at[z, y, c]), (table_hbm, table_ref), (len_hbm, len_ref)))
    ]
    for load in loads:
        load.start()
    greet([plane_id(wrap(z + 1), y, c), plane_id(wrap(z - 1), y, c), plane_id(z, wrap(y + 1), c),
           plane_id(z, wrap(y - 1), c), plane_id(wrap(z + 2), y, c), plane_id(z, wrap(y + 2), c), plane_id(z, y, 1 - c)])
    loads[0].wait()

    def place_pages():
        for load in loads[1:]:
            load.wait()
        slots = table_ref.shape[0]
        slot = lax.broadcasted_iota(jnp.int32, (slots, 128), 0)
        lane = lax.broadcasted_iota(jnp.int32, (slots, 128), 1)
        blocks = table_ref.shape[1] // 128
        mine, tokens, page, owner = [], [], [], []
        for t in range(blocks):
            ids = table_ref[:, t * 128:(t + 1) * 128]
            length = jnp.broadcast_to(len_ref[t:t + 1, :], (slots, 128))
            left = jnp.clip(length - slot * page_len, 0, page_len)
            mine.append(jnp.where(((ids >> pool_bits) == me) & (left > 0), 1.0, 0.0))
            tokens.append(left)
            page.append(ids & ((1 << pool_bits) - 1))
            owner.append(lane + t * 128)
        mine, tokens, page, owner = (jnp.concatenate(v, axis=0) for v in (mine, tokens, page, owner))
        rows = slots * blocks
        mine_h = mine.astype(BF16)
        i = lax.broadcasted_iota(jnp.int32, (rows, rows), 0)
        j = lax.broadcasted_iota(jnp.int32, (rows, rows), 1)
        same = (i // slots) == (j // slots)

        def count(which, what):
            return jnp.dot(jnp.where(which, 1.0, 0.0).astype(BF16), what, preferred_element_type=F32)

        earlier = count(same & (j < i), mine_h)
        column = count(same, mine_h)
        blocks_before = count((j // slots) < (i // slots), mine_h)
        i = lax.broadcasted_iota(jnp.int32, (128, 128), 0)
        j = lax.broadcasted_iota(jnp.int32, (128, 128), 1)
        ahead = jnp.where(i < j, 1.0, 0.0).astype(BF16)
        every = jnp.ones((128, 128), BF16)
        start = jnp.dot(column.astype(BF16), ahead, preferred_element_type=F32)
        start = start + jnp.dot(blocks_before.astype(BF16), every, preferred_element_type=F32)
        rank = (start + earlier).astype(jnp.int32)
        lo_ref[...] = jnp.where(mine > 0.0, rank & 127, -1)
        hi_ref[...] = jnp.where(mine > 0.0, rank >> 7, -1)
        part_ref[0] = (page & 255).astype(F32)
        part_ref[1] = (owner & 255).astype(F32)
        part_ref[2] = ((page >> 8) + ((owner >> 8) << 2) + ((tokens - 1) << 4)).astype(F32)
        part_ref[3] = jnp.where(earlier > 0.0, 0.0, 1.0)
        last = jnp.where(column > 0.0, start + column - 1.0, float(NOTHING)).astype(jnp.int32)
        list_ref[8:16, :] = jnp.concatenate([last[t * slots:t * slots + 1] for t in range(blocks)], axis=0)
        number = (start + column)[rows - 1:rows, 127:128]
        list_ref[16:24, :] = jnp.broadcast_to(number, (8, 128)).astype(jnp.int32)
        total_ref[...] = jnp.zeros_like(total_ref)

    sub = lax.broadcasted_iota(jnp.int32, (128, 128), 0).astype(F32).astype(BF16)
    one, nil = jnp.ones((128, 128), BF16), jnp.zeros((128, 128), BF16)
    sub8 = lax.broadcasted_iota(jnp.int32, (8, 128), 0)

    def scatter(part):
        def step(n, carry):
            base = pl.multiple_of(n * 8, 8)
            lo8 = lo_ref[pl.ds(base, 8), :].astype(F32)
            hi8 = hi_ref[pl.ds(base, 8), :]
            p8 = [part_ref[k, pl.ds(base, 8), :] for k in range(4)]
            wide, tall = [], []
            for r in range(8):
                wide.append(jnp.where(sub == jnp.broadcast_to(lo8[r:r + 1, :], (128, 128)).astype(BF16), one, nil))
                hit = sub8 == hi8[r:r + 1, :]
                tall.append(jnp.concatenate(
                    [jnp.where(hit, p8[k][r:r + 1, :], 0.0) for k in range(4)], axis=0).astype(BF16))
            wide = jnp.concatenate(wide, axis=1)
            tall = jnp.concatenate(tall, axis=1)
            total_ref[...] += lax.dot_general(wide, tall, NT, preferred_element_type=F32)
            return carry

        steps = lo_ref.shape[0] // 32
        lax.fori_loop(part * steps, (part + 1) * steps, step, 0)

    def write_list():
        total = jnp.concatenate([total_ref[...], jnp.zeros((128, 96), F32)], axis=1).T.astype(jnp.int32)
        p0, p1, p2, p3 = (total[8 * k:8 * k + 8, :] for k in range(4))
        page = p0 + ((p2 & 3) << 8)
        owner = p1 + (((p2 >> 2) & 3) << 8)
        tokens = (p2 >> 4) + 1
        list_ref[0:8, :] = page + (owner << 10) + (tokens << 20) + (p3 << 25)

    def start_list():
        place_pages()
        scatter(0)
        scatter(1)

    pieces = [start_list, None, functools.partial(scatter, 2), functools.partial(scatter, 3), None, None, write_list]
    for copy in plane_gather(full_ref.at[z, y, c], full_ref, ssem, rsem, dsend, drecv, between=pieces):
        copy.wait_send()


def gather_queries(queries, table, lengths, pool, page_len):
    req = table.shape[1]
    rows = table.shape[0] * req // 128
    _, half, heads, dim = queries.shape
    return pl.pallas_call(
        functools.partial(queries_kernel, pool.bit_length() - 1, page_len),
        out_shape=(
            jax.ShapeDtypeStruct((4, 4, 2, 2, half, heads, dim), BF16),
            jax.ShapeDtypeStruct((24, 128), jnp.int32),
        ),
        in_specs=[HBM] * 3,
        out_specs=(VMEM, VMEM),
        scratch_shapes=[
            pltpu.VMEM(table.shape, jnp.int32),
            pltpu.VMEM(lengths.shape, jnp.int32),
            pltpu.VMEM((rows, 128), jnp.int32),
            pltpu.VMEM((rows, 128), jnp.int32),
            pltpu.VMEM((4, rows, 128), F32),
            pltpu.VMEM((128, 32), F32),
            pltpu.SemaphoreType.DMA((3,)),
        ] + gather_sems(),
        compiler_params=pltpu.CompilerParams(collective_id=0, has_side_effects=True, vmem_limit_bytes=8 << 20),
        cost_estimate=pl.CostEstimate(flops=10**10, bytes_accessed=1 << 23, transcendentals=0),
        name="gather_queries",
    )(queries, table, lengths)


def pages_kernel(scale, list_ref, q_ref, k_ref, v_ref, acc_ref, sum_ref, top_ref, wait_ref, peak_ref, mass_ref):
    lane = lax.broadcasted_iota(jnp.int32, (16, 128), 1)
    blank = jnp.where(lane < 32, LOW, 0.0)
    zero = jnp.zeros((16, 128), F32)
    sum_ref[NOTHING] = zero
    top_ref[NOTHING] = blank
    wait_ref[...] = jnp.zeros_like(wait_ref)
    peak_ref[...] = jnp.zeros_like(peak_ref)
    mass_ref[...] = jnp.zeros_like(mass_ref)

    i = lax.broadcasted_iota(jnp.int32, (16, 128), 0)
    kv_match = (i // 8) == (lane % 2)
    token = (lane % 32) // 2
    token_of = [jnp.where(kv_match & (lane // 32 == n), token, 1 << 20) for n in range(4)]

    def entry(base, e):
        word = list_ref[base // 128, base % 128 + e]
        return word & 1023, (word >> 10) & 1023, (word >> 20) & 31, (word >> 25) & 1

    def step(n, carry):
        past = jnp.maximum(n - 1, 0) * BATCH
        base = n * BATCH
        before = [entry(past, e) for e in range(BATCH)]
        now = [entry(base, e) for e in range(BATCH)]
        outs, scores = [], []
        for g in range(BATCH // 4):
            four = slice(4 * g, 4 * g + 4)
            vs = jnp.concatenate([v_ref[p] for p, _, _, _ in before[four]], axis=0)
            outs.append(jnp.dot(wait_ref[g], vs, preferred_element_type=F32))
            qs = jnp.concatenate([q_ref[r] for _, r, _, _ in now[four]], axis=0)
            ks = jnp.concatenate([k_ref[p] for p, _, _, _ in now[four]], axis=0)
            scores.append(lax.dot_general(qs, ks, NT, preferred_element_type=F32))
        top, mass, acc = carry
        for e, (_, _, _, first) in enumerate(before):
            old = jnp.where(first == 1, LOW, top)
            p = peak_ref[e]
            top = jnp.maximum(old, p)
            f_old = jnp.exp(old - top)
            f_new = jnp.exp(p - top)
            mass = mass * f_old + mass_ref[e] * f_new
            acc = acc * f_old + outs[e // 4][16 * (e % 4):16 * (e % 4) + 16] * f_new
            sum_ref[past + e] = acc
            top_ref[past + e] = jnp.where(lane < 32, top, mass)
        for g in range(BATCH // 4):
            weights = []
            for e in range(4):
                valid = token_of[e] < now[4 * g + e][2]
                sc = jnp.where(valid, scores[g][16 * e:16 * e + 16] * scale, LOW)
                peak = jnp.max(sc, axis=1, keepdims=True)
                w = jnp.where(valid, jnp.exp(sc - peak), 0.0)
                peak_ref[4 * g + e] = jnp.broadcast_to(peak, (16, 128))
                mass_ref[4 * g + e] = jnp.broadcast_to(jnp.sum(w, axis=1, keepdims=True), (16, 128))
                weights.append(w)
            wait_ref[g] = jnp.concatenate(weights, axis=0).astype(BF16)
        return top, mass, acc

    batches = (list_ref[16, 0] + BATCH - 1) // BATCH
    lax.fori_loop(0, batches + 1, step, (zero, zero, zero))

    def spread(d, carry):
        tops = blank
        line, first = 8 + d // 4, (d % 4) * 32
        for row in range(32):
            last = list_ref[line, first + row]
            acc = sum_ref[last]
            tops = jnp.where((lane == row) | (lane == row + 32), top_ref[last], tops)
            for hh in range(2):
                acc_ref[hh, d, row] = acc[8 * hh:8 * hh + 8]
        for hh in range(2):
            acc_ref[hh, d, 32] = tops[8 * hh:8 * hh + 8]
        return carry

    lax.fori_loop(0, acc_ref.shape[1], spread, 0)


def attend_pages(words, all_queries, keys, values):
    req, heads, dim = all_queries.shape
    return pl.pallas_call(
        functools.partial(pages_kernel, dim ** (-0.5)),
        out_shape=jax.ShapeDtypeStruct((2, req // 32, 33, 8, 128), F32),
        in_specs=[SMEM, VMEM, VMEM, VMEM],
        out_specs=VMEM,
        scratch_shapes=[
            pltpu.VMEM((NOTHING + 1, heads, dim), F32),
            pltpu.VMEM((NOTHING + 1, heads, dim), F32),
            pltpu.VMEM((BATCH // 4, 4 * heads, dim), BF16),
            pltpu.VMEM((BATCH, heads, dim), F32),
            pltpu.VMEM((BATCH, heads, dim), F32),
        ],
        compiler_params=pltpu.CompilerParams(vmem_limit_bytes=20 << 20),
        name="attend_pages",
    )(words, all_queries, keys, values)


def merge(dst, one, other):
    lane = lax.broadcasted_iota(jnp.int32, (8, 128), 1)
    t1, t2 = one[32], other[32]
    top = jnp.maximum(t1, t2)
    f1 = jnp.exp(t1 - top)
    f2 = jnp.exp(t2 - top)
    mass = t1 * pltpu.roll(f1, 32, 1) + t2 * pltpu.roll(f2, 32, 1)
    for row in range(32):
        dst[row] = one[row] * f1[:, row:row + 1] + other[row] * f2[:, row:row + 1]
    dst[32] = jnp.where(lane < 32, top, mass)


def finish_kernel(part_ref, w_ref, att_ref, proj_ref, unit, pair, far1, near1, next1, far2, near2, next2,
                  tmp, own, full, cols, farx, nearx, nextx,
                  s0, r0, s1, r1, s2, r2, ssem, rsem, dsend, drecv, sx, rx):
    z, y, c, s = place()
    x = lax.axis_index("mp")
    home = plane_id(z, y, c)
    greet([plane_id(wrap(z + 1), y, c), plane_id(wrap(z - 1), y, c), plane_id(z, wrap(y + 1), c),
           plane_id(z, wrap(y - 1), c), plane_id(wrap(z + 2), y, c), plane_id(z, wrap(y + 2), c), plane_id(z, y, 1 - c), {"mp": wrap(x + 1)}, {"mp": wrap(x - 1)}])

    def spot(hh, oa, ob):
        dz = oa + hh * (ob - oa)
        dy = ob + hh * (oa - ob)
        return wrap(z + dz), wrap(y + dy)

    def step_of(n):
        m = n % 3
        return 2 * ((3 - n) // 3) + s * (m * (5 - 3 * m) // 2)

    def swap(hh, zt, yt):
        return remote(part_ref.at[hh, (zt * 4 + yt) * 2 + 1 - c], pair.at[hh, zt, yt], s0.at[hh, zt, yt],
                      r0.at[hh, zt, yt], plane_id(z, y, 1 - c))

    def hop(hh, sign):
        zt, yt = spot(hh, sign * s, 0)
        return plane_id(zt, yt, c)

    def hop2(hh, sign):
        zt, yt = spot(hh, 0, sign * s)
        return plane_id(zt, yt, c)

    def far_place(n):
        m, odd = (n + 1) // 2, n % 2
        return wrap(z + step_of((1 - odd) * m)), wrap(y + step_of(odd * m))

    def rest_place(n):
        m, k = n // 3, n % 3
        return wrap(z + step_of(2 - m + 3 * (m // 2))), wrap(y + step_of(2 - k + 3 * (k // 2)))

    def give(where):
        def step(n, carry):
            zt, yt = where(n)
            for hh in range(2):
                swap(hh, zt, yt).start()
            return carry
        return step

    def send1(kind, hh, ob, zt, yt):
        dst = (far1, near1, next1)[kind].at[hh, ob]
        return remote(unit.at[hh, zt, yt], dst, s1.at[kind, hh, ob], r1.at[kind, hh, ob], hop(hh, 1 if kind < 2 else -1))

    def both_cores(hh, zt, yt):
        swap(hh, zt, yt).wait_recv()
        merge(unit.at[hh, zt, yt], part_ref.at[hh, (zt * 4 + yt) * 2 + c], pair.at[hh, zt, yt])

    def far_units(k, carry):
        hh, ob = k % 2, k // 2
        zt, yt = spot(hh, 2, step_of(ob))
        both_cores(hh, zt, yt)
        send1(0, hh, ob, zt, yt).start()
        return carry

    def next_units(k, carry):
        hh, ob = k % 2, k // 2
        zt, yt = spot(hh, -s, step_of(ob))
        both_cores(hh, zt, yt)
        send1(2, hh, ob, zt, yt).start()
        return carry

    def near_units(k, carry):
        hh, ob = k % 2, k // 2
        zt, yt = spot(hh, s, step_of(ob))
        both_cores(hh, zt, yt)
        send1(0, hh, ob, zt, yt).wait_recv()
        merge(unit.at[hh, zt, yt], unit.at[hh, zt, yt], far1.at[hh, ob])
        send1(1, hh, ob, zt, yt).start()
        return carry

    def own_units(k, carry):
        hh, ob = k % 2, k // 2
        zt, yt = spot(hh, 0, step_of(ob))
        both_cores(hh, zt, yt)
        return carry

    lax.fori_loop(0, 7, give(far_place), 0)
    lax.fori_loop(0, 2, far_units, 0)
    lax.fori_loop(0, 9, give(rest_place), 0)
    lax.fori_loop(2, 8, far_units, 0)
    lax.fori_loop(0, 8, next_units, 0)
    lax.fori_loop(0, 8, near_units, 0)
    lax.fori_loop(0, 8, own_units, 0)

    def send2(kind, hh, zt, yt):
        dst = (far2, near2, next2)[kind].at[hh]
        return remote(unit.at[hh, zt, yt], dst, s2.at[kind, hh], r2.at[kind, hh], hop2(hh, -1 if kind < 2 else 1))

    def gathered(hh, ob):
        zt, yt = spot(hh, 0, step_of(ob))
        send1(2, hh, ob, zt, yt).wait_recv()
        merge(unit.at[hh, zt, yt], unit.at[hh, zt, yt], next1.at[hh, ob])
        send1(1, hh, ob, zt, yt).wait_recv()
        merge(unit.at[hh, zt, yt], unit.at[hh, zt, yt], near1.at[hh, ob])
        return zt, yt

    def far_blocks(hh, carry):
        zt, yt = gathered(hh, 0)
        send2(0, hh, zt, yt).start()
        return carry

    def next_blocks(hh, carry):
        zt, yt = gathered(hh, 1)
        send2(2, hh, zt, yt).start()
        return carry

    def near_sums(hh, carry):
        gathered(hh, 2)
        return carry

    def near_blocks(hh, carry):
        zt, yt = spot(hh, 0, -s)
        send2(0, hh, zt, yt).wait_recv()
        merge(unit.at[hh, zt, yt], unit.at[hh, zt, yt], far2.at[hh])
        send2(1, hh, zt, yt).start()
        return carry

    def own_blocks(hh, carry):
        zt, yt = gathered(hh, 3)
        send2(2, hh, zt, yt).wait_recv()
        merge(unit.at[hh, zt, yt], unit.at[hh, zt, yt], next2.at[hh])
        send2(1, hh, zt, yt).wait_recv()
        merge(unit.at[hh, zt, yt], unit.at[hh, zt, yt], near2.at[hh])
        return carry

    for phase in (far_blocks, next_blocks, near_sums, near_blocks, own_blocks):
        lax.fori_loop(0, 2, phase, 0)

    masses = [unit[hh, z, y, 32] for hh in range(2)]
    for row in range(32):
        both = [unit[hh, z, y, row] / masses[hh][:, 32 + row:33 + row] for hh in range(2)]
        for hh in range(2):
            tmp[hh, row] = both[hh]
        att_ref[row] = jnp.concatenate(both, axis=0).astype(BF16)
    for hh in range(2):
        for head in range(8):
            own[hh, head] = tmp[hh, :, head, :].astype(BF16)
    for hh in range(2):
        full[z, y, c, hh] = own[hh]

    def sendx(kind, t, q):
        rows = pl.ds(pl.multiple_of(q * QUARTER, QUARTER) if not isinstance(q, int) else q * QUARTER, QUARTER)
        dst = (farx, nearx, nextx)[kind].at[rows]
        return remote(cols.at[t, rows], dst, sx.at[kind, q], rx.at[kind, q],
                      {"mp": wrap(x + (s if kind < 2 else -s))})

    targets = [wrap(z + step) for step in (0, -s, s, 2)]
    columns_of = [wrap(y + step) for step in (0, -s, s, 2)]

    def pass_on(k):
        t = targets[k]

        @pl.when(wrap(t - x - s) == 0)
        def _():
            for q in columns_of:
                rows = pl.ds(pl.multiple_of(q * QUARTER, QUARTER), QUARTER)
                sendx(0, t, q).wait_recv()
                cols[t, rows] = cols[t, rows] + farx[rows]
                sendx(1, t, q).start()

    def send_on(t, quarters):
        @pl.when(wrap(t - x - 2) == 0)
        def _():
            for q in quarters:
                sendx(0, t, q).start()

        @pl.when(wrap(t - x + s) == 0)
        def _():
            for q in quarters:
                sendx(2, t, q).start()

    def project(k, columns):
        t = targets[k]
        if len(columns) == 4:
            rows = [full[t, :, :, hh, head].reshape(256, 128) for hh in range(2) for head in range(8)]
            cols[t] = jnp.dot(jnp.concatenate(rows, axis=1), w_ref[...], preferred_element_type=F32)
            send_on(t, columns_of)
            return
        for n in columns:
            q = columns_of[n]
            rows = [full[t, q, :, hh, head].reshape(QUARTER, 128) for hh in range(2) for head in range(8)]
            cols[t, pl.ds(pl.multiple_of(q * QUARTER, QUARTER), QUARTER)] = jnp.dot(
                jnp.concatenate(rows, axis=1), w_ref[...], preferred_element_type=F32)
            send_on(t, [q])

    sent = plane_gather(own, full, ssem, rsem, dsend, drecv, row_done=project)
    for k in range(4):
        pass_on(k)
    for q in columns_of:
        rows = pl.ds(pl.multiple_of(q * QUARTER, QUARTER), QUARTER)
        sendx(2, x, q).wait_recv()
        sendx(1, x, q).wait_recv()
        proj_ref[rows] = (cols[x, rows] + nextx[rows] + nearx[rows]).astype(BF16)

    for kind in range(3):
        for q in range(4):
            sendx(kind, x, q).wait_send()
    for copy in sent:
        copy.wait_send()

    def drain(k, carry):
        hh, ob = k % 2, k // 2
        for oa in range(4):
            zt, yt = spot(hh, step_of(oa), step_of(ob))
            swap(hh, zt, yt).wait_send()
        for kind in range(3):
            send1(kind, hh, ob, z, y).wait_send()
        return carry

    lax.fori_loop(0, 8, drain, 0)

    def drain2(hh, carry):
        for kind in range(3):
            send2(kind, hh, z, y).wait_send()
        return carry

    lax.fori_loop(0, 2, drain2, 0)


def finish(parts, weight, rows):
    unit = (33, 8, 128)
    dma = pltpu.SemaphoreType.DMA
    return pl.pallas_call(
        finish_kernel,
        out_shape=(
            jax.ShapeDtypeStruct((rows, 16, 128), BF16),
            jax.ShapeDtypeStruct((256, weight.shape[1]), BF16),
        ),
        in_specs=[VMEM, VMEM],
        out_specs=(VMEM, VMEM),
        scratch_shapes=[
            pltpu.VMEM((2, 4, 4) + unit, F32),
            pltpu.VMEM((2, 4, 4) + unit, F32),
            pltpu.VMEM((2, 4) + unit, F32),
            pltpu.VMEM((2, 4) + unit, F32),
            pltpu.VMEM((2, 4) + unit, F32),
            pltpu.VMEM((2,) + unit, F32),
            pltpu.VMEM((2,) + unit, F32),
            pltpu.VMEM((2,) + unit, F32),
            pltpu.VMEM((2, 32, 8, 128), F32),
            pltpu.VMEM((2, 8, 32, 128), BF16),
            pltpu.VMEM((4, 4, 2, 2, 8, 32, 128), BF16),
            pltpu.VMEM((4, 256, 256), F32),
            pltpu.VMEM((256, 256), F32),
            pltpu.VMEM((256, 256), F32),
            pltpu.VMEM((256, 256), F32),
            dma((2, 4, 4)),
            dma((2, 4, 4)),
            dma((3, 2, 4)),
            dma((3, 2, 4)),
            dma((3, 2)),
            dma((3, 2)),
        ] + gather_sems() + [dma((3, 4)), dma((3, 4))],
        compiler_params=pltpu.CompilerParams(collective_id=1, has_side_effects=True, vmem_limit_bytes=24 << 20),
        name="finish",
    )(parts, weight)


def body(queries, lookup_sheets, content_sheets, page_table, context_len, out_weight):
    req = page_table.shape[0]
    pool, page_len, kv, dim = lookup_sheets.shape
    rows, heads, _ = queries.shape
    all_queries, words = gather_queries(
        *(pltpu.with_memory_space_constraint(a, pltpu.HBM)
          for a in (queries.reshape(2, rows // 2, heads, dim), page_table.T, context_len.reshape(req // 128, 128))),
        pool,
        page_len,
    )
    parts = attend_pages(
        words,
        all_queries.reshape(req, heads, dim),
        lookup_sheets.reshape(pool, page_len * kv, dim),
        content_sheets.reshape(pool, page_len * kv, dim),
    )
    return finish(parts, out_weight, rows)


def solution(mesh):
    finer = Mesh(mesh.devices.reshape(4, 4, 2, mesh.shape["mp"]), ("dp_0", "dp_1", "dp_2", "mp"))
    return jax.shard_map(
        body,
        mesh=finer,
        in_specs=(
            P(DP, "mp", None),
            P(DP, None, "mp", None),
            P(DP, None, "mp", None),
            P(),
            P(),
            P("mp", DP),
        ),
        out_specs=(P(DP, "mp", None), P("mp", DP)),
        check_vma=False,
    )
```

```python
import functools

import jax
import jax.numpy as jnp
from jax import lax
from jax.experimental import pallas as pl
from jax.experimental.pallas import tpu as pltpu
from jax.sharding import Mesh
from jax.sharding import PartitionSpec as P

DP = ("dp_0", "dp_1", "dp_2")
MESH = pl.DeviceIdType.MESH
LOW = -1e30
QUARTER = 64
BATCH = 32
NOTHING = 1056
F32 = jnp.float32
BF16 = jnp.bfloat16
NT = (((1,), (1,)), ((), ()))
VMEM = pl.BlockSpec(memory_space=pltpu.VMEM)
HBM = pl.BlockSpec(memory_space=pltpu.HBM)
SMEM = pl.BlockSpec(memory_space=pltpu.SMEM)


def wrap(value):
    return lax.rem(value + 8, 4)


def place():
    z, y, c = (lax.axis_index(name) for name in DP)
    return z, y, c, 1 - 2 * c


def plane_id(z, y, c):
    return {"dp_0": z, "dp_1": y, "dp_2": c}


def greet(devices):
    barrier = pltpu.get_barrier_semaphore()
    for device in devices:
        pl.semaphore_signal(barrier, inc=1, device_id=device, device_id_type=MESH)
    pl.semaphore_wait(barrier, len(devices))


def remote(src, dst, send_sem, recv_sem, device):
    return pltpu.make_async_remote_copy(
        src_ref=src,
        dst_ref=dst,
        send_sem=send_sem,
        recv_sem=recv_sem,
        device_id=device,
        device_id_type=MESH,
    )


def plane_gather(own, full, ssem, rsem, dsend, drecv, between=(), row_done=None):
    z, y, c, s = place()
    work = list(between)

    def fill():
        piece = work.pop(0) if work else None
        if piece is not None:
            piece()

    def at(h, a, b):
        return full.at[a, b, c, h] if h == 0 else full.at[b, a, c, h]

    def device(h, a, b):
        return plane_id(a, b, c) if h == 0 else plane_id(b, a, c)

    def mine(h):
        return (z, y) if h == 0 else (y, z)

    sent = []

    def go(h, group, m, src, dst, target):
        copy = remote(src, dst, ssem.at[h, group, m], rsem.at[h, group, m], target)
        copy.start()
        sent.append(copy)

    def come(h, group, m, dst):
        remote(dst, dst, ssem.at[h, group, m], rsem.at[h, group, m], plane_id(z, y, c)).wait_recv()

    def share(h, slot, src, dst):
        copy = remote(src, dst, dsend.at[h, slot], drecv.at[h, slot], plane_id(z, y, 1 - c))
        copy.start()
        sent.append(copy)

    def spread(h, group, slot, src, a, b):
        go(h, group, 0, src, at(h, a, b), device(h, mine(h)[0], wrap(b + s)))
        go(h, group, 1, src, at(h, a, b), device(h, mine(h)[0], wrap(b - s)))

    def first(h):
        a, b = mine(h)
        go(h, 0, 0, own.at[h], at(h, a, b), device(h, wrap(a + s), b))
        go(h, 0, 1, own.at[h], at(h, a, b), device(h, wrap(a - s), b))
        go(h, 0, 2, own.at[h], at(h, a, b), device(h, wrap(a + 2), b))

    for h in range(2):
        first(h)
    for h in range(2):
        share(h, 0, own.at[h], at(h, *mine(h)))
        spread(h, 1, 0, own.at[h], *mine(h))
    fill()
    for h in range(2):
        a, b = mine(h)
        near = wrap(a - s)
        come(h, 0, 0, at(h, near, b))
        spread(h, 2, 4, at(h, near, b), near, b)
        share(h, 4, at(h, near, b), at(h, near, b))
    for h in range(2):
        a, b = mine(h)
        near = wrap(a + s)
        come(h, 0, 1, at(h, near, b))
        spread(h, 3, 8, at(h, near, b), near, b)
        share(h, 8, at(h, near, b), at(h, near, b))
    fill()
    for h in range(2):
        a, b = mine(h)
        far = wrap(a + 2)
        come(h, 0, 2, at(h, far, b))
        spread(h, 4, 12, at(h, far, b), far, b)
        share(h, 12, at(h, far, b), at(h, far, b))
    fill()
    steps = (0, 0, -1, 1, 2)

    def near(group):
        for h in range(2):
            a, b = mine(h)
            row = wrap(a + steps[group] * s)
            side = wrap(b - s)
            come(h, group, 0, at(h, row, side))
            go(h, group, 2, at(h, row, side), at(h, row, side), device(h, a, wrap(b + s)))
            share(h, 4 * (group - 1) + 1, at(h, row, side), at(h, row, side))
        fill()

    def other(group):
        for h in range(2):
            a, b = mine(h)
            row = wrap(a + steps[group] * s)
            side = wrap(b + s)
            come(h, group, 1, at(h, row, side))
            share(h, 4 * (group - 1) + 2, at(h, row, side), at(h, row, side))

    def far(group):
        for h in range(2):
            a, b = mine(h)
            row = wrap(a + steps[group] * s)
            opposite = wrap(b + 2)
            come(h, group, 2, at(h, row, opposite))
            share(h, 4 * (group - 1) + 3, at(h, row, opposite), at(h, row, opposite))

    across = (0, 2, 1, 3)

    def from_pair(k, n):
        for h, slot in ((0, 4 * across[k] + across[n]), (1, 4 * across[n] + across[k])):
            where = full.at[0, 0, 1 - c, h]
            remote(where, where, dsend.at[h, slot], drecv.at[h, slot], plane_id(z, y, 1 - c)).wait_recv()

    def arrived(k, columns=(0, 1, 2, 3)):
        for n in columns:
            from_pair(k, n)
        if row_done is not None:
            row_done(k, columns)

    near(1)
    near(2)
    other(1)
    near(3)
    other(2)
    near(4)
    other(3)
    other(4)
    far(1)
    if row_done is not None:
        arrived(0)
    far(2)
    far(3)
    if row_done is not None:
        arrived(1)
        arrived(2)
    far(4)
    if row_done is not None:
        arrived(3, (0, 1, 2))
        arrived(3, (3,))
    else:
        for k in range(4):
            arrived(k)
    return sent


def gather_sems():
    return [
        pltpu.SemaphoreType.DMA((2, 5, 3)),
        pltpu.SemaphoreType.DMA((2, 5, 3)),
        pltpu.SemaphoreType.DMA((2, 16)),
        pltpu.SemaphoreType.DMA((2, 16)),
    ]


def queries_kernel(pool_bits, page_len, q_hbm, table_hbm, len_hbm, full_ref, list_ref,
                   table_ref, len_ref, lo_ref, hi_ref, part_ref, total_ref, lsem, ssem, rsem, dsend, drecv):
    z, y, c, s = place()
    me = (z * 4 + y) * 2 + c
    loads = [
        pltpu.make_async_copy(src, dst, lsem.at[n])
        for n, (src, dst) in enumerate(
            ((q_hbm, full_ref.at[z, y, c]), (table_hbm, table_ref), (len_hbm, len_ref)))
    ]
    for load in loads:
        load.start()
    greet([plane_id(wrap(z + 1), y, c), plane_id(wrap(z - 1), y, c), plane_id(z, wrap(y + 1), c),
           plane_id(z, wrap(y - 1), c), plane_id(wrap(z + 2), y, c), plane_id(z, wrap(y + 2), c), plane_id(z, y, 1 - c)])
    loads[0].wait()

    def place_pages():
        for load in loads[1:]:
            load.wait()
        slots = table_ref.shape[0]
        slot = lax.broadcasted_iota(jnp.int32, (slots, 128), 0)
        lane = lax.broadcasted_iota(jnp.int32, (slots, 128), 1)
        blocks = table_ref.shape[1] // 128
        mine, tokens, page, owner = [], [], [], []
        for t in range(blocks):
            ids = table_ref[:, t * 128:(t + 1) * 128]
            length = jnp.broadcast_to(len_ref[t:t + 1, :], (slots, 128))
            left = jnp.clip(length - slot * page_len, 0, page_len)
            mine.append(jnp.where(((ids >> pool_bits) == me) & (left > 0), 1.0, 0.0))
            tokens.append(left)
            page.append(ids & ((1 << pool_bits) - 1))
            owner.append(lane + t * 128)
        mine, tokens, page, owner = (jnp.concatenate(v, axis=0) for v in (mine, tokens, page, owner))
        rows = slots * blocks
        mine_h = mine.astype(BF16)
        i = lax.broadcasted_iota(jnp.int32, (rows, rows), 0)
        j = lax.broadcasted_iota(jnp.int32, (rows, rows), 1)
        same = (i // slots) == (j // slots)

        def count(which, what):
            return jnp.dot(jnp.where(which, 1.0, 0.0).astype(BF16), what, preferred_element_type=F32)

        earlier = count(same & (j < i), mine_h)
        column = count(same, mine_h)
        blocks_before = count((j // slots) < (i // slots), mine_h)
        i = lax.broadcasted_iota(jnp.int32, (128, 128), 0)
        j = lax.broadcasted_iota(jnp.int32, (128, 128), 1)
        ahead = jnp.where(i < j, 1.0, 0.0).astype(BF16)
        every = jnp.ones((128, 128), BF16)
        start = jnp.dot(column.astype(BF16), ahead, preferred_element_type=F32)
        start = start + jnp.dot(blocks_before.astype(BF16), every, preferred_element_type=F32)
        rank = (start + earlier).astype(jnp.int32)
        lo_ref[...] = jnp.where(mine > 0.0, rank & 127, -1)
        hi_ref[...] = jnp.where(mine > 0.0, rank >> 7, -1)
        part_ref[0] = (page & 255).astype(F32)
        part_ref[1] = (owner & 255).astype(F32)
        part_ref[2] = ((page >> 8) + ((owner >> 8) << 2) + ((tokens - 1) << 4)).astype(F32)
        part_ref[3] = jnp.where(earlier > 0.0, 0.0, 1.0)
        last = jnp.where(column > 0.0, start + column - 1.0, float(NOTHING)).astype(jnp.int32)
        list_ref[8:16, :] = jnp.concatenate([last[t * slots:t * slots + 1] for t in range(blocks)], axis=0)
        number = (start + column)[rows - 1:rows, 127:128]
        list_ref[16:24, :] = jnp.broadcast_to(number, (8, 128)).astype(jnp.int32)
        total_ref[...] = jnp.zeros_like(total_ref)

    sub = lax.broadcasted_iota(jnp.int32, (128, 128), 0).astype(F32).astype(BF16)
    one, nil = jnp.ones((128, 128), BF16), jnp.zeros((128, 128), BF16)
    sub8 = lax.broadcasted_iota(jnp.int32, (8, 128), 0)

    def scatter(part):
        def step(n, carry):
            base = pl.multiple_of(n * 8, 8)
            lo8 = lo_ref[pl.ds(base, 8), :].astype(F32)
            hi8 = hi_ref[pl.ds(base, 8), :]
            p8 = [part_ref[k, pl.ds(base, 8), :] for k in range(4)]
            wide, tall = [], []
            for r in range(8):
                wide.append(jnp.where(sub == jnp.broadcast_to(lo8[r:r + 1, :], (128, 128)).astype(BF16), one, nil))
                hit = sub8 == hi8[r:r + 1, :]
                tall.append(jnp.concatenate(
                    [jnp.where(hit, p8[k][r:r + 1, :], 0.0) for k in range(4)], axis=0).astype(BF16))
            wide = jnp.concatenate(wide, axis=1)
            tall = jnp.concatenate(tall, axis=1)
            total_ref[...] += lax.dot_general(wide, tall, NT, preferred_element_type=F32)
            return carry

        steps = lo_ref.shape[0] // 32
        lax.fori_loop(part * steps, (part + 1) * steps, step, 0)

    def write_list():
        total = jnp.concatenate([total_ref[...], jnp.zeros((128, 96), F32)], axis=1).T.astype(jnp.int32)
        p0, p1, p2, p3 = (total[8 * k:8 * k + 8, :] for k in range(4))
        page = p0 + ((p2 & 3) << 8)
        owner = p1 + (((p2 >> 2) & 3) << 8)
        tokens = (p2 >> 4) + 1
        list_ref[0:8, :] = page + (owner << 10) + (tokens << 20) + (p3 << 25)

    def start_list():
        place_pages()
        scatter(0)
        scatter(1)

    pieces = [start_list, None, functools.partial(scatter, 2), functools.partial(scatter, 3), None, None, write_list]
    for copy in plane_gather(full_ref.at[z, y, c], full_ref, ssem, rsem, dsend, drecv, between=pieces):
        copy.wait_send()


def gather_queries(queries, table, lengths, pool, page_len):
    req = table.shape[1]
    rows = table.shape[0] * req // 128
    _, half, heads, dim = queries.shape
    return pl.pallas_call(
        functools.partial(queries_kernel, pool.bit_length() - 1, page_len),
        out_shape=(
            jax.ShapeDtypeStruct((4, 4, 2, 2, half, heads, dim), BF16),
            jax.ShapeDtypeStruct((24, 128), jnp.int32),
        ),
        in_specs=[HBM] * 3,
        out_specs=(VMEM, VMEM),
        scratch_shapes=[
            pltpu.VMEM(table.shape, jnp.int32),
            pltpu.VMEM(lengths.shape, jnp.int32),
            pltpu.VMEM((rows, 128), jnp.int32),
            pltpu.VMEM((rows, 128), jnp.int32),
            pltpu.VMEM((4, rows, 128), F32),
            pltpu.VMEM((128, 32), F32),
            pltpu.SemaphoreType.DMA((3,)),
        ] + gather_sems(),
        compiler_params=pltpu.CompilerParams(collective_id=0, has_side_effects=True, vmem_limit_bytes=8 << 20),
        cost_estimate=pl.CostEstimate(flops=10**10, bytes_accessed=1 << 23, transcendentals=0),
        name="gather_queries",
    )(queries, table, lengths)


def pages_kernel(scale, list_ref, q_ref, k_ref, v_ref, acc_ref, sum_ref, top_ref, wait_ref, peak_ref, mass_ref):
    lane = lax.broadcasted_iota(jnp.int32, (16, 128), 1)
    blank = jnp.where(lane < 32, LOW, 0.0)
    zero = jnp.zeros((16, 128), F32)
    sum_ref[NOTHING] = zero
    top_ref[NOTHING] = blank
    wait_ref[...] = jnp.zeros_like(wait_ref)
    peak_ref[...] = jnp.zeros_like(peak_ref)
    mass_ref[...] = jnp.zeros_like(mass_ref)

    i = lax.broadcasted_iota(jnp.int32, (16, 128), 0)
    kv_match = (i // 8) == (lane % 2)
    token = (lane % 32) // 2
    token_of = [jnp.where(kv_match & (lane // 32 == n), token, 1 << 20) for n in range(4)]

    def entry(base, e):
        word = list_ref[base // 128, base % 128 + e]
        return word & 1023, (word >> 10) & 1023, (word >> 20) & 31, (word >> 25) & 1

    def step(n, carry):
        past = jnp.maximum(n - 1, 0) * BATCH
        base = n * BATCH
        before = [entry(past, e) for e in range(BATCH)]
        now = [entry(base, e) for e in range(BATCH)]
        outs, scores = [], []
        for g in range(BATCH // 4):
            four = slice(4 * g, 4 * g + 4)
            vs = jnp.concatenate([v_ref[p] for p, _, _, _ in before[four]], axis=0)
            outs.append(jnp.dot(wait_ref[g], vs, preferred_element_type=F32))
            qs = jnp.concatenate([q_ref[r] for _, r, _, _ in now[four]], axis=0)
            ks = jnp.concatenate([k_ref[p] for p, _, _, _ in now[four]], axis=0)
            scores.append(lax.dot_general(qs, ks, NT, preferred_element_type=F32))
        top, mass, acc = carry
        for e, (_, _, _, first) in enumerate(before):
            old = jnp.where(first == 1, LOW, top)
            p = peak_ref[e]
            top = jnp.maximum(old, p)
            f_old = jnp.exp(old - top)
            f_new = jnp.exp(p - top)
            mass = mass * f_old + mass_ref[e] * f_new
            acc = acc * f_old + outs[e // 4][16 * (e % 4):16 * (e % 4) + 16] * f_new
            sum_ref[past + e] = acc
            top_ref[past + e] = jnp.where(lane < 32, top, mass)
        for g in range(BATCH // 4):
            weights = []
            for e in range(4):
                valid = token_of[e] < now[4 * g + e][2]
                sc = jnp.where(valid, scores[g][16 * e:16 * e + 16] * scale, LOW)
                peak = jnp.max(sc, axis=1, keepdims=True)
                w = jnp.where(valid, jnp.exp(sc - peak), 0.0)
                peak_ref[4 * g + e] = jnp.broadcast_to(peak, (16, 128))
                mass_ref[4 * g + e] = jnp.broadcast_to(jnp.sum(w, axis=1, keepdims=True), (16, 128))
                weights.append(w)
            wait_ref[g] = jnp.concatenate(weights, axis=0).astype(BF16)
        return top, mass, acc

    batches = (list_ref[16, 0] + BATCH - 1) // BATCH
    lax.fori_loop(0, batches + 1, step, (zero, zero, zero))

    def spread(d, carry):
        tops = blank
        line, first = 8 + d // 4, (d % 4) * 32
        for row in range(32):
            last = list_ref[line, first + row]
            acc = sum_ref[last]
            tops = jnp.where((lane == row) | (lane == row + 32), top_ref[last], tops)
            for hh in range(2):
                acc_ref[hh, d, row] = acc[8 * hh:8 * hh + 8]
        for hh in range(2):
            acc_ref[hh, d, 32] = tops[8 * hh:8 * hh + 8]
        return carry

    lax.fori_loop(0, acc_ref.shape[1], spread, 0)


def attend_pages(words, all_queries, keys, values):
    req, heads, dim = all_queries.shape
    return pl.pallas_call(
        functools.partial(pages_kernel, dim ** (-0.5)),
        out_shape=jax.ShapeDtypeStruct((2, req // 32, 33, 8, 128), F32),
        in_specs=[SMEM, VMEM, VMEM, VMEM],
        out_specs=VMEM,
        scratch_shapes=[
            pltpu.VMEM((NOTHING + 1, heads, dim), F32),
            pltpu.VMEM((NOTHING + 1, heads, dim), F32),
            pltpu.VMEM((BATCH // 4, 4 * heads, dim), BF16),
            pltpu.VMEM((BATCH, heads, dim), F32),
            pltpu.VMEM((BATCH, heads, dim), F32),
        ],
        compiler_params=pltpu.CompilerParams(vmem_limit_bytes=20 << 20),
        name="attend_pages",
    )(words, all_queries, keys, values)


def merge(dst, one, other):
    lane = lax.broadcasted_iota(jnp.int32, (8, 128), 1)
    t1, t2 = one[32], other[32]
    top = jnp.maximum(t1, t2)
    f1 = jnp.exp(t1 - top)
    f2 = jnp.exp(t2 - top)
    mass = t1 * pltpu.roll(f1, 32, 1) + t2 * pltpu.roll(f2, 32, 1)
    for row in range(32):
        dst[row] = one[row] * f1[:, row:row + 1] + other[row] * f2[:, row:row + 1]
    dst[32] = jnp.where(lane < 32, top, mass)


def finish_kernel(part_ref, w_ref, att_ref, proj_ref, unit, pair, far1, near1, next1, far2, near2, next2,
                  tmp, own, full, cols, farx, nearx, nextx,
                  s0, r0, s1, r1, s2, r2, ssem, rsem, dsend, drecv, sx, rx):
    z, y, c, s = place()
    x = lax.axis_index("mp")
    home = plane_id(z, y, c)
    greet([plane_id(wrap(z + 1), y, c), plane_id(wrap(z - 1), y, c), plane_id(z, wrap(y + 1), c),
           plane_id(z, wrap(y - 1), c), plane_id(wrap(z + 2), y, c), plane_id(z, wrap(y + 2), c), plane_id(z, y, 1 - c), {"mp": wrap(x + 1)}, {"mp": wrap(x - 1)}])

    def spot(hh, oa, ob):
        dz = oa + hh * (ob - oa)
        dy = ob + hh * (oa - ob)
        return wrap(z + dz), wrap(y + dy)

    def step_of(n):
        m = n % 3
        return 2 * ((3 - n) // 3) + s * (m * (5 - 3 * m) // 2)

    def swap(hh, zt, yt):
        return remote(part_ref.at[hh, (zt * 4 + yt) * 2 + 1 - c], pair.at[hh, zt, yt], s0.at[hh, zt, yt],
                      r0.at[hh, zt, yt], plane_id(z, y, 1 - c))

    def hop(hh, sign):
        zt, yt = spot(hh, sign * s, 0)
        return plane_id(zt, yt, c)

    def hop2(hh, sign):
        zt, yt = spot(hh, 0, sign * s)
        return plane_id(zt, yt, c)

    def far_place(n):
        m, odd = (n + 1) // 2, n % 2
        return wrap(z + step_of((1 - odd) * m)), wrap(y + step_of(odd * m))

    def rest_place(n):
        m, k = n // 3, n % 3
        return wrap(z + step_of(2 - m + 3 * (m // 2))), wrap(y + step_of(2 - k + 3 * (k // 2)))

    def give(where):
        def step(n, carry):
            zt, yt = where(n)
            for hh in range(2):
                swap(hh, zt, yt).start()
            return carry
        return step

    def send1(kind, hh, ob, zt, yt):
        dst = (far1, near1, next1)[kind].at[hh, ob]
        return remote(unit.at[hh, zt, yt], dst, s1.at[kind, hh, ob], r1.at[kind, hh, ob], hop(hh, 1 if kind < 2 else -1))

    def both_cores(hh, zt, yt):
        swap(hh, zt, yt).wait_recv()
        merge(unit.at[hh, zt, yt], part_ref.at[hh, (zt * 4 + yt) * 2 + c], pair.at[hh, zt, yt])

    def far_units(k, carry):
        hh, ob = k % 2, k // 2
        zt, yt = spot(hh, 2, step_of(ob))
        both_cores(hh, zt, yt)
        send1(0, hh, ob, zt, yt).start()
        return carry

    def next_units(k, carry):
        hh, ob = k % 2, k // 2
        zt, yt = spot(hh, -s, step_of(ob))
        both_cores(hh, zt, yt)
        send1(2, hh, ob, zt, yt).start()
        return carry

    def near_units(k, carry):
        hh, ob = k % 2, k // 2
        zt, yt = spot(hh, s, step_of(ob))
        both_cores(hh, zt, yt)
        send1(0, hh, ob, zt, yt).wait_recv()
        merge(unit.at[hh, zt, yt], unit.at[hh, zt, yt], far1.at[hh, ob])
        send1(1, hh, ob, zt, yt).start()
        return carry

    def own_units(k, carry):
        hh, ob = k % 2, k // 2
        zt, yt = spot(hh, 0, step_of(ob))
        both_cores(hh, zt, yt)
        return carry

    lax.fori_loop(0, 7, give(far_place), 0)
    lax.fori_loop(0, 9, give(rest_place), 0)
    lax.fori_loop(0, 8, far_units, 0)
    lax.fori_loop(0, 8, next_units, 0)
    lax.fori_loop(0, 8, near_units, 0)
    lax.fori_loop(0, 8, own_units, 0)

    def send2(kind, hh, zt, yt):
        dst = (far2, near2, next2)[kind].at[hh]
        return remote(unit.at[hh, zt, yt], dst, s2.at[kind, hh], r2.at[kind, hh], hop2(hh, -1 if kind < 2 else 1))

    def gathered(hh, ob):
        zt, yt = spot(hh, 0, step_of(ob))
        send1(2, hh, ob, zt, yt).wait_recv()
        merge(unit.at[hh, zt, yt], unit.at[hh, zt, yt], next1.at[hh, ob])
        send1(1, hh, ob, zt, yt).wait_recv()
        merge(unit.at[hh, zt, yt], unit.at[hh, zt, yt], near1.at[hh, ob])
        return zt, yt

    def far_blocks(hh, carry):
        zt, yt = gathered(hh, 0)
        send2(0, hh, zt, yt).start()
        return carry

    def next_blocks(hh, carry):
        zt, yt = gathered(hh, 1)
        send2(2, hh, zt, yt).start()
        return carry

    def near_sums(hh, carry):
        gathered(hh, 2)
        return carry

    def near_blocks(hh, carry):
        zt, yt = spot(hh, 0, -s)
        send2(0, hh, zt, yt).wait_recv()
        merge(unit.at[hh, zt, yt], unit.at[hh, zt, yt], far2.at[hh])
        send2(1, hh, zt, yt).start()
        return carry

    def own_blocks(hh, carry):
        zt, yt = gathered(hh, 3)
        send2(2, hh, zt, yt).wait_recv()
        merge(unit.at[hh, zt, yt], unit.at[hh, zt, yt], next2.at[hh])
        send2(1, hh, zt, yt).wait_recv()
        merge(unit.at[hh, zt, yt], unit.at[hh, zt, yt], near2.at[hh])
        return carry

    for phase in (far_blocks, next_blocks, near_sums, near_blocks, own_blocks):
        lax.fori_loop(0, 2, phase, 0)

    masses = [unit[hh, z, y, 32] for hh in range(2)]
    for row in range(32):
        both = [unit[hh, z, y, row] / masses[hh][:, 32 + row:33 + row] for hh in range(2)]
        for hh in range(2):
            tmp[hh, row] = both[hh]
        att_ref[row] = jnp.concatenate(both, axis=0).astype(BF16)
    for hh in range(2):
        for head in range(8):
            own[hh, head] = tmp[hh, :, head, :].astype(BF16)
    for hh in range(2):
        full[z, y, c, hh] = own[hh]

    def sendx(kind, t, q):
        rows = pl.ds(pl.multiple_of(q * QUARTER, QUARTER) if not isinstance(q, int) else q * QUARTER, QUARTER)
        dst = (farx, nearx, nextx)[kind].at[rows]
        return remote(cols.at[t, rows], dst, sx.at[kind, q], rx.at[kind, q],
                      {"mp": wrap(x + (s if kind < 2 else -s))})

    targets = [wrap(z + step) for step in (0, -s, s, 2)]
    columns_of = [wrap(y + step) for step in (0, -s, s, 2)]

    def pass_on(k):
        t = targets[k]

        @pl.when(wrap(t - x - s) == 0)
        def _():
            for q in columns_of:
                rows = pl.ds(pl.multiple_of(q * QUARTER, QUARTER), QUARTER)
                sendx(0, t, q).wait_recv()
                cols[t, rows] = cols[t, rows] + farx[rows]
                sendx(1, t, q).start()

    def send_on(t, quarters):
        @pl.when(wrap(t - x - 2) == 0)
        def _():
            for q in quarters:
                sendx(0, t, q).start()

        @pl.when(wrap(t - x + s) == 0)
        def _():
            for q in quarters:
                sendx(2, t, q).start()

    def project(k, columns):
        t = targets[k]
        if len(columns) == 4:
            rows = [full[t, :, :, hh, head].reshape(256, 128) for hh in range(2) for head in range(8)]
            cols[t] = jnp.dot(jnp.concatenate(rows, axis=1), w_ref[...], preferred_element_type=F32)
            send_on(t, columns_of)
            return
        for n in columns:
            q = columns_of[n]
            rows = [full[t, q, :, hh, head].reshape(QUARTER, 128) for hh in range(2) for head in range(8)]
            cols[t, pl.ds(pl.multiple_of(q * QUARTER, QUARTER), QUARTER)] = jnp.dot(
                jnp.concatenate(rows, axis=1), w_ref[...], preferred_element_type=F32)
            send_on(t, [q])

    sent = plane_gather(own, full, ssem, rsem, dsend, drecv, row_done=project)
    for k in range(4):
        pass_on(k)
    for q in columns_of:
        rows = pl.ds(pl.multiple_of(q * QUARTER, QUARTER), QUARTER)
        sendx(2, x, q).wait_recv()
        sendx(1, x, q).wait_recv()
        proj_ref[rows] = (cols[x, rows] + nextx[rows] + nearx[rows]).astype(BF16)

    for kind in range(3):
        for q in range(4):
            sendx(kind, x, q).wait_send()
    for copy in sent:
        copy.wait_send()

    def drain(k, carry):
        hh, ob = k % 2, k // 2
        for oa in range(4):
            zt, yt = spot(hh, step_of(oa), step_of(ob))
            swap(hh, zt, yt).wait_send()
        for kind in range(3):
            send1(kind, hh, ob, z, y).wait_send()
        return carry

    lax.fori_loop(0, 8, drain, 0)

    def drain2(hh, carry):
        for kind in range(3):
            send2(kind, hh, z, y).wait_send()
        return carry

    lax.fori_loop(0, 2, drain2, 0)


def finish(parts, weight, rows):
    unit = (33, 8, 128)
    dma = pltpu.SemaphoreType.DMA
    return pl.pallas_call(
        finish_kernel,
        out_shape=(
            jax.ShapeDtypeStruct((rows, 16, 128), BF16),
            jax.ShapeDtypeStruct((256, weight.shape[1]), BF16),
        ),
        in_specs=[VMEM, VMEM],
        out_specs=(VMEM, VMEM),
        scratch_shapes=[
            pltpu.VMEM((2, 4, 4) + unit, F32),
            pltpu.VMEM((2, 4, 4) + unit, F32),
            pltpu.VMEM((2, 4) + unit, F32),
            pltpu.VMEM((2, 4) + unit, F32),
            pltpu.VMEM((2, 4) + unit, F32),
            pltpu.VMEM((2,) + unit, F32),
            pltpu.VMEM((2,) + unit, F32),
            pltpu.VMEM((2,) + unit, F32),
            pltpu.VMEM((2, 32, 8, 128), F32),
            pltpu.VMEM((2, 8, 32, 128), BF16),
            pltpu.VMEM((4, 4, 2, 2, 8, 32, 128), BF16),
            pltpu.VMEM((4, 256, 256), F32),
            pltpu.VMEM((256, 256), F32),
            pltpu.VMEM((256, 256), F32),
            pltpu.VMEM((256, 256), F32),
            dma((2, 4, 4)),
            dma((2, 4, 4)),
            dma((3, 2, 4)),
            dma((3, 2, 4)),
            dma((3, 2)),
            dma((3, 2)),
        ] + gather_sems() + [dma((3, 4)), dma((3, 4))],
        compiler_params=pltpu.CompilerParams(collective_id=1, has_side_effects=True, vmem_limit_bytes=24 << 20),
        name="finish",
    )(parts, weight)


def body(queries, lookup_sheets, content_sheets, page_table, context_len, out_weight):
    req = page_table.shape[0]
    pool, page_len, kv, dim = lookup_sheets.shape
    rows, heads, _ = queries.shape
    all_queries, words = gather_queries(
        queries.reshape(2, rows // 2, heads, dim),
        *(pltpu.with_memory_space_constraint(a, pltpu.HBM)
          for a in (page_table.T, context_len.reshape(req // 128, 128))),
        pool,
        page_len,
    )
    parts = attend_pages(
        words,
        all_queries.reshape(req, heads, dim),
        lookup_sheets.reshape(pool, page_len * kv, dim),
        content_sheets.reshape(pool, page_len * kv, dim),
    )
    return finish(parts, out_weight, rows)


def solution(mesh):
    finer = Mesh(mesh.devices.reshape(4, 4, 2, mesh.shape["mp"]), ("dp_0", "dp_1", "dp_2", "mp"))
    return jax.shard_map(
        body,
        mesh=finer,
        in_specs=(
            P(DP, "mp", None),
            P(DP, None, "mp", None),
            P(DP, None, "mp", None),
            P(),
            P(),
            P("mp", DP),
        ),
        out_specs=(P(DP, "mp", None), P("mp", DP)),
        check_vma=False,
    )
```
